32 devices in a mesh: dp: 4 (over x, y), tp: 8 (over z, core).
Axes of the slice: x: 2, y: 2, z: 4, core: 2. Of those that a mesh axis runs over, the one named last changes fastest.
Arguments:
- x: bfloat16 [8192, 8192], P('dp'), parts along dimension 0
- gain: bfloat16 [8192], replicated
- wq: bfloat16 [8192, 8192], P(None, 'tp')
- wk: bfloat16 [8192, 8192], P(None, 'tp')
- wv: bfloat16 [8192, 8192], P(None, 'tp')
- wo: bfloat16 [8192, 8192], P('tp')
Outputs:
- output: bfloat16 [8192, 8192], P('dp'), parts along dimension 0
There are 4 independent parts. The reference program is written for one: setup_inputs(seed, part) draws one part's arguments, and reference() takes and returns one part's arrays. A program takes and returns all parts, laid end to end along the dimension named above; an argument that names none is the same for every part.
All inputs are finite; a program needn't handle non-finite values.
Results may differ from the reference program's by a relative error of at most 0.012.
Values are sent between devices in bfloat16 or wider.
A program may use at most 2 GiB of HBM per device.

```python
import jax
import jax.numpy as jnp
from jax import lax

ROWS = 2048
D = 8192
HEADS = 64
KV_HEADS = 64
HEAD = 128
THETA = 10000


def setup_inputs(seed: int = 0, part: int = 0) -> dict:
    kx, kn, kq, kk, kv, ko = jax.random.split(jax.random.key(seed), 6)

    def weights(key, rows, columns):
        return jax.random.normal(key, (rows, columns), jnp.float32) * rows**-0.5

    drawn = {
        "x": jax.random.normal(jax.random.fold_in(kx, part), (ROWS, D), jnp.float32),
        "gain": 1 + 0.1 * jax.random.normal(kn, (D,), jnp.float32),
        "wq": 2 * weights(kq, D, HEADS * HEAD),
        "wk": 2 * weights(kk, D, KV_HEADS * HEAD),
        "wv": 4 * weights(kv, D, KV_HEADS * HEAD),
        "wo": weights(ko, HEADS * HEAD, D),
    }
    return {k: v.astype(jnp.bfloat16) for k, v in drawn.items()}


def normed(x, gain):
    wide = x.astype(jnp.float32)
    scale = lax.rsqrt(jnp.mean(wide * wide, -1, keepdims=True) + 1e-6)
    return (wide * scale * gain.astype(jnp.float32)).astype(jnp.bfloat16)


def turned(t, place, theta):
    half = t.shape[-1] // 2
    angle = place.astype(jnp.float32)[:, None] * theta ** (-jnp.arange(half, dtype=jnp.float32) / half)
    cos, sin = jnp.cos(angle)[:, None], jnp.sin(angle)[:, None]
    a, b = t[..., :half].astype(jnp.float32), t[..., half:].astype(jnp.float32)
    return jnp.concatenate([a * cos - b * sin, b * cos + a * sin], -1).astype(jnp.bfloat16)


def matmul(a, w):
    return jnp.dot(a, w, preferred_element_type=jnp.float32).astype(jnp.bfloat16)


def einsum(form, a, b):
    return jnp.einsum(form, a.astype(jnp.float32), b.astype(jnp.float32))


def attention(q, k, v):
    scores = einsum("tgsd,ugd->gstu", q, k) * q.shape[-1] ** -0.5
    token = jnp.arange(q.shape[0])
    scores = jnp.where(token[:, None] >= token, scores, -jnp.inf)
    weights = jax.nn.softmax(scores, -1).astype(jnp.bfloat16)
    return einsum("gstu,ugd->tgsd", weights, v).astype(jnp.bfloat16)


def reference(x, gain, wq, wk, wv, wo):
    a, place = normed(x, gain), jnp.arange(ROWS)
    q = turned(matmul(a, wq).reshape(ROWS, HEADS, HEAD), place, THETA).reshape(ROWS, KV_HEADS, -1, HEAD)
    k = turned(matmul(a, wk).reshape(ROWS, KV_HEADS, HEAD), place, THETA)
    v = matmul(a, wv).reshape(ROWS, KV_HEADS, HEAD)
    seen = attention(q, k, v).reshape(ROWS, HEADS * HEAD)
    return (x.astype(jnp.float32) + jnp.dot(seen, wo, preferred_element_type=jnp.float32)).astype(jnp.bfloat16)
```

```python
import functools

import jax
import jax.numpy as jnp
import numpy as np
from jax import lax
from jax.experimental import pallas as pl
from jax.experimental.pallas import tpu as pltpu
from jax.sharding import PartitionSpec as P

HEAD = 128
THETA = 10000
NEG = -1e30
HIDDEN = 2 * NEG
LOG2E = 1.4426950408889634
R = 256
KB = 2048
PC = 512
NB = 8
KEYS = 512
NI = 4
MESH = pl.DeviceIdType.MESH


def _dot(a, b, ca, cb):
    return lax.dot_general(a, b, (((ca,), (cb,)), ((), ())), preferred_element_type=jnp.float32)


def _kernel(x_ref, gain_ref, freq_ref, wq_ref, wk_ref, wv_ref, wo_ref, y_ref,
            xb, a_s, wbuf, wo_s, k_s, vt_s, s_s, q_s, cos_s, sin_s, top_s, mix_s,
            part, from_e, from_m, obuf, sbuf, xres,
            x_sem, w_sem, wo_sem, xr_sem, r_part, r_e, r_m, r_res, r_y, s_o, s_u, s_e, s_p, s_l):
    rows, d = x_ref.shape
    chunks = rows // R
    n_comm = chunks * NI
    scale = HEAD**-0.5
    e = scale * LOG2E
    tp = lax.axis_index("tp")
    z, core = lax.div(tp, 2), lax.rem(tp, 2)
    middle = (z == 1) | (z == 2)
    end = jnp.logical_not(middle)
    partner = z * 2 + 1 - core
    inner = jnp.where(z < 2, 1, 2) * 2 + core
    outer = jnp.where(z < 2, 0, 3) * 2 + core
    other = (3 - z) * 2 + core
    near = jnp.where(z < 2, 0, 1)
    half = d // 2
    quarter = d // 4

    def col(side, ab, i):
        g = near if ab == 1 else 1 - near
        return pl.multiple_of(side * half + g * quarter + i * PC, PC)

    def row(k):
        return pl.ds(pl.multiple_of(k * R, R), R)

    def remote(src, dst, send, recv, to):
        return pltpu.make_async_remote_copy(src, dst, send, recv, device_id={"tp": to}, device_id_type=MESH)

    def load_x(k):
        return pltpu.make_async_copy(x_ref.at[row(k)], xb, x_sem)

    def load_w(t, n):
        m, kb = n // 4, n % 4
        w = (wq_ref, wk_ref, wv_ref)[m]
        i = lax.rem(t, NI)
        slot = lax.rem(t * 12 + n, NB)
        return pltpu.make_async_copy(
            w.at[pl.ds(kb * KB, KB), pl.ds(pl.multiple_of(i * 256, 256), 256)], wbuf.at[slot], w_sem.at[slot])

    def load_wo(i, ty):
        side = 1 - core if ty < 2 else core
        return pltpu.make_async_copy(wo_ref.at[:, pl.ds(col(side, ty % 2, i), PC)], wo_s.at[i, ty], wo_sem.at[i, ty])

    def load_res(k, i):
        return pltpu.make_async_copy(x_ref.at[row(k), pl.ds(col(core, 1, i), PC)], xres.at[i], xr_sem.at[i])

    def to_partner(k, ab, i):
        return remote(obuf.at[ab, i], part.at[lax.rem(k, 2), ab, i], s_o.at[ab, i], r_part.at[k, ab, i], partner)

    def to_inner(k, ab, i):
        p = lax.rem(k, 2)
        return remote(sbuf.at[p, ab, i], from_e.at[p, ab, i], s_u.at[p, ab, i], r_e.at[k, ab, i], inner)

    def to_other(k, i):
        p = lax.rem(k, 2)
        return remote(sbuf.at[p, 0, i], from_m.at[p, i], s_u.at[p, 0, i], r_m.at[k, i], other)

    def y_at(k, side, ab, i):
        return y_ref.at[row(k), pl.ds(col(side, ab, i), PC)]

    def result_to_other(k, i):
        p = lax.rem(k, 2)
        return remote(sbuf.at[p, 1, i], y_at(k, core, 1, i), s_u.at[p, 1, i], r_res.at[k, 0, i], other)

    def result_to_outer(k, ab, i, src):
        return remote(src, y_at(k, core, ab, i), s_e.at[lax.rem(k, 2), ab, i], r_res.at[k, ab, i], outer)

    def result_to_partner(k, ab, i, src):
        return remote(src, y_at(k, core, ab, i), s_p.at[lax.rem(k, 2), ab, i], r_y.at[k, ab, i], partner)

    def result_here(k, i):
        p = lax.rem(k, 2)
        return pltpu.make_async_copy(sbuf.at[p, 1, i], y_at(k, core, 1, i), s_l.at[p, i])

    barrier = pltpu.get_barrier_semaphore()

    def greet(to):
        pl.semaphore_signal(barrier, inc=1, device_id={"tp": to}, device_id_type=MESH)

    load_x(0).start()
    for n in range(NB):
        load_w(0, n).start()
    greet(partner)

    @pl.when(end)
    def _():
        greet(inner)
        pl.semaphore_wait(barrier, 2)

    @pl.when(middle)
    def _():
        greet(outer)
        greet(other)
        pl.semaphore_wait(barrier, 3)

    def clear(h, carry):
        vt_s[h, :HEAD, :] = jnp.zeros((HEAD, rows), jnp.bfloat16)
        vt_s[h, HEAD:, :] = jnp.ones((8, rows), jnp.bfloat16)
        return carry

    lax.fori_loop(0, 2 * NI, clear, 0)

    def norm(k):
        load_x(k).wait()

        def some(b, carry):
            at = pl.ds(pl.multiple_of(b * 16, 16), 16)
            wide = xb[at, :].astype(jnp.float32)
            size = lax.rsqrt(jnp.mean(wide * wide, -1, keepdims=True) + 1e-6)
            a_s[at, :] = (wide * size * gain_ref[...].astype(jnp.float32)).astype(jnp.bfloat16)
            return carry

        lax.fori_loop(0, R // 16, some, 0)

        @pl.when(k < chunks - 1)
        def _():
            load_x(k + 1).start()

        place = (k * R + lax.broadcasted_iota(jnp.int32, (R, HEAD), 0)).astype(jnp.float32)
        angle = place * freq_ref[...]
        sign = jnp.where(lax.broadcasted_iota(jnp.int32, (R, HEAD), 1) < HEAD // 2, -1.0, 1.0)
        cos_s[...] = jnp.cos(angle)
        sin_s[...] = jnp.sin(angle) * sign

    def project(t, m):
        total = None
        for kb in range(4):
            n = m * 4 + kb
            slot = lax.rem(t * 12 + n, NB)
            load_w(t, n).wait()
            some = _dot(a_s[:, kb * KB : (kb + 1) * KB], wbuf[slot], 1, 0)
            total = some if total is None else total + some
            ahead, to = (t, n + NB) if n + NB < 12 else (t + 1, n + NB - 12)
            if n + NB < 12:
                load_w(t, n + NB).start()
            else:
                @pl.when(t + 1 < n_comm)
                def _(to=to):
                    load_w(t + 1, to).start()
        return total.astype(jnp.bfloat16)

    def turned(two, h):
        one = two[:, h * HEAD : (h + 1) * HEAD].astype(jnp.float32)
        return (one * cos_s[...] + pltpu.roll(one, HEAD // 2, 1) * sin_s[...]).astype(jnp.bfloat16)

    def heads(t):
        k, i = lax.div(t, NI), lax.rem(t, NI)
        lane = lambda h: pl.ds(pl.multiple_of(i * 256 + h * HEAD, HEAD), HEAD)
        q = project(t, 0)
        for h in range(2):
            q_s[h] = turned(q, h)
        kk = project(t, 1)
        for h in range(2):
            k_s[row(k), lane(h)] = turned(kk, h)
        v = project(t, 2)
        for h in range(2):
            vt_s[2 * i + h, :HEAD, row(k)] = v[:, h * HEAD : (h + 1) * HEAD].T
        for h in range(2):
            top_s[h] = jnp.full((1, R), NEG, jnp.float32)
            mix_s[h] = jnp.zeros((HEAD + 8, R), jnp.float32)

        def block(j, masked):
            here = pl.ds(pl.multiple_of(j * KEYS, KEYS), KEYS)
            scores = [_dot(k_s[here, lane(h)], q_s[h], 1, 1) for h in range(2)]
            if masked:
                gap = lax.broadcasted_iota(jnp.int32, (KEYS, R), 1) - lax.broadcasted_iota(jnp.int32, (KEYS, R), 0)
                seen = gap >= j * KEYS - k * R
                scores = [jnp.where(seen, s, HIDDEN) for s in scores]
            weights, keeps = [], []
            for h, s in enumerate(scores):
                old = top_s[h]
                top = jnp.maximum(old, s.max(axis=0, keepdims=True))
                top_s[h] = top
                weights.append(jnp.exp2((s - top) * e).astype(jnp.bfloat16))
                keeps.append(jnp.exp2((old - top) * e))
            for h in range(2):
                mix_s[h] = mix_s[h] * keeps[h] + _dot(vt_s[2 * i + h, :, here], weights[h], 1, 0)

        whole = lax.div(k * R, KEYS)

        def plain(j, carry):
            block(j, False)
            return carry

        lax.fori_loop(0, whole, plain, 0)
        block(whole, True)
        for h in range(2):
            out = mix_s[h, :HEAD, :] * (1 / mix_s[h, HEAD : HEAD + 1, :])
            s_s[lax.rem(k, 2), :, lane(h)] = out.T.astype(jnp.bfloat16)

    def term(k, i, ty):
        return _dot(s_s[lax.rem(k, 2)], wo_s[i, ty], 1, 0)

    def step(t, carry):
        c = t - NI
        k, i = lax.div(c, NI), lax.rem(c, NI)
        p = lax.rem(k, 2)
        busy = (c >= 0) & (c < n_comm)

        @pl.when(t == 2)
        def _():
            for ty in range(4):
                load_wo(0, ty).start()

        @pl.when((t >= 3) & (t < 3 + NI - 1))
        def _():
            for ty in range(4):
                load_wo(t - 2, ty).start()

        late = c - NI
        lk, li = lax.div(late, NI), lax.rem(late, NI)

        @pl.when((late >= 0) & (late < n_comm))
        def _():
            for ab in range(2):
                to_partner(lk, ab, li).wait_send()

            @pl.when(end)
            def _():
                for ab in range(2):
                    to_inner(lk, ab, li).wait_send()

            @pl.when(middle)
            def _():
                to_other(lk, li).wait_send()
                result_to_other(lk, li).wait_send()
                result_here(lk, li).wait()
                for ab in range(2):
                    src = sbuf.at[lax.rem(lk, 2), 1, li]
                    result_to_outer(lk, ab, li, src).wait_send()
                    result_to_partner(lk, ab, li, src).wait_send()

        @pl.when(busy)
        def _():
            @pl.when(c < NI)
            def _():
                for ty in range(4):
                    load_wo(i, ty).wait()

            @pl.when(middle)
            def _():
                load_res(k, i).start()

            for ab in range(2):
                obuf[ab, i] = term(k, i, ab).astype(jnp.bfloat16)
                to_partner(k, ab, i).start()

            @pl.when(end)
            def _():
                for ab in range(2):
                    mine = term(k, i, 2 + ab)
                    to_partner(k, ab, i).wait_recv()
                    sbuf[p, ab, i] = (mine + part[p, ab, i].astype(jnp.float32)).astype(jnp.bfloat16)
                    to_inner(k, ab, i).start()

        @pl.when(t < n_comm)
        def _():
            @pl.when(lax.rem(t, NI) == 0)
            def _():
                norm(lax.div(t, NI))

            heads(t)

        @pl.when(busy & middle)
        def _():
            mine = term(k, i, 2)
            to_partner(k, 0, i).wait_recv()
            to_inner(k, 0, i).wait_recv()
            sbuf[p, 0, i] = (mine + part[p, 0, i].astype(jnp.float32) + from_e[p, 0, i].astype(jnp.float32)).astype(jnp.bfloat16)
            to_other(k, i).start()

        before = c - 1
        bk, bi = lax.div(before, NI), lax.rem(before, NI)

        @pl.when((before >= 0) & (before < n_comm) & middle)
        def _():
            result_to_outer(bk, 0, bi, y_at(bk, core, 0, bi)).wait_recv()
            src = y_at(bk, core, 0, bi)
            result_to_outer(bk, 0, bi, src).start()
            result_to_partner(bk, 0, bi, src).start()

        @pl.when(busy & middle)
        def _():
            mine = term(k, i, 3)
            to_partner(k, 1, i).wait_recv()
            load_res(k, i).wait()
            mine = mine + part[p, 1, i].astype(jnp.float32)
            to_inner(k, 1, i).wait_recv()
            to_other(k, i).wait_recv()
            mine = mine + from_e[p, 1, i].astype(jnp.float32) + from_m[p, i].astype(jnp.float32)
            sbuf[p, 1, i] = (mine + xres[i].astype(jnp.float32)).astype(jnp.bfloat16)
            src = sbuf.at[p, 1, i]
            result_to_outer(k, 1, i, src).start()
            result_to_other(k, i).start()
            result_to_partner(k, 1, i, src).start()
            result_here(k, i).start()

        @pl.when((late >= 0) & (late < n_comm) & end)
        def _():
            for ab in (1, 0):
                src = y_at(lk, core, ab, li)
                result_to_outer(lk, ab, li, src).wait_recv()
                result_to_partner(lk, ab, li, src).start()

        last = late - 1
        fk, fi = lax.div(last, NI), lax.rem(last, NI)

        @pl.when(last >= 0)
        def _():
            @pl.when(end)
            def _():
                for ab in range(2):
                    result_to_partner(fk, ab, fi, y_at(fk, core, ab, fi)).wait_send()

            for ab in range(2):
                result_to_partner(fk, ab, fi, y_at(fk, 1 - core, ab, fi)).wait_recv()

        return carry

    lax.fori_loop(0, n_comm + 2 * NI + 1, step, 0)


def solution(mesh):
    def step(x, gain, wq, wk, wv, wo):
        rows, d = x.shape
        own = wq.shape[1]
        chunks = rows // R
        half = HEAD // 2
        freq = np.float32(THETA) ** (-np.arange(half, dtype=np.float32) / half)
        freq = jnp.asarray(np.concatenate([freq, freq])[None], jnp.float32)
        bf16, f32 = jnp.bfloat16, jnp.float32
        hbm = pl.BlockSpec(memory_space=pl.ANY)
        vmem = pl.BlockSpec(memory_space=pltpu.VMEM)
        dma = pltpu.SemaphoreType.DMA
        return pl.pallas_call(
            _kernel,
            out_shape=jax.ShapeDtypeStruct((rows, d), bf16),
            in_specs=[hbm, vmem, vmem, hbm, hbm, hbm, hbm],
            out_specs=hbm,
            scratch_shapes=[
                pltpu.VMEM((R, d), bf16),
                pltpu.VMEM((R, d), bf16),
                pltpu.VMEM((NB, KB, 256), bf16),
                pltpu.VMEM((NI, 4, own, PC), bf16),
                pltpu.VMEM((rows, own), bf16),
                pltpu.VMEM((own // HEAD, HEAD + 8, rows), bf16),
                pltpu.VMEM((2, R, own), bf16),
                pltpu.VMEM((2, R, HEAD), bf16),
                pltpu.VMEM((R, HEAD), f32),
                pltpu.VMEM((R, HEAD), f32),
                pltpu.VMEM((2, 1, R), f32),
                pltpu.VMEM((2, HEAD + 8, R), f32),
                pltpu.VMEM((2, 2, NI, R, PC), bf16),
                pltpu.VMEM((2, 2, NI, R, PC), bf16),
                pltpu.VMEM((2, NI, R, PC), bf16),
                pltpu.VMEM((2, NI, R, PC), bf16),
                pltpu.VMEM((2, 2, NI, R, PC), bf16),
                pltpu.VMEM((NI, R, PC), bf16),
                dma,
                dma((NB,)),
                dma((NI, 4)),
                dma((NI,)),
                dma((chunks, 2, NI)),
                dma((chunks, 2, NI)),
                dma((chunks, NI)),
                dma((chunks, 2, NI)),
                dma((chunks, 2, NI)),
                dma((2, NI)),
                dma((2, 2, NI)),
                dma((2, 2, NI)),
                dma((2, 2, NI)),
                dma((2, NI)),
            ],
            compiler_params=pltpu.CompilerParams(collective_id=1, has_side_effects=True, vmem_limit_bytes=67_000_000),
            name="layer",
        )(x, gain[None], freq, wq, wk, wv, wo)

    tokens, columns = P("dp", None), P(None, "tp")
    return jax.shard_map(
        step,
        mesh=mesh,
        in_specs=(tokens, P(None), columns, columns, columns, P("tp", None)),
        out_specs=tokens,
        check_vma=False,
    )
```

```python
import functools

import jax
import jax.numpy as jnp
import numpy as np
from jax import lax
from jax.experimental import pallas as pl
from jax.experimental.pallas import tpu as pltpu
from jax.sharding import PartitionSpec as P

HEAD = 128
THETA = 10000
NEG = -1e30
HIDDEN = 2 * NEG
LOG2E = 1.4426950408889634
R = 256
KB = 2048
PC = 256
NB = 4
XR = R // 4
KEYS = 512
NI = 4
NP = 2 * NI
MESH = pl.DeviceIdType.MESH


def _dot(a, b, ca, cb):
    return lax.dot_general(a, b, (((ca,), (cb,)), ((), ())), preferred_element_type=jnp.float32)


def _kernel(x_ref, gain_ref, freq_ref, wq_ref, wk_ref, wv_ref, wo_ref, y_ref,
            xb, gain_s, a_s, wbuf, acc_s, wo_s, k_s, vt_s, s_s, q_s, cos_s, sin_s, top_s, mix_s,
            part, from_e, from_m, obuf, sbuf, xres, away_s,
            x_sem, w_sem, wo_sem, away_sem, xr_sem, r_part, r_e, r_m, r_res, r_y, s_o, s_u, s_e, s_p, s_l):
    rows, d = x_ref.shape
    chunks = rows // R
    steps = chunks * NI
    pieces = chunks * NP
    scale = HEAD**-0.5
    e = scale * LOG2E
    tp = lax.axis_index("tp")
    z, core = lax.div(tp, 2), lax.rem(tp, 2)
    middle = (z == 1) | (z == 2)
    end = jnp.logical_not(middle)
    partner = z * 2 + 1 - core
    inner = jnp.where(z < 2, 1, 2) * 2 + core
    outer = jnp.where(z < 2, 0, 3) * 2 + core
    other = (3 - z) * 2 + core
    near = jnp.where(z < 2, 0, 1)
    half = d // 2
    quarter = d // 4

    def col(side, ab, i):
        g = near if ab == 1 else 1 - near
        return pl.multiple_of(side * half + g * quarter + i * PC, PC)

    def chunk(c):
        return lax.div(c, NP)

    def place(c):
        return chunk(c), lax.rem(c, NP)

    def row(k):
        return pl.ds(pl.multiple_of(k * R, R), R)

    def remote(src, dst, send, recv, to):
        return pltpu.make_async_remote_copy(src, dst, send, recv, device_id={"tp": to}, device_id_type=MESH)

    def is_piece(c):
        return (c >= 0) & (c < pieces)

    def load_x(b):
        slot = lax.rem(b, NI)
        return pltpu.make_async_copy(x_ref.at[pl.ds(pl.multiple_of(b * XR, XR), XR)], xb.at[slot], x_sem.at[slot])

    def load_w(t, kb, m):
        w = (wq_ref, wk_ref, wv_ref)[m]
        i = lax.rem(t, NI)
        return pltpu.make_async_copy(
            w.at[pl.ds(kb * KB, KB), pl.ds(pl.multiple_of(i * 256, 256), 256)],
            wbuf.at[kb, :, pl.ds(m * 256, 256)], w_sem.at[kb, m])

    def load_away(q, ab):
        slot = lax.rem(q, 2)
        at = pl.ds(col(1 - core, ab, 2 * lax.rem(q, NI)), 2 * PC)
        return pltpu.make_async_copy(wo_ref.at[:, at], away_s.at[slot, ab], away_sem.at[slot, ab])

    def load_wo(i, ab):
        at = pl.ds(col(core, ab, 2 * i), 2 * PC)
        return pltpu.make_async_copy(wo_ref.at[:, at], wo_s.at[i, ab], wo_sem.at[i, ab])

    def load_res(q):
        slot, i = lax.rem(q, 2), lax.rem(q, NI)
        return pltpu.make_async_copy(
            x_ref.at[row(lax.div(q, NI)), pl.ds(col(core, 1, 2 * i), 2 * PC)], xres.at[slot], xr_sem.at[slot])

    def to_partner(c, ab):
        (k, i), p = place(c), lax.rem(c, 4)
        return remote(obuf.at[ab, p], part.at[ab, lax.rem(c, 16)], s_o.at[ab, p], r_part.at[k, ab, i], partner)

    def to_inner(c, ab):
        k, i = place(c)
        return remote(sbuf.at[ab, i], from_e.at[ab, lax.rem(c, 16)], s_u.at[ab, i], r_e.at[k, ab, i], inner)

    def to_other(c):
        k, i = place(c)
        return remote(sbuf.at[0, i], from_m.at[lax.rem(c, 4)], s_u.at[0, i], r_m.at[k, i], other)

    def y_at(c, side, ab):
        k, i = place(c)
        return y_ref.at[row(k), pl.ds(col(side, ab, i), PC)]

    def result_to_other(c):
        k, i = place(c)
        return remote(sbuf.at[1, i], y_at(c, core, 1), s_u.at[1, i], r_res.at[k, 0, i], other)

    def result_to_outer(c, ab, src):
        k, i = place(c)
        return remote(src, y_at(c, core, ab), s_e.at[ab, i], r_res.at[k, ab, i], outer)

    def result_to_partner(c, ab, src, side):
        k, i = place(c)
        return remote(src, y_at(c, side, ab), s_p.at[ab, i], r_y.at[k, ab, i], partner)

    def result_here(c):
        i = lax.rem(c, NP)
        return pltpu.make_async_copy(sbuf.at[1, i], y_at(c, core, 1), s_l.at[i])

    barrier = pltpu.get_barrier_semaphore()

    def greet(to):
        pl.semaphore_signal(barrier, inc=1, device_id={"tp": to}, device_id_type=MESH)

    for b in range(NI):
        load_x(b).start()
    for kb in range(NB):
        for m in range(3):
            load_w(0, kb, m).start()
    greet(partner)

    @pl.when(end)
    def _():
        greet(inner)

    @pl.when(middle)
    def _():
        greet(outer)
        greet(other)

    gain_s[...] = jnp.broadcast_to(gain_ref[...].astype(jnp.float32), gain_s.shape)

    def clear(h, carry):
        vt_s[h, :HEAD, :] = jnp.zeros((HEAD, rows), jnp.bfloat16)
        vt_s[h, HEAD:, :] = jnp.ones((8, rows), jnp.bfloat16)
        return carry

    lax.fori_loop(0, 2 * NI, clear, 0)

    def norm(b):
        k, at = lax.rem(lax.div(b, NI), 2), lax.rem(b, NI) * XR
        load_x(b).wait()
        slot = lax.rem(b, NI)
        sizes = []
        for g in range(XR // 16):
            wide = xb[slot, g * 16 : g * 16 + 16, :].astype(jnp.float32)
            sizes.append(lax.rsqrt(jnp.mean(wide * wide, -1, keepdims=True) + 1e-6))
        for g, size in enumerate(sizes):
            wide = xb[slot, g * 16 : g * 16 + 16, :].astype(jnp.float32) * size
            wide = wide.reshape(2, 8, d) * gain_s[...][None]
            a_s[k, pl.ds(pl.multiple_of(at + g * 16, 16), 16), :] = wide.reshape(16, d).astype(jnp.bfloat16)

        @pl.when(b + NI < steps)
        def _():
            load_x(b + NI).start()

        token = (b * XR + lax.broadcasted_iota(jnp.int32, (XR, HEAD), 0)).astype(jnp.float32)
        angle = token * freq_ref[...]
        sign = jnp.where(lax.broadcasted_iota(jnp.int32, (XR, HEAD), 1) < HEAD // 2, -1.0, 1.0)
        here = pl.ds(pl.multiple_of(at, XR), XR)
        cos_s[k, here, :] = jnp.cos(angle)
        sin_s[k, here, :] = jnp.sin(angle) * sign

    def project(t):
        k, i = lax.div(t, NI), lax.rem(t, NI)
        p = lax.rem(k, 2)
        lane = lambda h: pl.ds(pl.multiple_of(i * 256 + h * HEAD, HEAD), HEAD)
        for pair in range(2):
            for kb in (2 * pair, 2 * pair + 1):
                for m in range(3):
                    load_w(t, kb, m).wait()
            for kb in (2 * pair, 2 * pair + 1):
                some = _dot(a_s[p, :, kb * KB : (kb + 1) * KB], wbuf[kb], 1, 0)
                acc_s[...] = some if kb == 0 else acc_s[...] + some

            @pl.when(t + 1 < steps)
            def _(pair=pair):
                for kb in (2 * pair, 2 * pair + 1):
                    for m in range(3):
                        load_w(t + 1, kb, m).start()

        def turned(at):
            one = acc_s[:, at : at + HEAD].astype(jnp.bfloat16).astype(jnp.float32)
            return (one * cos_s[p] + pltpu.roll(one, HEAD // 2, 1) * sin_s[p]).astype(jnp.bfloat16)

        for h in range(2):
            q_s[h] = turned(h * HEAD)
            k_s[row(k), lane(h)] = turned(256 + h * HEAD)
            vt_s[2 * i + h, :HEAD, row(k)] = acc_s[:, 512 + h * HEAD : 512 + (h + 1) * HEAD].astype(jnp.bfloat16).T

    def attend(t):
        k, i = lax.div(t, NI), lax.rem(t, NI)
        lane = lambda h: pl.ds(pl.multiple_of(i * 256 + h * HEAD, HEAD), HEAD)
        for h in range(2):
            top_s[h] = jnp.full((1, R), NEG, jnp.float32)
            mix_s[h] = jnp.zeros((HEAD + 8, R), jnp.float32)

        def block(j, masked):
            here = pl.ds(pl.multiple_of(j * KEYS, KEYS), KEYS)
            scores = [_dot(k_s[here, lane(h)], q_s[h], 1, 1) for h in range(2)]
            if masked:
                gap = lax.broadcasted_iota(jnp.int32, (KEYS, R), 1) - lax.broadcasted_iota(jnp.int32, (KEYS, R), 0)
                seen = gap >= j * KEYS - k * R
                scores = [jnp.where(seen, s, HIDDEN) for s in scores]
            weights, keeps = [], []
            for h, s in enumerate(scores):
                old = top_s[h]
                top = jnp.maximum(old, s.max(axis=0, keepdims=True))
                top_s[h] = top
                weights.append(jnp.exp2((s - top) * e).astype(jnp.bfloat16))
                keeps.append(jnp.exp2((old - top) * e))
            for h in range(2):
                mix_s[h] = mix_s[h] * keeps[h] + _dot(vt_s[2 * i + h, :, here], weights[h], 1, 0)

        whole = lax.div(k * R, KEYS)

        def plain(j, carry):
            block(j, False)
            return carry

        lax.fori_loop(0, whole, plain, 0)
        block(whole, True)
        for h in range(2):
            out = mix_s[h, :HEAD, :] * (1 / mix_s[h, HEAD : HEAD + 1, :])
            s_s[lax.rem(k, 3), :, lane(h)] = out.T.astype(jnp.bfloat16)

    def mine(k):
        return s_s[lax.rem(k, 3)]

    def send_away(q):
        with jax.named_scope("away"):
            for ab in range(2):
                load_away(q, ab).wait()
            terms = [_dot(mine(lax.div(q, NI)), away_s[lax.rem(q, 2), ab], 1, 0) for ab in range(2)]
            for ab in range(2):
                for u in range(2):
                    obuf[ab, lax.rem(2 * q + u, 4)] = terms[ab][:, u * PC : (u + 1) * PC].astype(jnp.bfloat16)
            for u in range(2):
                for ab in range(2):
                    to_partner(2 * q + u, ab).start()

    def end_sum(q):
        with jax.named_scope("end_sum"):
            i = lax.rem(q, NI)

            @pl.when(q < NI)
            def _():
                for ab in range(2):
                    load_wo(q, ab).wait()

            for ab in range(2):
                term = _dot(mine(lax.div(q, NI)), wo_s[i, ab], 1, 0)
                for u in range(2):
                    c = 2 * q + u
                    to_partner(c, ab).wait_recv()
                    some = term[:, u * PC : (u + 1) * PC] + part[ab, lax.rem(c, 16)].astype(jnp.float32)
                    sbuf[ab, lax.rem(c, NP)] = some.astype(jnp.bfloat16)
                if ab == 0:
                    to_inner(2 * q, 0).start()

                    @pl.when(q > 0)
                    def _():
                        to_inner(2 * q - 1, 1).start()

                    to_inner(2 * q + 1, 0).start()
                else:
                    to_inner(2 * q, 1).start()

    def middle_pass(c, u):
        k, i = place(c)
        q, at = lax.div(c, 2), lax.rem(c, 16)
        with jax.named_scope("pass_w"):
            if u == 0:
                @pl.when(q < NI)
                def _():
                    load_wo(q, 0).wait()

            to_partner(c, 0).wait_recv()
            to_inner(c, 0).wait_recv()
        with jax.named_scope("pass"):
            term = _dot(mine(k), wo_s[lax.rem(q, NI), 0, :, u * PC : (u + 1) * PC], 1, 0)
            term = term + part[0, at].astype(jnp.float32) + from_e[0, at].astype(jnp.float32)
            sbuf[0, i] = term.astype(jnp.bfloat16)
            to_other(c).start()

    def middle_finish(c, u):
        k, i = place(c)
        q, at = lax.div(c, 2), lax.rem(c, 16)
        with jax.named_scope("finish_w"):
            if u == 0:
                @pl.when(q < NI)
                def _():
                    load_wo(q, 1).wait()

                load_res(q).wait()
            to_partner(c, 1).wait_recv()
            to_inner(c, 1).wait_recv()
            to_other(c).wait_recv()
        with jax.named_scope("finish"):
            term = _dot(mine(k), wo_s[lax.rem(q, NI), 1, :, u * PC : (u + 1) * PC], 1, 0)
            term = term + part[1, at].astype(jnp.float32)
            term = term + from_e[1, at].astype(jnp.float32) + from_m[lax.rem(c, 4)].astype(jnp.float32)
            term = term + xres[lax.rem(q, 2), :, u * PC : (u + 1) * PC].astype(jnp.float32)
            sbuf[1, i] = term.astype(jnp.bfloat16)
            src = sbuf.at[1, i]
            result_to_outer(c, 1, src).start()
            result_to_other(c).start()
            result_to_partner(c, 1, src, core).start()
            result_here(c).start()

    def middle_forward(c):
        src = y_at(c, core, 0)
        with jax.named_scope("forward_w"):
            result_to_outer(c, 0, src).wait_recv()
        result_to_outer(c, 0, src).start()
        result_to_partner(c, 0, src, core).start()

    def middle_turn(s, u):
        @pl.when(is_piece(s - 10) & middle)
        def _():
            middle_finish(s - 10, u)

        @pl.when(is_piece(s - 11) & middle)
        def _():
            middle_forward(s - 11)

        @pl.when(is_piece(s - 8) & middle)
        def _():
            middle_pass(s - 8, u)

    def step(t, carry):
        def is_pair(q):
            return (q >= 0) & (q < steps)

        @pl.when(is_pair(t - 8) & middle)
        def _():
            for u in range(2):
                to_other(2 * (t - 8) + u).wait_send()

        @pl.when(is_pair(t - 9) & middle)
        def _():
            for u in range(2):
                c = 2 * (t - 9) + u
                result_to_other(c).wait_send()
                result_to_outer(c, 1, sbuf.at[1, 0]).wait_send()
                result_to_partner(c, 1, sbuf.at[1, 0], core).wait_send()
                result_here(c).wait()

        for c in (2 * t - 19, 2 * t - 18):
            @pl.when(is_piece(c) & middle)
            def _(c=c):
                src = y_at(c, core, 0)
                result_to_outer(c, 0, src).wait_send()
                result_to_partner(c, 0, src, core).wait_send()

        @pl.when((t >= 2) & (t - 2 < steps))
        def _():
            for ab in range(2):
                load_away(t - 2, ab).start()

        @pl.when((t >= 2) & (t < 2 + NI))
        def _():
            for ab in range(2):
                load_wo(t - 2, ab).start()

        @pl.when(t < steps)
        def _():
            with jax.named_scope("project"):
                project(t)

        middle_turn(2 * t, 0)

        @pl.when(t + NI < steps)
        def _():
            with jax.named_scope("norm"):
                norm(t + NI)

        @pl.when(t < steps)
        def _():
            with jax.named_scope("attend"):
                attend(t)

        @pl.when(is_pair(t - 5))
        def _():
            for u in range(2):
                for ab in range(2):
                    to_partner(2 * (t - 5) + u, ab).wait_send()

        @pl.when(is_pair(t - 3))
        def _():
            send_away(t - 3)

        @pl.when(is_pair(t - 7) & end)
        def _():
            for u in range(2):
                for ab in range(2):
                    to_inner(2 * (t - 7) + u, ab).wait_send()

        @pl.when(is_pair(t - 3) & end)
        def _():
            end_sum(t - 3)

        @pl.when((t - 3 == steps) & end)
        def _():
            to_inner(pieces - 1, 1).start()

        middle_turn(2 * t + 1, 1)

        @pl.when(is_pair(t - 4) & middle)
        def _():
            load_res(t - 4).start()

        @pl.when(is_pair(t - 8) & end)
        def _():
            for u in range(2):
                for ab in (1, 0):
                    c = 2 * (t - 8) + u
                    src = y_at(c, core, ab)
                    with jax.named_scope("result_w"):
                        result_to_outer(c, ab, src).wait_recv()
                    result_to_partner(c, ab, src, core).start()

        @pl.when(is_pair(t - 9) & end)
        def _():
            for u in range(2):
                for ab in range(2):
                    c = 2 * (t - 9) + u
                    result_to_partner(c, ab, y_at(c, core, ab), core).wait_send()

        @pl.when(is_pair(t - 9))
        def _():
            with jax.named_scope("y_w"):
                for u in range(2):
                    for ab in range(2):
                        c = 2 * (t - 9) + u
                        result_to_partner(c, ab, y_at(c, core, ab), 1 - core).wait_recv()

        return carry

    with jax.named_scope("norm0"):
        def first(b, carry):
            norm(b)
            return carry

        lax.fori_loop(0, NI, first, 0)

    with jax.named_scope("barrier"):
        @pl.when(end)
        def _():
            pl.semaphore_wait(barrier, 2)

        @pl.when(middle)
        def _():
            pl.semaphore_wait(barrier, 3)

    lax.fori_loop(0, steps + 10, step, 0)


def solution(mesh):
    def step(x, gain, wq, wk, wv, wo):
        rows, d = x.shape
        own = wq.shape[1]
        chunks = rows // R
        half = HEAD // 2
        freq = np.float32(THETA) ** (-np.arange(half, dtype=np.float32) / half)
        freq = jnp.asarray(np.concatenate([freq, freq])[None], jnp.float32)
        bf16, f32 = jnp.bfloat16, jnp.float32
        hbm = pl.BlockSpec(memory_space=pl.ANY)
        vmem = pl.BlockSpec(memory_space=pltpu.VMEM)
        dma = pltpu.SemaphoreType.DMA
        return pl.pallas_call(
            _kernel,
            out_shape=jax.ShapeDtypeStruct((rows, d), bf16),
            in_specs=[hbm, vmem, vmem, hbm, hbm, hbm, hbm],
            out_specs=hbm,
            scratch_shapes=[
                pltpu.VMEM((NI, XR, d), bf16),
                pltpu.VMEM((8, d), f32),
                pltpu.VMEM((2, R, d), bf16),
                pltpu.VMEM((NB, KB, 768), bf16),
                pltpu.VMEM((R, 768), f32),
                pltpu.VMEM((NI, 2, own, 2 * PC), bf16),
                pltpu.VMEM((rows, own), bf16),
                pltpu.VMEM((own // HEAD, HEAD + 8, rows), bf16),
                pltpu.VMEM((3, R, own), bf16),
                pltpu.VMEM((2, R, HEAD), bf16),
                pltpu.VMEM((2, R, HEAD), f32),
                pltpu.VMEM((2, R, HEAD), f32),
                pltpu.VMEM((2, 1, R), f32),
                pltpu.VMEM((2, HEAD + 8, R), f32),
                pltpu.VMEM((2, 16, R, PC), bf16),
                pltpu.VMEM((2, 16, R, PC), bf16),
                pltpu.VMEM((4, R, PC), bf16),
                pltpu.VMEM((2, 4, R, PC), bf16),
                pltpu.VMEM((2, NP, R, PC), bf16),
                pltpu.VMEM((2, R, 2 * PC), bf16),
                pltpu.VMEM((2, 2, own, 2 * PC), bf16),
                dma((NI,)),
                dma((NB, 3)),
                dma((NI, 2)),
                dma((2, 2)),
                dma((2,)),
                dma((chunks, 2, NP)),
                dma((chunks, 2, NP)),
                dma((chunks, NP)),
                dma((chunks, 2, NP)),
                dma((chunks, 2, NP)),
                dma((2, 4)),
                dma((2, NP)),
                dma((2, NP)),
                dma((2, NP)),
                dma((NP,)),
            ],
            compiler_params=pltpu.CompilerParams(collective_id=1, has_side_effects=True, vmem_limit_bytes=67_000_000),
            name="layer",
        )(x, gain[None], freq, wq, wk, wv, wo)

    tokens, columns = P("dp", None), P(None, "tp")
    return jax.shard_map(
        step,
        mesh=mesh,
        in_specs=(tokens, P(None), columns, columns, columns, P("tp", None)),
        out_specs=tokens,
        check_vma=False,
    )
```

```python
import functools

import jax
import jax.numpy as jnp
import numpy as np
from jax import lax
from jax.experimental import pallas as pl
from jax.experimental.pallas import tpu as pltpu
from jax.sharding import PartitionSpec as P

HEAD = 128
THETA = 10000
NEG = -1e30
HIDDEN = 2 * NEG
LOG2E = 1.4426950408889634
R = 256
KB = 2048
PC = 256
NB = 4
XR = R // 4
KEYS = 512
NI = 4
NP = 2 * NI
RING = 16
MESH = pl.DeviceIdType.MESH


def _dot(a, b, ca, cb):
    return lax.dot_general(a, b, (((ca,), (cb,)), ((), ())), preferred_element_type=jnp.float32)


def _kernel(x_ref, gain_ref, freq_ref, wq_ref, wk_ref, wv_ref, wo_ref, y_ref,
            xb, gain_s, a_s, stage_s, wbuf, acc_s, wo_s, k_s, vt_s, s_s, q_s, turns_s, cos_s, sin_s, top_s, mix_s,
            part, from_e, from_m, obuf, sbuf, xres, away_s,
            x_sem, w_sem, wo_sem, away_sem, xr_sem, r_part, r_e, r_m, r_res, r_y, s_o, s_u, s_e, s_p, s_l):
    rows, d = x_ref.shape
    chunks = rows // R
    steps = chunks * NI
    pieces = chunks * NP
    scale = HEAD**-0.5
    e = scale * LOG2E
    tp = lax.axis_index("tp")
    z, core = lax.div(tp, 2), lax.rem(tp, 2)
    middle = (z == 1) | (z == 2)
    end = jnp.logical_not(middle)
    partner = z * 2 + 1 - core
    inner = jnp.where(z < 2, 1, 2) * 2 + core
    outer = jnp.where(z < 2, 0, 3) * 2 + core
    other = (3 - z) * 2 + core
    near = jnp.where(z < 2, 0, 1)
    half = d // 2
    quarter = d // 4

    def col(side, ab, i):
        g = near if ab == 1 else 1 - near
        return pl.multiple_of(side * half + g * quarter + i * PC, PC)

    def chunk(c):
        return lax.div(c, NP)

    def place(c):
        return chunk(c), lax.rem(c, NP)

    def ring(c):
        return lax.rem(c, RING)

    def row(k):
        return pl.ds(pl.multiple_of(k * R, R), R)

    def remote(src, dst, send, recv, to):
        return pltpu.make_async_remote_copy(src, dst, send, recv, device_id={"tp": to}, device_id_type=MESH)

    def is_piece(c):
        return (c >= 0) & (c < pieces)

    def load_x(b):
        slot = lax.rem(b, NI)
        return pltpu.make_async_copy(x_ref.at[pl.ds(pl.multiple_of(b * XR, XR), XR)], xb.at[slot], x_sem.at[slot])

    def load_w(t, kb, m):
        w = (wq_ref, wk_ref, wv_ref)[m]
        i = lax.rem(t, NI)
        return pltpu.make_async_copy(
            w.at[pl.ds(kb * KB, KB), pl.ds(pl.multiple_of(i * 256, 256), 256)],
            wbuf.at[kb, :, pl.ds(m * 256, 256)], w_sem.at[kb, m])

    def load_away(q, ab):
        slot = lax.rem(q, 2)
        at = pl.ds(col(1 - core, ab, 2 * lax.rem(q, NI)), 2 * PC)
        return pltpu.make_async_copy(wo_ref.at[:, at], away_s.at[slot, ab], away_sem.at[slot, ab])

    def load_wo(i, ab):
        at = pl.ds(col(core, ab, 2 * i), 2 * PC)
        return pltpu.make_async_copy(wo_ref.at[:, at], wo_s.at[i, ab], wo_sem.at[i, ab])

    def load_res(q):
        slot, i = lax.rem(q, 2), lax.rem(q, NI)
        return pltpu.make_async_copy(
            x_ref.at[row(lax.div(q, NI)), pl.ds(col(core, 1, 2 * i), 2 * PC)], xres.at[slot], xr_sem.at[slot])

    def to_partner(c, ab):
        p = lax.rem(c, 4)
        return remote(obuf.at[ab, p], part.at[ab, ring(c)], s_o.at[ab, p], r_part.at[ab, ring(c)], partner)

    def to_inner(c, ab):
        k, i = place(c)
        return remote(sbuf.at[ab, i], from_e.at[ab, ring(c)], s_u.at[ab, i], r_e.at[ab, ring(c)], inner)

    def to_other(c):
        k, i = place(c)
        return remote(sbuf.at[0, i], from_m.at[lax.rem(c, 4)], s_u.at[0, i], r_m.at[lax.rem(c, 4)], other)

    def y_at(c, side, ab):
        k, i = place(c)
        return y_ref.at[row(k), pl.ds(col(side, ab, i), PC)]

    def result_to_other(c):
        k, i = place(c)
        return remote(sbuf.at[1, i], y_at(c, core, 1), s_u.at[1, i], r_res.at[0, ring(c)], other)

    def result_to_outer(c, ab, src):
        k, i = place(c)
        return remote(src, y_at(c, core, ab), s_e.at[ab, i], r_res.at[ab, ring(c)], outer)

    def result_to_partner(c, ab, src, side):
        k, i = place(c)
        return remote(src, y_at(c, side, ab), s_p.at[ab, i], r_y.at[ab, ring(c)], partner)

    def result_here(c):
        i = lax.rem(c, NP)
        return pltpu.make_async_copy(sbuf.at[1, i], y_at(c, core, 1), s_l.at[i])

    barrier = pltpu.get_barrier_semaphore()

    def greet(to):
        pl.semaphore_signal(barrier, inc=1, device_id={"tp": to}, device_id_type=MESH)

    for b in range(NI):
        load_x(b).start()
    greet(partner)

    @pl.when(end)
    def _():
        greet(inner)

    @pl.when(middle)
    def _():
        greet(outer)
        greet(other)

    gain_s[...] = jnp.broadcast_to(gain_ref[...].astype(jnp.float32)[None], gain_s.shape)

    for h in range(2 * NI):
        vt_s[h, HEAD:, :] = jnp.ones((8, rows), jnp.bfloat16)
    for kb in range(2):
        for m in range(3):
            load_w(0, kb, m).start()

    def norm(b, to, top):
        slot = lax.rem(b, NI)
        sizes = []
        for g in range(XR // 16):
            wide = xb[slot, g * 16 : g * 16 + 16, :].astype(jnp.float32)
            sizes.append(lax.rsqrt(jnp.mean(wide * wide, -1, keepdims=True) + 1e-6))
        for g, size in enumerate(sizes):
            wide = xb[slot, g * 16 : g * 16 + 16, :].astype(jnp.float32) * size
            wide = wide.reshape(2, 8, d) * gain_s[...][None]
            to[pl.ds(pl.multiple_of(top + g * 16, 16), 16), :] = wide.reshape(16, d).astype(jnp.bfloat16)
        angles(b)

    sign = jnp.where(lax.broadcasted_iota(jnp.int32, (8, HEAD), 1) < HEAD // 2, -1.0, 1.0)

    def angles(b):
        k, i = lax.div(b, NI), lax.rem(b, NI)
        here = pl.ds(pl.multiple_of(i * XR, XR), XR)
        angle = jnp.full((8, HEAD), k * R, jnp.int32).astype(jnp.float32) * freq_ref[...]
        c, s = jnp.cos(angle)[:1], (jnp.sin(angle) * sign)[:1]
        cos, sin = turns_s[0, here, :], turns_s[1, here, :]
        cos_s[lax.rem(k, 2), here, :] = cos * c - sin * s
        sin_s[lax.rem(k, 2), here, :] = sin * c + cos * s

    def first_angles():
        token = lax.broadcasted_iota(jnp.int32, (R, HEAD), 0).astype(jnp.float32)
        angle = token * freq_ref[...]
        turns_s[0] = jnp.cos(angle)
        turns_s[1] = jnp.sin(angle) * jnp.concatenate([sign] * (R // 8), axis=0)

    def more_x(b):
        @pl.when(b < steps)
        def _():
            load_x(b).start()

    def project(t, part, ahead):
        p = lax.rem(lax.div(t, NI), 2)
        blocks = (2 * part, 2 * part + 1)
        for kb in blocks:
            for m in range(3):
                load_w(t, kb, m).wait()
        if ahead:
            load_x(t + NI).wait()
            norm(t + NI, stage_s, 0)
        for kb in blocks:
            some = _dot(a_s[p, :, kb * KB : (kb + 1) * KB], wbuf[kb], 1, 0)
            acc_s[...] = some if kb == 0 else acc_s[...] + some
        if ahead:
            k, at = lax.rem(lax.div(t + NI, NI), 2), lax.rem(t, NI) * XR
            a_s[k, pl.ds(pl.multiple_of(at, XR), XR), :] = stage_s[...]
            more_x(t + 2 * NI)

        @pl.when(t + 1 < steps)
        def _():
            for kb in blocks:
                for m in range(3):
                    load_w(t + 1, kb, m).start()

    def rotate(t):
        k, i = lax.div(t, NI), lax.rem(t, NI)
        p = lax.rem(k, 2)
        lane = lambda h: pl.ds(pl.multiple_of(i * 256 + h * HEAD, HEAD), HEAD)

        def turned(at):
            one = acc_s[:, at : at + HEAD].astype(jnp.bfloat16).astype(jnp.float32)
            return (one * cos_s[p] + pltpu.roll(one, HEAD // 2, 1) * sin_s[p]).astype(jnp.bfloat16)

        for h in range(2):
            q_s[h] = turned(h * HEAD)
            k_s[row(k), lane(h)] = turned(256 + h * HEAD)
            vt_s[2 * i + h, :HEAD, row(k)] = acc_s[:, 512 + h * HEAD : 512 + (h + 1) * HEAD].astype(jnp.bfloat16).T

    def attend(t):
        k, i = lax.div(t, NI), lax.rem(t, NI)
        lane = lambda h: pl.ds(pl.multiple_of(i * 256 + h * HEAD, HEAD), HEAD)
        for h in range(2):
            top_s[h] = jnp.full((1, R), NEG, jnp.float32)
            mix_s[h] = jnp.zeros((HEAD + 8, R), jnp.float32)

        def block(first, keys, masked):
            here = pl.ds(pl.multiple_of(first, keys), keys)
            scores = [_dot(k_s[here, lane(h)], q_s[h], 1, 1) for h in range(2)]
            if masked:
                gap = lax.broadcasted_iota(jnp.int32, (keys, R), 1) - lax.broadcasted_iota(jnp.int32, (keys, R), 0)
                seen = gap >= first - k * R
                scores = [jnp.where(seen, s, HIDDEN) for s in scores]
            weights, keeps = [], []
            for h, s in enumerate(scores):
                old = top_s[h]
                top = jnp.maximum(old, s.max(axis=0, keepdims=True))
                top_s[h] = top
                weights.append(jnp.exp2((s - top) * e).astype(jnp.bfloat16))
                keeps.append(jnp.exp2((old - top) * e))
            for h in range(2):
                mix_s[h] = mix_s[h] * keeps[h] + _dot(vt_s[2 * i + h, :, here], weights[h], 1, 0)

        whole = lax.div(k * R, KEYS)

        def plain(j, carry):
            block(j * KEYS, KEYS, False)
            return carry

        lax.fori_loop(0, whole, plain, 0)

        @pl.when(lax.rem(k, 2) == 1)
        def _():
            block(whole * KEYS, KEYS, True)

        @pl.when(lax.rem(k, 2) == 0)
        def _():
            block(k * R, R, True)

        for h in range(2):
            out = mix_s[h, :HEAD, :] * (1 / mix_s[h, HEAD : HEAD + 1, :])
            s_s[lax.rem(k, 3), :, lane(h)] = out.T.astype(jnp.bfloat16)

    def mine(k):
        return s_s[lax.rem(k, 3)]

    def send_away(q):
        with jax.named_scope("away"):
            @pl.when(q >= 2)
            def _():
                away_sent(q - 2)

            for ab in range(2):
                load_away(q, ab).wait()
                term = _dot(mine(lax.div(q, NI)), away_s[lax.rem(q, 2), ab], 1, 0)
                for u in range(2):
                    obuf[ab, lax.rem(2 * q + u, 4)] = term[:, u * PC : (u + 1) * PC].astype(jnp.bfloat16)
                for u in range(2):
                    to_partner(2 * q + u, ab).start()

            @pl.when(q + 2 < steps)
            def _():
                for ab in range(2):
                    load_away(q + 2, ab).start()

    def away_sent(q):
        for u in range(2):
            for ab in range(2):
                to_partner(2 * q + u, ab).wait_send()

    def end_sent(q):
        for u in range(2):
            for ab in range(2):
                to_inner(2 * q + u, ab).wait_send()

    def end_sum(q):
        with jax.named_scope("end_sum"):
            i = lax.rem(q, NI)

            @pl.when(q < NI)
            def _():
                for ab in range(2):
                    load_wo(q, ab).wait()

            @pl.when(q >= NI)
            def _():
                end_sent(q - NI)

            for ab in range(2):
                term = _dot(mine(lax.div(q, NI)), wo_s[i, ab], 1, 0)
                for u in range(2):
                    c = 2 * q + u
                    to_partner(c, ab).wait_recv()
                    some = term[:, u * PC : (u + 1) * PC] + part[ab, ring(c)].astype(jnp.float32)
                    sbuf[ab, lax.rem(c, NP)] = some.astype(jnp.bfloat16)
                if ab == 0:
                    to_inner(2 * q, 0).start()

                    @pl.when(q > 0)
                    def _():
                        to_inner(2 * q - 1, 1).start()

                    to_inner(2 * q + 1, 0).start()
                else:
                    to_inner(2 * q, 1).start()

                    @pl.when(q == steps - 1)
                    def _():
                        to_inner(2 * q + 1, 1).start()

    def middle_pass(c, u):
        k, i = place(c)
        q, at = lax.div(c, 2), ring(c)
        with jax.named_scope("pass_w"):
            if u == 0:
                @pl.when(q < NI)
                def _():
                    load_wo(q, 0).wait()

            to_partner(c, 0).wait_recv()
            to_inner(c, 0).wait_recv()
        with jax.named_scope("pass"):
            term = _dot(mine(k), wo_s[lax.rem(q, NI), 0, :, u * PC : (u + 1) * PC], 1, 0)
            term = term + part[0, at].astype(jnp.float32) + from_e[0, at].astype(jnp.float32)
            sbuf[0, i] = term.astype(jnp.bfloat16)
            to_other(c).start()

    def middle_finish(c, u):
        k, i = place(c)
        q, at = lax.div(c, 2), ring(c)
        with jax.named_scope("finish_w"):
            if u == 0:
                @pl.when(q < NI)
                def _():
                    load_wo(q, 1).wait()

                load_res(q).wait()
            to_partner(c, 1).wait_recv()
            to_inner(c, 1).wait_recv()
            to_other(c).wait_recv()
        with jax.named_scope("finish"):
            term = _dot(mine(k), wo_s[lax.rem(q, NI), 1, :, u * PC : (u + 1) * PC], 1, 0)
            term = term + part[1, at].astype(jnp.float32)
            term = term + from_e[1, at].astype(jnp.float32) + from_m[lax.rem(c, 4)].astype(jnp.float32)
            term = term + xres[lax.rem(q, 2), :, u * PC : (u + 1) * PC].astype(jnp.float32)
            sbuf[1, i] = term.astype(jnp.bfloat16)
            src = sbuf.at[1, i]
            result_to_outer(c, 1, src).start()
            result_to_other(c).start()
            result_to_partner(c, 1, src, core).start()
            result_here(c).start()

    def middle_forward(c):
        src = y_at(c, core, 0)
        with jax.named_scope("forward_w"):
            result_to_outer(c, 0, src).wait_recv()
        result_to_outer(c, 0, src).start()
        result_to_partner(c, 0, src, core).start()

    def middle_turn(s, u):
        @pl.when(is_piece(s - 8) & (s > 8) & middle)
        def _():
            middle_pass(s - 8, u)

        @pl.when(is_piece(s - 9) & middle)
        def _():
            middle_finish(s - 9, 1 - u)

    def norms(first, k):
        def one(i, carry):
            b = first + i
            with jax.named_scope("x_w"):
                load_x(b).wait()
            slot = lax.rem(b, NI)

            def squares(j, total):
                at = pl.ds(pl.multiple_of(j * 1024, 1024), 1024)
                for g in range(XR // 16):
                    wide = xb[slot, g * 16 : g * 16 + 16, at].astype(jnp.float32)
                    wide = wide * wide
                    some = wide[:, :HEAD]
                    for n in range(1, 8):
                        some = some + wide[:, n * HEAD : (n + 1) * HEAD]
                    total = total[:g] + (total[g] + some,) + total[g + 1 :]
                return total

            total = lax.fori_loop(0, d // 1024, squares, (jnp.zeros((16, HEAD), jnp.float32),) * (XR // 16))
            sizes = [lax.rsqrt(jnp.sum(v, -1, keepdims=True) / d + 1e-6) for v in total]
            sizes = tuple(jnp.broadcast_to(v, (16, HEAD)) for v in sizes)

            def scaled(j, sizes):
                at = pl.ds(pl.multiple_of(j * 1024, 1024), 1024)
                for g in range(XR // 16):
                    wide = xb[slot, g * 16 : g * 16 + 16, at].astype(jnp.float32)
                    wide = wide * jnp.concatenate([sizes[g]] * 8, axis=1)
                    wide = wide.reshape(2, 8, 1024) * gain_s[:, at][None]
                    a_s[k, pl.ds(pl.multiple_of(i * XR + g * 16, 16), 16), at] = wide.reshape(16, 1024).astype(jnp.bfloat16)
                return sizes

            lax.fori_loop(0, d // 1024, scaled, sizes)
            angles(b)
            if k == 0:
                @pl.when(b == 1)
                def _():
                    for kb in (2, 3):
                        for m in range(3):
                            load_w(0, kb, m).start()
            else:
                more_x(b + NI)
            return carry

        lax.fori_loop(0, NI, one, 0)

    def step(t, carry):
        def is_pair(q):
            return (q >= 0) & (q < steps)

        @pl.when(is_pair(t - 8) & middle)
        def _():
            for u in range(2):
                to_other(2 * (t - 8) + u).wait_send()

        for c in (2 * t - 17, 2 * t - 16):
            @pl.when(is_piece(c) & middle)
            def _(c=c):
                result_to_other(c).wait_send()
                result_to_outer(c, 1, sbuf.at[1, 0]).wait_send()
                result_to_partner(c, 1, sbuf.at[1, 0], core).wait_send()
                result_here(c).wait()

        for c in (2 * t - 19, 2 * t - 18):
            @pl.when(is_piece(c) & middle)
            def _(c=c):
                src = y_at(c, core, 0)
                result_to_outer(c, 0, src).wait_send()
                result_to_partner(c, 0, src, core).wait_send()

        @pl.when(t == 2)
        def _():
            for ab in range(2):
                load_away(0, ab).start()

        @pl.when((t >= 2) & (t < 2 + NI))
        def _():
            for ab in range(2):
                load_wo(t - 2, ab).start()

        @pl.when(t == 3)
        def _():
            for ab in range(2):
                load_away(1, ab).start()

        ahead = (t >= NI) & (t + NI < steps)

        @pl.when(ahead)
        def _():
            with jax.named_scope("project0"):
                project(t, 0, True)

        @pl.when(jnp.logical_not(ahead) & (t < steps))
        def _():
            with jax.named_scope("project0_"):
                project(t, 0, False)

        @pl.when(t == NI - 1)
        def _():
            for b in range(NI, 2 * NI):
                load_x(b).start()

        @pl.when(is_piece(2 * t - 11) & middle)
        def _():
            middle_forward(2 * t - 11)

        @pl.when((t == NI) & middle)
        def _():
            middle_pass(t - NI, 0)

        @pl.when(t < steps)
        def _():
            with jax.named_scope("project1"):
                project(t, 1, False)

        middle_turn(2 * t, 0)

        @pl.when(t < steps)
        def _():
            with jax.named_scope("rotate"):
                rotate(t)
            with jax.named_scope("attend"):
                attend(t)

        i = lax.rem(t, NI)

        @pl.when(is_pair(t - 3) & (i == NI - 1))
        def _():
            send_away(t - 3)

            @pl.when(end)
            def _():
                end_sum(t - 3)

        @pl.when(is_pair(t - 2) & (i != NI - 2))
        def _():
            send_away(t - 2)

            @pl.when(end)
            def _():
                end_sum(t - 2)

        @pl.when(t == NI - 1)
        def _():
            with jax.named_scope("norm1"):
                norms(NI, 1)

        @pl.when(is_piece(2 * t - 10) & middle)
        def _():
            middle_forward(2 * t - 10)

        middle_turn(2 * t + 1, 1)

        @pl.when(is_pair(t - 3) & middle)
        def _():
            load_res(t - 3).start()

        @pl.when(is_pair(t - 8) & end)
        def _():
            for u in range(2):
                for ab in (1, 0):
                    c = 2 * (t - 8) + u
                    src = y_at(c, core, ab)
                    with jax.named_scope("result_w"):
                        result_to_outer(c, ab, src).wait_recv()
                    result_to_partner(c, ab, src, core).start()

        @pl.when(is_pair(t - 9) & end)
        def _():
            for u in range(2):
                for ab in range(2):
                    c = 2 * (t - 9) + u
                    result_to_partner(c, ab, y_at(c, core, ab), core).wait_send()

        @pl.when(is_pair(t - 9))
        def _():
            with jax.named_scope("y_w"):
                for u in range(2):
                    for ab in range(2):
                        c = 2 * (t - 9) + u
                        result_to_partner(c, ab, y_at(c, core, ab), 1 - core).wait_recv()

        return carry

    with jax.named_scope("angles"):
        first_angles()
    with jax.named_scope("norm0"):
        norms(0, 0)

    with jax.named_scope("barrier"):
        @pl.when(end)
        def _():
            pl.semaphore_wait(barrier, 2)

        @pl.when(middle)
        def _():
            pl.semaphore_wait(barrier, 3)

    lax.fori_loop(0, steps + 10, step, 0)
    for q in range(steps - 2, steps):
        away_sent(q)

    @pl.when(end)
    def _():
        for q in range(steps - NI, steps):
            end_sent(q)


def solution(mesh):
    def step(x, gain, wq, wk, wv, wo):
        rows, d = x.shape
        own = wq.shape[1]
        chunks = rows // R
        half = HEAD // 2
        freq = np.float32(THETA) ** (-np.arange(half, dtype=np.float32) / half)
        freq = jnp.asarray(np.concatenate([freq, freq])[None], jnp.float32)
        bf16, f32 = jnp.bfloat16, jnp.float32
        hbm = pl.BlockSpec(memory_space=pl.ANY)
        vmem = pl.BlockSpec(memory_space=pltpu.VMEM)
        dma = pltpu.SemaphoreType.DMA
        return pl.pallas_call(
            _kernel,
            out_shape=jax.ShapeDtypeStruct((rows, d), bf16),
            in_specs=[hbm, vmem, vmem, hbm, hbm, hbm, hbm],
            out_specs=hbm,
            scratch_shapes=[
                pltpu.VMEM((NI, XR, d), bf16),
                pltpu.VMEM((8, d), f32),
                pltpu.VMEM((2, R, d), bf16),
                pltpu.VMEM((XR, d), bf16),
                pltpu.VMEM((NB, KB, 768), bf16),
                pltpu.VMEM((R, 768), f32),
                pltpu.VMEM((NI, 2, own, 2 * PC), bf16),
                pltpu.VMEM((rows, own), bf16),
                pltpu.VMEM((own // HEAD, HEAD + 8, rows), bf16),
                pltpu.VMEM((3, R, own), bf16),
                pltpu.VMEM((2, R, HEAD), bf16),
                pltpu.VMEM((2, R, HEAD), f32),
                pltpu.VMEM((2, R, HEAD), f32),
                pltpu.VMEM((2, R, HEAD), f32),
                pltpu.VMEM((2, 1, R), f32),
                pltpu.VMEM((2, HEAD + 8, R), f32),
                pltpu.VMEM((2, RING, R, PC), bf16),
                pltpu.VMEM((2, RING, R, PC), bf16),
                pltpu.VMEM((4, R, PC), bf16),
                pltpu.VMEM((2, 4, R, PC), bf16),
                pltpu.VMEM((2, NP, R, PC), bf16),
                pltpu.VMEM((2, R, 2 * PC), bf16),
                pltpu.VMEM((2, 2, own, 2 * PC), bf16),
                dma((NI,)),
                dma((NB, 3)),
                dma((NI, 2)),
                dma((2, 2)),
                dma((2,)),
                dma((2, RING)),
                dma((2, RING)),
                dma((4,)),
                dma((2, RING)),
                dma((2, RING)),
                dma((2, 4)),
                dma((2, NP)),
                dma((2, NP)),
                dma((2, NP)),
                dma((NP,)),
            ],
            compiler_params=pltpu.CompilerParams(collective_id=1, has_side_effects=True, vmem_limit_bytes=67_000_000),
            name="layer",
        )(x, gain, freq, wq, wk, wv, wo)

    tokens, columns = P("dp", None), P(None, "tp")
    return jax.shard_map(
        step,
        mesh=mesh,
        in_specs=(tokens, P(None), columns, columns, columns, P("tp", None)),
        out_specs=tokens,
        check_vma=False,
    )
```

```python
import functools

import jax
import jax.numpy as jnp
import numpy as np
from jax import lax
from jax.experimental import pallas as pl
from jax.experimental.pallas import tpu as pltpu
from jax.sharding import PartitionSpec as P

HEAD = 128
THETA = 10000
NEG = -1e30
HIDDEN = 2 * NEG
LOG2E = 1.4426950408889634
VMEM = 358 * 2**20 // 10
R = 256
KB = 2048
PC = 256
NB = 4
XR = R // 4
KEYS = 512
PR = R // 2
NI = 4
NP = 4 * NI
RING = 32
MESH = pl.DeviceIdType.MESH


def _dot(a, b, ca, cb):
    return lax.dot_general(a, b, (((ca,), (cb,)), ((), ())), preferred_element_type=jnp.float32)


def _parts(xb, a_s, wbuf, k_s):
    half = KB // 2
    some = [((pl.ds(0, half), pl.ds((2 * kb + n) * 768, 768)), wbuf.at[kb, pl.ds(n * half, half)]) for kb in range(NB) for n in range(2)]
    some += [((pl.ds(0, half), pl.ds(2 * NB * 768 + n * 1024, 1024)), k_s.at[pl.ds(n * half, half)]) for n in range(2)]
    some += [((pl.ds(half + n * R, R), slice(None)), a_s.at[n]) for n in range(2)]
    return some + [((pl.ds(half + 2 * R + n * XR, XR), slice(None)), xb.at[n]) for n in range(NI)]


def _gather(y_ref, xb, a_s, wbuf, k_s, out_ref, buf, i_sem, o_sem, sem):
    rows, n = y_ref.shape[0], 4
    last = [pl.ds(rows - R + b * (R // n), R // n) for b in range(n)]
    loads = [pltpu.make_async_copy(y_ref.at[at], buf.at[b], i_sem.at[b]) for b, at in enumerate(last)]
    stores = [pltpu.make_async_copy(buf.at[b], out_ref.at[at], o_sem.at[b]) for b, at in enumerate(last)]
    kept = [pltpu.make_async_copy(ref, out_ref.at[at], sem.at[i]) for i, (at, ref) in enumerate(_parts(xb, a_s, wbuf, k_s))]
    for copy in loads + kept:
        copy.start()
    for load, store in zip(loads, stores):
        load.wait()
        store.start()
    for copy in stores + kept:
        copy.wait()


def _kernel(x_ref, gain_ref, freq_ref, wq_ref, wk_ref, wv_ref, wo_ref, y_ref, xb, a_s, wbuf, k_s,
            gain_s, stage_s, acc_s, wo_s, vt_s, s_s, q_s, turns_s, cos_s, sin_s, top_s, mix_s,
            part, from_e, from_m, obuf, sbuf, xres, away_s,
            x_sem, w_sem, wo_sem, away_sem, xr_sem, r_part, r_e, r_m, r_res, r_y, s_o, s_u, s_e, s_p, s_l, keep_sem):
    rows, d = x_ref.shape
    chunks = rows // R
    steps = chunks * NI
    pieces = chunks * NP
    scale = HEAD**-0.5
    e = scale * LOG2E
    tp = lax.axis_index("tp")
    z, core = lax.div(tp, 2), lax.rem(tp, 2)
    middle = (z == 1) | (z == 2)
    end = jnp.logical_not(middle)
    partner = z * 2 + 1 - core
    inner = jnp.where(z < 2, 1, 2) * 2 + core
    outer = jnp.where(z < 2, 0, 3) * 2 + core
    other = (3 - z) * 2 + core
    near = jnp.where(z < 2, 0, 1)
    half = d // 2
    quarter = d // 4

    def col(side, ab, i):
        g = near if ab == 1 else 1 - near
        return pl.multiple_of(side * half + g * quarter + i * PC, PC)

    def chunk(c):
        return lax.div(c, NP)

    def ring(c):
        return lax.rem(c, RING)

    def unit(c):
        return lax.div(lax.rem(c, NP), 2), pl.ds(pl.multiple_of(lax.rem(c, 2) * PR, PR), PR)

    def row(k):
        return pl.ds(pl.multiple_of(k * R, R), R)

    def remote(src, dst, send, recv, to):
        return pltpu.make_async_remote_copy(src, dst, send, recv, device_id={"tp": to}, device_id_type=MESH)

    def stash():
        return _parts(xb, a_s, wbuf, k_s)

    def keep(n):
        at, ref = stash()[n]
        return pltpu.make_async_copy(y_ref.at[at], ref, keep_sem.at[n])

    def done(ref, sem):
        pltpu.make_async_copy(ref, ref, sem).wait()

    def is_piece(c):
        return (c >= 0) & (c < pieces)

    def load_x(b):
        slot = lax.rem(b, NI)
        return pltpu.make_async_copy(x_ref.at[pl.ds(pl.multiple_of(b * XR, XR), XR)], xb.at[slot], x_sem.at[slot])

    def load_w(t, kb, m):
        w = (wq_ref, wk_ref, wv_ref)[m]
        i = lax.rem(t, NI)
        return pltpu.make_async_copy(
            w.at[pl.ds(kb * KB, KB), pl.ds(pl.multiple_of(i * 256, 256), 256)],
            wbuf.at[kb, :, pl.ds(m * 256, 256)], w_sem.at[kb])

    def load_away(q, ab):
        slot = lax.rem(q, 2)
        at = pl.ds(col(1 - core, ab, 2 * lax.rem(q, NI)), 2 * PC)
        return pltpu.make_async_copy(wo_ref.at[:, at], away_s.at[slot, ab], away_sem.at[slot, ab])

    def load_wo(i, ab):
        at = pl.ds(col(core, ab, 2 * i), 2 * PC)
        return pltpu.make_async_copy(wo_ref.at[:, at], wo_s.at[i, ab], wo_sem.at[i, ab])

    def load_res(q):
        slot, i = lax.rem(q, 2), lax.rem(q, NI)
        return pltpu.make_async_copy(
            x_ref.at[row(lax.div(q, NI)), pl.ds(col(core, 1, 2 * i), 2 * PC)], xres.at[slot], xr_sem.at[slot])

    def to_partner(n, ab):
        p, r = lax.rem(n, 4), lax.rem(n, RING // 2)
        return remote(obuf.at[ab, p], part.at[ab, r], s_o.at[lax.div(p, 2)], r_part.at[ab, r], partner)

    def turn_of(c):
        return lax.rem(lax.div(c, 4), NI)

    def held(ab, c):
        i, at = unit(c)
        return sbuf.at[ab, i, at]

    def to_inner(c, ab):
        return remote(held(ab, c), from_e.at[ab, ring(c)], s_u.at[ab, turn_of(c)], r_e.at[ab, ring(c)], inner)

    def to_other(c):
        p = lax.rem(c, 8)
        return remote(held(0, c), from_m.at[p], s_u.at[0, turn_of(c)], r_m.at[p], other)

    def y_at(c, side, ab):
        i, _ = unit(c)
        at = pl.ds(pl.multiple_of(chunk(c) * R + lax.rem(c, 2) * PR, PR), PR)
        return y_ref.at[at, pl.ds(col(side, ab, i), PC)]

    def y_unit(n, side, ab):
        return y_ref.at[row(lax.div(n, NP // 2)), pl.ds(col(side, ab, lax.rem(n, NP // 2)), PC)]

    def result_to_other(c):
        return remote(held(1, c), y_at(c, core, 1), s_u.at[1, turn_of(c)], r_res.at[0, ring(c)], other)

    def result_to_outer(c, ab, src):
        return remote(src, y_at(c, core, ab), s_e.at[ab, turn_of(c)], r_res.at[ab, ring(c)], outer)

    def result_to_partner(n, ab, src, side):
        q = lax.div(n, 2)
        return remote(src, y_unit(n, side, ab), s_p.at[ab, lax.rem(q, NI)], r_y.at[ab, lax.rem(q, RING // 4)], partner)

    def result_here(n):
        i = lax.rem(n, NP // 2)
        return pltpu.make_async_copy(sbuf.at[1, i], y_unit(n, core, 1), s_l.at[lax.rem(lax.div(n, 2), NI)])

    barrier = pltpu.get_barrier_semaphore()

    def greet(to):
        pl.semaphore_signal(barrier, inc=1, device_id={"tp": to}, device_id_type=MESH)

    for b in range(NI):
        load_x(b).start()
    greet(partner)

    @pl.when(end)
    def _():
        greet(inner)

    @pl.when(middle)
    def _():
        greet(outer)
        greet(other)

    gain_s[...] = jnp.broadcast_to(gain_ref[...].astype(jnp.float32)[None], gain_s.shape)

    for h in range(2 * NI):
        vt_s[h, HEAD:, :] = jnp.ones((8, rows), jnp.bfloat16)
    for kb in range(2):
        for m in range(3):
            load_w(0, kb, m).start()

    def norm(b, to, top):
        slot = lax.rem(b, NI)
        sizes = []
        for g in range(XR // 16):
            wide = xb[slot, g * 16 : g * 16 + 16, :].astype(jnp.float32)
            sizes.append(lax.rsqrt(jnp.mean(wide * wide, -1, keepdims=True) + 1e-6))
        for g, size in enumerate(sizes):
            wide = xb[slot, g * 16 : g * 16 + 16, :].astype(jnp.float32) * size
            wide = wide.reshape(2, 8, d) * gain_s[...][None]
            to[pl.ds(pl.multiple_of(top + g * 16, 16), 16), :] = wide.reshape(16, d).astype(jnp.bfloat16)
        angles(b)

    sign = jnp.where(lax.broadcasted_iota(jnp.int32, (8, HEAD), 1) < HEAD // 2, -1.0, 1.0)

    def angles(b):
        k, i = lax.div(b, NI), lax.rem(b, NI)
        here = pl.ds(pl.multiple_of(i * XR, XR), XR)
        angle = jnp.full((8, HEAD), k * R, jnp.int32).astype(jnp.float32) * freq_ref[...]
        c, s = jnp.cos(angle)[:1], (jnp.sin(angle) * sign)[:1]
        cos, sin = turns_s[0, here, :], turns_s[1, here, :]
        cos_s[lax.rem(k, 2), here, :] = cos * c - sin * s
        sin_s[lax.rem(k, 2), here, :] = sin * c + cos * s

    def first_angles():
        token = lax.broadcasted_iota(jnp.int32, (R, HEAD), 0).astype(jnp.float32)
        angle = token * freq_ref[...]
        turns_s[0] = jnp.cos(angle)
        turns_s[1] = jnp.sin(angle) * jnp.concatenate([sign] * (R // 8), axis=0)

    def more_x(b):
        @pl.when(b < steps)
        def _():
            load_x(b).start()

    def project(t, part, ahead):
        p = lax.rem(lax.div(t, NI), 2)
        blocks = (2 * part, 2 * part + 1)
        for kb in blocks:
            done(wbuf.at[kb], w_sem.at[kb])
        if ahead:
            load_x(t + NI).wait()
            norm(t + NI, stage_s, 0)
        for kb in blocks:
            some = _dot(a_s[p, :, kb * KB : (kb + 1) * KB], wbuf[kb], 1, 0)
            acc_s[...] = some if kb == 0 else acc_s[...] + some
        if ahead:
            k, at = lax.rem(lax.div(t + NI, NI), 2), lax.rem(t, NI) * XR
            a_s[k, pl.ds(pl.multiple_of(at, XR), XR), :] = stage_s[...]
            more_x(t + 2 * NI)

        @pl.when(t + 1 < steps)
        def _():
            for kb in blocks:
                for m in range(3):
                    load_w(t + 1, kb, m).start()

    def rotate(t):
        k, i = lax.div(t, NI), lax.rem(t, NI)
        p = lax.rem(k, 2)
        lane = lambda h: pl.ds(pl.multiple_of(i * 256 + h * HEAD, HEAD), HEAD)

        def turned(at):
            one = acc_s[:, at : at + HEAD].astype(jnp.bfloat16).astype(jnp.float32)
            return (one * cos_s[p] + pltpu.roll(one, HEAD // 2, 1) * sin_s[p]).astype(jnp.bfloat16)

        for h in range(2):
            q_s[2 * i + h] = turned(h * HEAD)
            k_s[row(k), lane(h)] = turned(256 + h * HEAD)
            vt_s[2 * i + h, :HEAD, row(k)] = acc_s[:, 512 + h * HEAD : 512 + (h + 1) * HEAD].astype(jnp.bfloat16).T

    def attend(t):
        k, i = lax.div(t, NI), lax.rem(t, NI)
        lane = lambda h: pl.ds(pl.multiple_of(i * 256 + h * HEAD, HEAD), HEAD)
        for h in range(2):
            top_s[h] = jnp.full((1, R), NEG, jnp.float32)
            mix_s[h] = jnp.zeros((HEAD + 8, R), jnp.float32)

        def block(first, keys, masked):
            here = pl.ds(pl.multiple_of(first, keys), keys)
            scores = [_dot(k_s[here, lane(h)], q_s[2 * i + h], 1, 1) for h in range(2)]
            if masked:
                gap = lax.broadcasted_iota(jnp.int32, (keys, R), 1) - lax.broadcasted_iota(jnp.int32, (keys, R), 0)
                seen = gap >= first - k * R
                scores = [jnp.where(seen, s, HIDDEN) for s in scores]
            weights, keeps = [], []
            for h, s in enumerate(scores):
                old = top_s[h]
                top = jnp.maximum(old, s.max(axis=0, keepdims=True))
                top_s[h] = top
                weights.append(jnp.exp2((s - top) * e).astype(jnp.bfloat16))
                keeps.append(jnp.exp2((old - top) * e))
            for h in range(2):
                mix_s[h] = mix_s[h] * keeps[h] + _dot(vt_s[2 * i + h, :, here], weights[h], 1, 0)

        whole = lax.div(k * R, KEYS)

        def plain(j, carry):
            block(j * KEYS, KEYS, False)
            return carry

        lax.fori_loop(0, whole, plain, 0)

        @pl.when(lax.rem(k, 2) == 1)
        def _():
            block(whole * KEYS, KEYS, True)

        @pl.when(lax.rem(k, 2) == 0)
        def _():
            block(k * R, R, True)

        for h in range(2):
            out = mix_s[h, :HEAD, :] * (1 / mix_s[h, HEAD : HEAD + 1, :])
            s_s[lax.rem(k, 3), :, lane(h)] = out.T.astype(jnp.bfloat16)

    def attend_first():
        gap = lax.broadcasted_iota(jnp.int32, (R, R), 1) - lax.broadcasted_iota(jnp.int32, (R, R), 0)
        heads = range(2 * NI)
        scores = [_dot(k_s[:R, h * HEAD : (h + 1) * HEAD], q_s[h], 1, 1) for h in heads]
        weights = []
        for s in scores:
            s = jnp.where(gap >= 0, s, HIDDEN)
            weights.append(jnp.exp2((s - s.max(axis=0, keepdims=True)) * e).astype(jnp.bfloat16))
        for h in heads:
            mix = _dot(vt_s[h, :, :R], weights[h], 1, 0)
            out = mix[:HEAD] * (1 / mix[HEAD : HEAD + 1])
            s_s[0, :, h * HEAD : (h + 1) * HEAD] = out.T.astype(jnp.bfloat16)

    def mine(k):
        return s_s[lax.rem(k, 3)]

    def send_away(q):
        with jax.named_scope("away"):
            @pl.when(q >= 2)
            def _():
                away_sent(q - 2)

            for ab in range(2):
                load_away(q, ab).wait()
                term = _dot(mine(lax.div(q, NI)), away_s[lax.rem(q, 2), ab], 1, 0)
                for u in range(2):
                    obuf[ab, lax.rem(2 * q + u, 4)] = term[:, u * PC : (u + 1) * PC].astype(jnp.bfloat16)
                for u in range(2):
                    to_partner(2 * q + u, ab).start()

            @pl.when(q + 2 < steps)
            def _():
                for ab in range(2):
                    load_away(q + 2, ab).start()

    def away_sent(q):
        i = lax.rem(q, 2)
        done(obuf.at[:, pl.ds(2 * i, 2)], s_o.at[i])

    def block(q, ab):
        i = lax.rem(q, NI)
        return sbuf.at[ab, pl.ds(2 * i, 2)]

    def end_sent(q):
        for ab in range(2):
            done(block(q, ab), s_u.at[ab, lax.rem(q, NI)])

    def end_sum(q):
        with jax.named_scope("end_sum"):
            i = lax.rem(q, NI)

            @pl.when(q < NI)
            def _():
                for ab in range(2):
                    load_wo(q, ab).wait()

            @pl.when(q >= NI)
            def _():
                end_sent(q - NI)

            for ab in range(2):
                term = _dot(mine(lax.div(q, NI)), wo_s[i, ab], 1, 0)
                for u in range(2):
                    n = 2 * q + u
                    to_partner(n, ab).wait_recv()
                    some = term[:, u * PC : (u + 1) * PC] + part[ab, lax.rem(n, RING // 2)].astype(jnp.float32)
                    sbuf[ab, lax.rem(n, NP // 2)] = some.astype(jnp.bfloat16)
                if ab == 0:
                    to_inner(4 * q, 0).start()

                    @pl.when(q > 0)
                    def _():
                        to_inner(4 * q - 2, 1).start()

                    to_inner(4 * q + 1, 0).start()

                    @pl.when(q > 0)
                    def _():
                        to_inner(4 * q - 1, 1).start()

                    to_inner(4 * q + 2, 0).start()
                else:
                    to_inner(4 * q, 1).start()
                    to_inner(4 * q + 3, 0).start()
                    to_inner(4 * q + 1, 1).start()

                    @pl.when(q == steps - 1)
                    def _():
                        to_inner(4 * q + 2, 1).start()
                        to_inner(4 * q + 3, 1).start()

    def middle_pass(c, v):
        q, n, u = lax.div(c, 4), lax.div(c, 2), v // 2
        at = pl.ds(v % 2 * PR, PR)
        with jax.named_scope("pass_w"):
            if v == 0:
                @pl.when(q < NI)
                def _():
                    load_wo(q, 0).wait()

            if v % 2 == 0:
                to_partner(n, 0).wait_recv()
            to_inner(c, 0).wait_recv()
        with jax.named_scope("pass"):
            term = _dot(s_s[lax.rem(chunk(c), 3), at, :], wo_s[lax.rem(q, NI), 0, :, u * PC : (u + 1) * PC], 1, 0)
            term = term + part[0, lax.rem(n, RING // 2), at, :].astype(jnp.float32) + from_e[0, ring(c)].astype(jnp.float32)
            sbuf[0, lax.rem(n, NP // 2), at, :] = term.astype(jnp.bfloat16)
            to_other(c).start()

    def middle_finish(c, v):
        q, n, u = lax.div(c, 4), lax.div(c, 2), v // 2
        at = pl.ds(v % 2 * PR, PR)
        with jax.named_scope("finish_w"):
            if v == 0:
                @pl.when(q < NI)
                def _():
                    load_wo(q, 1).wait()

                load_res(q).wait()
            if v % 2 == 0:
                to_partner(n, 1).wait_recv()
            to_inner(c, 1).wait_recv()
            to_other(c).wait_recv()
        with jax.named_scope("finish"):
            term = _dot(s_s[lax.rem(chunk(c), 3), at, :], wo_s[lax.rem(q, NI), 1, :, u * PC : (u + 1) * PC], 1, 0)
            term = term + part[1, lax.rem(n, RING // 2), at, :].astype(jnp.float32)
            term = term + from_e[1, ring(c)].astype(jnp.float32) + from_m[lax.rem(c, 8)].astype(jnp.float32)
            term = term + xres[lax.rem(q, 2), at, u * PC : (u + 1) * PC].astype(jnp.float32)
            sbuf[1, lax.rem(n, NP // 2), at, :] = term.astype(jnp.bfloat16)
            result_to_outer(c, 1, held(1, c)).start()
            result_to_other(c).start()
            if v % 2 == 1:
                result_to_partner(n, 1, sbuf.at[1, lax.rem(n, NP // 2)], core).start()
                result_here(n).start()

    def middle_forward(c, v):
        src = y_at(c, core, 0)
        with jax.named_scope("forward_w"):
            result_to_outer(c, 0, src).wait_recv()
        result_to_outer(c, 0, src).start()
        if v % 2 == 1:
            n = lax.div(c, 2)
            result_to_partner(n, 0, y_unit(n, core, 0), core).start()

    def middle_turn(t, j):
        s = 4 * t + j

        @pl.when(is_piece(s - 16) & middle)
        def _():
            middle_pass(s - 16, j)

        @pl.when(is_piece(s - 18) & middle)
        def _():
            middle_finish(s - 18, (j + 2) % 4)

        @pl.when(is_piece(s - 20) & middle)
        def _():
            middle_forward(s - 20, j)

    def norms(first, k):
        def one(i, carry):
            b = first + i
            with jax.named_scope("x_w"):
                load_x(b).wait()
            slot = lax.rem(b, NI)

            def squares(j, total):
                at = pl.ds(pl.multiple_of(j * 1024, 1024), 1024)
                for g in range(XR // 16):
                    wide = xb[slot, g * 16 : g * 16 + 16, at].astype(jnp.float32)
                    wide = wide * wide
                    some = wide[:, :HEAD]
                    for n in range(1, 8):
                        some = some + wide[:, n * HEAD : (n + 1) * HEAD]
                    total = total[:g] + (total[g] + some,) + total[g + 1 :]
                return total

            total = lax.fori_loop(0, d // 1024, squares, (jnp.zeros((16, HEAD), jnp.float32),) * (XR // 16))
            sizes = [lax.rsqrt(jnp.sum(v, -1, keepdims=True) / d + 1e-6) for v in total]
            sizes = tuple(jnp.broadcast_to(v, (16, HEAD)) for v in sizes)

            def scaled(j, sizes):
                at = pl.ds(pl.multiple_of(j * 1024, 1024), 1024)
                for g in range(XR // 16):
                    wide = xb[slot, g * 16 : g * 16 + 16, at].astype(jnp.float32)
                    wide = wide * jnp.concatenate([sizes[g]] * 8, axis=1)
                    wide = wide.reshape(2, 8, 1024) * gain_s[:, at][None]
                    a_s[k, pl.ds(pl.multiple_of(i * XR + g * 16, 16), 16), at] = wide.reshape(16, 1024).astype(jnp.bfloat16)
                return sizes

            lax.fori_loop(0, d // 1024, scaled, sizes)
            angles(b)
            if k == 0:
                @pl.when(b == 1)
                def _():
                    for kb in (2, 3):
                        for m in range(3):
                            load_w(0, kb, m).start()
            else:
                more_x(b + NI)
            return carry

        lax.fori_loop(0, NI, one, 0)

    def step(t, carry):
        def is_block(q):
            return (q >= 0) & (q < steps)

        @pl.when(is_block(t - 8) & middle)
        def _():
            q = t - 8
            done(block(q, 0), s_u.at[0, lax.rem(q, NI)])
            for sem in (s_u.at[1], s_e.at[1], s_p.at[1], s_l):
                done(block(q, 1), sem.at[lax.rem(q, NI)])

        @pl.when(is_block(t - 9) & middle)
        def _():
            q = t - 9
            for sem in (s_e, s_p):
                done(block(q, 0), sem.at[0, lax.rem(q, NI)])

        @pl.when(is_block(t - 4) & middle)
        def _():
            load_res(t - 4).start()

        @pl.when(t == 2)
        def _():
            for ab in range(2):
                load_away(0, ab).start()

        @pl.when((t >= 2) & (t < 2 + NI))
        def _():
            for ab in range(2):
                load_wo(t - 2, ab).start()

        @pl.when(t == 3)
        def _():
            for ab in range(2):
                load_away(1, ab).start()

        ahead = (t >= NI) & (t + NI < steps)
        middle_turn(t, 0)

        @pl.when(ahead)
        def _():
            with jax.named_scope("project0"):
                project(t, 0, True)

        @pl.when(jnp.logical_not(ahead) & (t < steps))
        def _():
            with jax.named_scope("project0_"):
                project(t, 0, False)

        @pl.when(t == NI - 1)
        def _():
            for b in range(NI, 2 * NI):
                load_x(b).start()

        middle_turn(t, 1)

        @pl.when(t < steps)
        def _():
            with jax.named_scope("project1"):
                project(t, 1, False)
            with jax.named_scope("rotate"):
                rotate(t)

        middle_turn(t, 2)

        @pl.when((t >= NI) & (t < steps))
        def _():
            with jax.named_scope("attend"):
                attend(t)

        @pl.when(t == NI - 1)
        def _():
            with jax.named_scope("attend_first"):
                attend_first()

        middle_turn(t, 3)
        i = lax.rem(t, NI)

        @pl.when(is_block(t - 3) & (i == NI - 1))
        def _():
            send_away(t - 3)

            @pl.when(end)
            def _():
                end_sum(t - 3)

        @pl.when(is_block(t - 2) & (i != NI - 2))
        def _():
            send_away(t - 2)

            @pl.when(end)
            def _():
                end_sum(t - 2)

        @pl.when(t == NI - 1)
        def _():
            with jax.named_scope("norm1"):
                norms(NI, 1)

        @pl.when(is_block(t - 8) & end)
        def _():
            for u in range(2):
                n = 2 * (t - 8) + u
                for ab in (1, 0):
                    with jax.named_scope("result_w"):
                        for r in range(2):
                            c = 2 * n + r
                            result_to_outer(c, ab, y_at(c, core, ab)).wait_recv()
                    result_to_partner(n, ab, y_unit(n, core, ab), core).start()

        @pl.when(is_block(t - 9) & end)
        def _():
            for ab in range(2):
                done(block(t - 9, ab), s_p.at[ab, lax.rem(t - 9, NI)])

        @pl.when(t == steps + 2)
        def _():
            for n in range(len(stash()) - NI):
                keep(n).start()

        @pl.when(t == steps + 6)
        def _():
            for n in range(len(stash()) - NI, len(stash())):
                keep(n).start()

        @pl.when(is_block(t - 9))
        def _():
            with jax.named_scope("y_w"):
                for ab in range(2):
                    done(block(t - 9, ab), r_y.at[ab, lax.rem(t - 9, RING // 4)])

        return carry

    with jax.named_scope("angles"):
        first_angles()
    with jax.named_scope("norm0"):
        norms(0, 0)

    with jax.named_scope("barrier"):
        @pl.when(end)
        def _():
            pl.semaphore_wait(barrier, 2)

        @pl.when(middle)
        def _():
            pl.semaphore_wait(barrier, 3)

    lax.fori_loop(0, steps + 9, step, 0)
    for n in range(len(stash())):
        keep(n).wait()

    for q in range(steps - 2, steps):
        away_sent(q)

    @pl.when(end)
    def _():
        for q in range(steps - NI, steps):
            end_sent(q)


def solution(mesh):
    def step(x, gain, wq, wk, wv, wo):
        rows, d = x.shape
        own = wq.shape[1]
        chunks = rows // R
        half = HEAD // 2
        freq = np.float32(THETA) ** (-np.arange(half, dtype=np.float32) / half)
        freq = jnp.asarray(np.concatenate([freq, freq])[None], jnp.float32)
        bf16, f32 = jnp.bfloat16, jnp.float32
        hbm = pl.BlockSpec(memory_space=pl.ANY)
        vmem = pl.BlockSpec(memory_space=pltpu.VMEM)
        dma = pltpu.SemaphoreType.DMA
        parts = [((NI, XR, d), "xb"), ((2, R, d), "a"), ((NB, KB, 768), "w"), ((rows, own), "k")]
        y, *kept = pl.pallas_call(
            _kernel,
            out_shape=[jax.ShapeDtypeStruct((rows, d), bf16)] + [pltpu.VMEM(shape, bf16) for shape, _ in parts],
            in_specs=[hbm, vmem, vmem, hbm, hbm, hbm, hbm],
            out_specs=[hbm] + [vmem] * 4,
            scratch_shapes=[
                pltpu.VMEM((8, d), f32),
                pltpu.VMEM((XR, d), bf16),
                pltpu.VMEM((R, 768), f32),
                pltpu.VMEM((NI, 2, own, 2 * PC), bf16),
                pltpu.VMEM((own // HEAD, HEAD + 8, rows), bf16),
                pltpu.VMEM((3, R, own), bf16),
                pltpu.VMEM((own // HEAD, R, HEAD), bf16),
                pltpu.VMEM((2, R, HEAD), f32),
                pltpu.VMEM((2, R, HEAD), f32),
                pltpu.VMEM((2, R, HEAD), f32),
                pltpu.VMEM((2, 1, R), f32),
                pltpu.VMEM((2, HEAD + 8, R), f32),
                pltpu.VMEM((2, RING // 2, R, PC), bf16),
                pltpu.VMEM((2, RING, PR, PC), bf16),
                pltpu.VMEM((8, PR, PC), bf16),
                pltpu.VMEM((2, 4, R, PC), bf16),
                pltpu.VMEM((2, NP // 2, R, PC), bf16),
                pltpu.VMEM((2, R, 2 * PC), bf16),
                pltpu.VMEM((2, 2, own, 2 * PC), bf16),
                dma((NI,)),
                dma((NB,)),
                dma((NI, 2)),
                dma((2, 2)),
                dma((2,)),
                dma((2, RING // 2)),
                dma((2, RING)),
                dma((8,)),
                dma((2, RING)),
                dma((2, RING // 4)),
                dma((2,)),
                dma((2, NI)),
                dma((2, NI)),
                dma((2, NI)),
                dma((NI,)),
                dma((20,)),
            ],
            compiler_params=pltpu.CompilerParams(collective_id=1, has_side_effects=True, vmem_limit_bytes=VMEM),
            name="layer",
        )(x, gain, freq, wq, wk, wv, wo)
        return pl.pallas_call(
            _gather,
            out_shape=jax.ShapeDtypeStruct((rows, d), bf16),
            in_specs=[hbm] + [vmem] * 4,
            out_specs=hbm,
            scratch_shapes=[pltpu.VMEM((4, R // 4, d), bf16), dma((4,)), dma((4,)), dma((20,))],
            compiler_params=pltpu.CompilerParams(vmem_limit_bytes=9 * 2**19),
            name="gather",
        )(y, *kept)

    tokens, columns = P("dp", None), P(None, "tp")
    return jax.shard_map(
        step,
        mesh=mesh,
        in_specs=(tokens, P(None), columns, columns, columns, P("tp", None)),
        out_specs=tokens,
        check_vma=False,
    )
```

```python
import functools

import jax
import jax.numpy as jnp
import numpy as np
from jax import lax
from jax.experimental import pallas as pl
from jax.experimental.pallas import tpu as pltpu
from jax.sharding import PartitionSpec as P

HEAD = 128
THETA = 10000
NEG = -1e30
HIDDEN = 2 * NEG
LOG2E = 1.4426950408889634
VMEM = 358 * 2**20 // 10
R = 256
KB = 2048
PC = 256
NB = 4
XR = R // 4
KEYS = 512
BOTH = (0, 1)
ROWS = 16
WIDE = 1024
PR = R // 2
NI = 4
NP = 4 * NI
RING = 32
MESH = pl.DeviceIdType.MESH


def _dot(a, b, ca, cb):
    return lax.dot_general(a, b, (((ca,), (cb,)), ((), ())), preferred_element_type=jnp.float32)


def _parts(xb, a_s, wbuf, k_s):
    half = KB // 2
    some = [((pl.ds(0, half), pl.ds((2 * kb + n) * 768, 768)), wbuf.at[kb, pl.ds(n * half, half)]) for kb in range(NB) for n in BOTH]
    some += [((pl.ds(0, half), pl.ds(2 * NB * 768 + n * 1024, 1024)), k_s.at[pl.ds(n * half, half)]) for n in BOTH]
    some += [((pl.ds(half + n * R, R), slice(None)), a_s.at[n]) for n in BOTH]
    return some + [((pl.ds(half + 2 * R + n * XR, XR), slice(None)), xb.at[n]) for n in range(NI)]


def _gather(y_ref, xb, a_s, wbuf, k_s, out_ref, buf, i_sem, o_sem, sem):
    rows, n = y_ref.shape[0], 4
    last = [pl.ds(rows - R + b * (R // n), R // n) for b in range(n)]
    loads = [pltpu.make_async_copy(y_ref.at[at], buf.at[b], i_sem.at[b]) for b, at in enumerate(last)]
    stores = [pltpu.make_async_copy(buf.at[b], out_ref.at[at], o_sem.at[b]) for b, at in enumerate(last)]
    kept = [pltpu.make_async_copy(ref, out_ref.at[at], sem.at[i]) for i, (at, ref) in enumerate(_parts(xb, a_s, wbuf, k_s))]
    for copy in loads + kept:
        copy.start()
    for load, store in zip(loads, stores):
        load.wait()
        store.start()
    for copy in stores + kept:
        copy.wait()


def _kernel(x_ref, gain_ref, freq_ref, wq_ref, wk_ref, wv_ref, wo_ref, y_ref, xb, a_s, wbuf, k_s,
            gain_s, stage_s, acc_s, wo_s, vt_s, s_s, q_s, turns_s, cos_s, sin_s, top_s, mix_s,
            part, from_e, from_m, obuf, sbuf, xres, away_s,
            x_sem, w_sem, wo_sem, away_sem, xr_sem, r_part, r_e, r_m, r_end, r_mid, r_y, s_o, s_u, s_e, s_p, s_l, keep_sem):
    rows, d = x_ref.shape
    chunks = rows // R
    steps = chunks * NI
    pieces = chunks * NP
    scale = HEAD**-0.5
    e = scale * LOG2E
    tp = lax.axis_index("tp")
    z, core = lax.div(tp, 2), lax.rem(tp, 2)
    middle = (z == 1) | (z == 2)
    end = jnp.logical_not(middle)
    partner = z * 2 + 1 - core
    inner = jnp.where(z < 2, 1, 2) * 2 + core
    outer = jnp.where(z < 2, 0, 3) * 2 + core
    other = (3 - z) * 2 + core
    near = jnp.where(z < 2, 0, 1)
    half = d // 2
    quarter = d // 4

    def col(side, ab, i):
        g = near if ab == 1 else 1 - near
        return pl.multiple_of(side * half + g * quarter + i * PC, PC)

    def chunk(c):
        return lax.div(c, NP)

    def ring(c):
        return lax.rem(c, RING)

    def unit(c):
        return lax.div(lax.rem(c, NP), 2), pl.ds(pl.multiple_of(lax.rem(c, 2) * PR, PR), PR)

    def row(k):
        return pl.ds(pl.multiple_of(k * R, R), R)

    def remote(src, dst, send, recv, to):
        return pltpu.make_async_remote_copy(src, dst, send, recv, device_id={"tp": to}, device_id_type=MESH)

    def stash():
        return _parts(xb, a_s, wbuf, k_s)

    def keep(n):
        at, ref = stash()[n]
        return pltpu.make_async_copy(y_ref.at[at], ref, keep_sem)

    def done(ref, sem):
        pltpu.make_async_copy(ref, ref, sem).wait()

    def is_piece(c):
        return (c >= 0) & (c < pieces)

    def load_x(b):
        slot = lax.rem(b, NI)
        return pltpu.make_async_copy(x_ref.at[pl.ds(pl.multiple_of(b * XR, XR), XR)], xb.at[slot], x_sem.at[slot])

    def load_w(t, kb, m):
        w = (wq_ref, wk_ref, wv_ref)[m]
        i = lax.rem(t, NI)
        return pltpu.make_async_copy(
            w.at[pl.ds(kb * KB, KB), pl.ds(pl.multiple_of(i * 256, 256), 256)],
            wbuf.at[kb, :, pl.ds(m * 256, 256)], w_sem.at[kb])

    def load_away(q, ab):
        slot = lax.rem(q, 2)
        at = pl.ds(col(1 - core, ab, 2 * lax.rem(q, NI)), 2 * PC)
        return pltpu.make_async_copy(wo_ref.at[:, at], away_s.at[slot, ab], away_sem.at[slot, ab])

    def load_wo(i, ab):
        at = pl.ds(col(core, ab, 2 * i), 2 * PC)
        return pltpu.make_async_copy(wo_ref.at[:, at], wo_s.at[i, ab], wo_sem.at[i, ab])

    def load_res(q):
        slot, i = lax.rem(q, 2), lax.rem(q, NI)
        return pltpu.make_async_copy(
            x_ref.at[row(lax.div(q, NI)), pl.ds(col(core, 1, 2 * i), 2 * PC)], xres.at[slot], xr_sem.at[slot])

    def to_partner(n, ab):
        p, r = lax.rem(n, 4), lax.rem(n, RING // 2)
        return remote(obuf.at[ab, p], part.at[ab, r], s_o.at[lax.div(p, 2)], r_part.at[ab, lax.div(r, 2)], partner)

    def turn_of(c):
        return lax.rem(lax.div(c, 4), NI)

    def held(ab, c):
        i, at = unit(c)
        return sbuf.at[ab, i, at]

    def to_inner(c, ab):
        return remote(held(ab, c), from_e.at[ab, ring(c)], s_u.at[ab, turn_of(c)], r_e.at[ab, ring(c)], inner)

    def to_other(c):
        p = lax.rem(c, 8)
        return remote(held(0, c), from_m.at[p], s_u.at[0, turn_of(c)], r_m.at[p], other)

    def y_at(c, side, ab):
        i, _ = unit(c)
        at = pl.ds(pl.multiple_of(chunk(c) * R + lax.rem(c, 2) * PR, PR), PR)
        return y_ref.at[at, pl.ds(col(side, ab, i), PC)]

    def y_unit(n, side, ab):
        return y_ref.at[row(lax.div(n, NP // 2)), pl.ds(col(side, ab, lax.rem(n, NP // 2)), PC)]

    def result_to_other(c):
        return remote(held(1, c), y_at(c, core, 1), s_u.at[1, turn_of(c)], r_mid.at[lax.rem(c, 8)], other)

    def result_to_outer(c, ab, src):
        return remote(src, y_at(c, core, ab), s_e.at[ab, turn_of(c)], r_end.at[ab, lax.div(ring(c), 4)], outer)

    def result_to_partner(n, ab, src, side):
        q = lax.div(n, 2)
        return remote(src, y_unit(n, side, ab), s_p.at[ab, lax.rem(q, NI)], r_y.at[ab, lax.rem(q, RING // 4)], partner)

    def result_here(n):
        i = lax.rem(n, NP // 2)
        return pltpu.make_async_copy(sbuf.at[1, i], y_unit(n, core, 1), s_l.at[lax.rem(lax.div(n, 2), NI)])

    barrier = pltpu.get_barrier_semaphore()

    def greet(to):
        pl.semaphore_signal(barrier, inc=1, device_id={"tp": to}, device_id_type=MESH)

    for b in range(NI):
        load_x(b).start()
    greet(partner)

    @pl.when(end)
    def _():
        greet(inner)

    @pl.when(middle)
    def _():
        greet(outer)
        greet(other)

    gain_s[...] = jnp.broadcast_to(gain_ref[...].astype(jnp.float32)[None], gain_s.shape)

    for h in range(2 * NI):
        vt_s[h, HEAD:, :] = jnp.ones((8, rows), jnp.bfloat16)
    for kb in BOTH:
        for m in range(3):
            load_w(0, kb, m).start()

    def norm(b, to, top):
        slot = lax.rem(b, NI)
        sizes = []
        for g in range(XR // ROWS):
            wide = xb[slot, g * ROWS : g * ROWS + ROWS, :].astype(jnp.float32)
            sizes.append(lax.rsqrt(jnp.mean(wide * wide, -1, keepdims=True) + 1e-6))
        for g, size in enumerate(sizes):
            wide = xb[slot, g * ROWS : g * ROWS + ROWS, :].astype(jnp.float32) * size
            wide = wide.reshape(2, 8, d) * gain_s[...][None]
            to[pl.ds(pl.multiple_of(top + g * ROWS, ROWS), ROWS), :] = wide.reshape(ROWS, d).astype(jnp.bfloat16)
        angles(b)

    sign = jnp.where(lax.broadcasted_iota(jnp.int32, (8, HEAD), 1) < HEAD // 2, -1.0, 1.0)

    def angles(b):
        k, i = lax.div(b, NI), lax.rem(b, NI)
        here = pl.ds(pl.multiple_of(i * XR, XR), XR)
        angle = jnp.full((8, HEAD), k * R, jnp.int32).astype(jnp.float32) * freq_ref[...]
        c, s = jnp.cos(angle)[:1], (jnp.sin(angle) * sign)[:1]
        cos, sin = turns_s[0, here, :], turns_s[1, here, :]
        cos_s[lax.rem(k, 2), here, :] = cos * c - sin * s
        sin_s[lax.rem(k, 2), here, :] = sin * c + cos * s

    def first_angles():
        token = lax.broadcasted_iota(jnp.int32, (R, HEAD), 0).astype(jnp.float32)
        angle = token * freq_ref[...]
        turns_s[0] = jnp.cos(angle)
        turns_s[1] = jnp.sin(angle) * jnp.concatenate([sign] * (R // 8), axis=0)

    def more_x(b):
        @pl.when(b < steps)
        def _():
            load_x(b).start()

    def project(t, part, ahead):
        p = lax.rem(lax.div(t, NI), 2)
        blocks = (2 * part, 2 * part + 1)
        for kb in blocks:
            done(wbuf.at[kb], w_sem.at[kb])
        if ahead:
            load_x(t + NI).wait()
            norm(t + NI, stage_s, 0)
        for kb in blocks:
            some = _dot(a_s[p, :, kb * KB : (kb + 1) * KB], wbuf[kb], 1, 0)
            acc_s[...] = some if kb == 0 else acc_s[...] + some
        if ahead:
            k, at = lax.rem(lax.div(t + NI, NI), 2), lax.rem(t, NI) * XR
            a_s[k, pl.ds(pl.multiple_of(at, XR), XR), :] = stage_s[...]
            more_x(t + 2 * NI)

        @pl.when((t + 1 < steps) & (t != NI - 1))
        def _():
            more_w(t, part)

    def more_w(t, part):
        for kb in (2 * part, 2 * part + 1):
            for m in range(3):
                load_w(t + 1, kb, m).start()

    def rotate(t):
        k, i = lax.div(t, NI), lax.rem(t, NI)
        p = lax.rem(k, 2)
        lane = lambda h: pl.ds(pl.multiple_of(i * 256 + h * HEAD, HEAD), HEAD)

        def turned(at):
            one = acc_s[:, at : at + HEAD].astype(jnp.bfloat16).astype(jnp.float32)
            return (one * cos_s[p] + pltpu.roll(one, HEAD // 2, 1) * sin_s[p]).astype(jnp.bfloat16)

        for h in BOTH:
            q_s[2 * i + h] = turned(h * HEAD)
            k_s[row(k), lane(h)] = turned(256 + h * HEAD)
            vt_s[2 * i + h, :HEAD, row(k)] = acc_s[:, 512 + h * HEAD : 512 + (h + 1) * HEAD].astype(jnp.bfloat16).T

    def attend(t):
        k, i = lax.div(t, NI), lax.rem(t, NI)
        lane = lambda h: pl.ds(pl.multiple_of(i * 256 + h * HEAD, HEAD), HEAD)
        for h in BOTH:
            top_s[h] = jnp.full((1, R), NEG, jnp.float32)
            mix_s[h] = jnp.zeros((HEAD + 8, R), jnp.float32)

        def block(first, keys, masked):
            here = pl.ds(pl.multiple_of(first, keys), keys)
            scores = [_dot(k_s[here, lane(h)], q_s[2 * i + h], 1, 1) for h in BOTH]
            if masked:
                gap = lax.broadcasted_iota(jnp.int32, (keys, R), 1) - lax.broadcasted_iota(jnp.int32, (keys, R), 0)
                seen = gap >= first - k * R
                scores = [jnp.where(seen, s, HIDDEN) for s in scores]
            weights, keeps = [], []
            for h, s in enumerate(scores):
                old = top_s[h]
                top = jnp.maximum(old, s.max(axis=0, keepdims=True))
                top_s[h] = top
                weights.append(jnp.exp2((s - top) * e).astype(jnp.bfloat16))
                keeps.append(jnp.exp2((old - top) * e))
            for h in BOTH:
                mix_s[h] = mix_s[h] * keeps[h] + _dot(vt_s[2 * i + h, :, here], weights[h], 1, 0)

        whole = lax.div(k * R, KEYS)

        def plain(j, carry):
            block(j * KEYS, KEYS, False)
            return carry

        lax.fori_loop(0, whole, plain, 0)

        @pl.when(lax.rem(k, 2) == 1)
        def _():
            block(whole * KEYS, KEYS, True)

        @pl.when(lax.rem(k, 2) == 0)
        def _():
            block(k * R, R, True)

        for h in BOTH:
            out = mix_s[h, :HEAD, :] * (1 / mix_s[h, HEAD : HEAD + 1, :])
            s_s[lax.rem(k, 3), :, lane(h)] = out.T.astype(jnp.bfloat16)

    def attend_first():
        gap = lax.broadcasted_iota(jnp.int32, (R, R), 1) - lax.broadcasted_iota(jnp.int32, (R, R), 0)
        heads = range(2 * NI)
        scores = [_dot(k_s[:R, h * HEAD : (h + 1) * HEAD], q_s[h], 1, 1) for h in heads]
        weights = []
        for s in scores:
            s = jnp.where(gap >= 0, s, HIDDEN)
            weights.append(jnp.exp2((s - s.max(axis=0, keepdims=True)) * e).astype(jnp.bfloat16))
        for h in heads:
            mix = _dot(vt_s[h, :, :R], weights[h], 1, 0)
            out = mix[:HEAD] * (1 / mix[HEAD : HEAD + 1])
            s_s[0, :, h * HEAD : (h + 1) * HEAD] = out.T.astype(jnp.bfloat16)

    def mine(k):
        return s_s[lax.rem(k, 3)]

    def send_away(q):
        with jax.named_scope("away"):
            @pl.when(q >= 2)
            def _():
                away_sent(q - 2)

            for ab in BOTH:
                load_away(q, ab).wait()
                term = _dot(mine(lax.div(q, NI)), away_s[lax.rem(q, 2), ab], 1, 0)
                for u in BOTH:
                    obuf[ab, lax.rem(2 * q + u, 4)] = term[:, u * PC : (u + 1) * PC].astype(jnp.bfloat16)
                for u in BOTH:
                    to_partner(2 * q + u, ab).start()

            @pl.when(q + 2 < steps)
            def _():
                for ab in BOTH:
                    load_away(q + 2, ab).start()

    def away_sent(q):
        i = lax.rem(q, 2)
        done(obuf.at[:, pl.ds(2 * i, 2)], s_o.at[i])

    def block(q, ab):
        i = lax.rem(q, NI)
        return sbuf.at[ab, pl.ds(2 * i, 2)]

    def terms_of(q, ab):
        return part.at[ab, pl.ds(2 * lax.rem(q, RING // 4), 2)]

    def end_sent(q):
        for ab in BOTH:
            done(block(q, ab), s_u.at[ab, lax.rem(q, NI)])

    def end_sum(q):
        with jax.named_scope("end_sum"):
            i = lax.rem(q, NI)

            @pl.when(q < NI)
            def _():
                for ab in BOTH:
                    load_wo(q, ab).wait()

            @pl.when(q >= NI)
            def _():
                end_sent(q - NI)

            for ab in BOTH:
                term = _dot(mine(lax.div(q, NI)), wo_s[i, ab], 1, 0)
                for u in BOTH:
                    n = 2 * q + u
                    if u == 0:
                        done(terms_of(q, ab), r_part.at[ab, lax.rem(q, RING // 4)])
                    some = term[:, u * PC : (u + 1) * PC] + part[ab, lax.rem(n, RING // 2)].astype(jnp.float32)
                    sbuf[ab, lax.rem(n, NP // 2)] = some.astype(jnp.bfloat16)
                if ab == 0:
                    to_inner(4 * q, 0).start()

                    @pl.when(q > 0)
                    def _():
                        to_inner(4 * q - 2, 1).start()

                    to_inner(4 * q + 1, 0).start()

                    @pl.when(q > 0)
                    def _():
                        to_inner(4 * q - 1, 1).start()

                    to_inner(4 * q + 2, 0).start()
                else:
                    to_inner(4 * q, 1).start()
                    to_inner(4 * q + 3, 0).start()
                    to_inner(4 * q + 1, 1).start()

                    @pl.when(q == steps - 1)
                    def _():
                        to_inner(4 * q + 2, 1).start()
                        to_inner(4 * q + 3, 1).start()

    def middle_pass(c, v):
        q, n, u = lax.div(c, 4), lax.div(c, 2), v // 2
        at = pl.ds(v % 2 * PR, PR)
        with jax.named_scope("pass_w"):
            if v == 0:
                @pl.when(q < NI)
                def _():
                    load_wo(q, 0).wait()

            if v == 0:
                done(terms_of(q, 0), r_part.at[0, lax.rem(q, RING // 4)])
            to_inner(c, 0).wait_recv()
        with jax.named_scope("pass"):
            term = _dot(s_s[lax.rem(chunk(c), 3), at, :], wo_s[lax.rem(q, NI), 0, :, u * PC : (u + 1) * PC], 1, 0)
            term = term + part[0, lax.rem(n, RING // 2), at, :].astype(jnp.float32) + from_e[0, ring(c)].astype(jnp.float32)
            sbuf[0, lax.rem(n, NP // 2), at, :] = term.astype(jnp.bfloat16)
            to_other(c).start()

    def middle_finish(c, v):
        q, n, u = lax.div(c, 4), lax.div(c, 2), v // 2
        at = pl.ds(v % 2 * PR, PR)
        with jax.named_scope("finish_w"):
            if v == 0:
                @pl.when(q < NI)
                def _():
                    load_wo(q, 1).wait()

                load_res(q).wait()
            if v == 0:
                done(terms_of(q, 1), r_part.at[1, lax.rem(q, RING // 4)])
            to_inner(c, 1).wait_recv()
            to_other(c).wait_recv()
        with jax.named_scope("finish"):
            term = _dot(s_s[lax.rem(chunk(c), 3), at, :], wo_s[lax.rem(q, NI), 1, :, u * PC : (u + 1) * PC], 1, 0)
            term = term + part[1, lax.rem(n, RING // 2), at, :].astype(jnp.float32)
            term = term + from_e[1, ring(c)].astype(jnp.float32) + from_m[lax.rem(c, 8)].astype(jnp.float32)
            term = term + xres[lax.rem(q, 2), at, u * PC : (u + 1) * PC].astype(jnp.float32)
            sbuf[1, lax.rem(n, NP // 2), at, :] = term.astype(jnp.bfloat16)
            result_to_outer(c, 1, held(1, c)).start()
            result_to_other(c).start()
            if v % 2 == 1:
                result_to_partner(n, 1, sbuf.at[1, lax.rem(n, NP // 2)], core).start()
                result_here(n).start()

    def middle_forward(c, v):
        src = y_at(c, core, 0)
        with jax.named_scope("forward_w"):
            done(from_m.at[0], r_mid.at[lax.rem(c, 8)])
        result_to_outer(c, 0, src).start()
        if v % 2 == 1:
            n = lax.div(c, 2)
            result_to_partner(n, 0, y_unit(n, core, 0), core).start()

    def middle_turn(t, j):
        s = 4 * t + j

        @pl.when(is_piece(s - 16) & middle)
        def _():
            middle_pass(s - 16, j)

        @pl.when(is_piece(s - 18) & middle)
        def _():
            middle_finish(s - 18, (j + 2) % 4)

        @pl.when(is_piece(s - 20) & middle)
        def _():
            middle_forward(s - 20, j)

    def norms(first, k):
        def one(i, carry):
            b = first + i
            with jax.named_scope("x_w"):
                load_x(b).wait()
            slot = lax.rem(b, NI)

            def squares(j, total):
                at = pl.ds(pl.multiple_of(j * WIDE, WIDE), WIDE)
                for g in range(XR // ROWS):
                    wide = xb[slot, g * ROWS : g * ROWS + ROWS, at].astype(jnp.float32)
                    wide = wide * wide
                    some = wide[:, :HEAD]
                    for n in range(1, 8):
                        some = some + wide[:, n * HEAD : (n + 1) * HEAD]
                    total = total[:g] + (total[g] + some,) + total[g + 1 :]
                return total

            total = lax.fori_loop(0, d // WIDE, squares, (jnp.zeros((ROWS, HEAD), jnp.float32),) * (XR // ROWS))
            sizes = [lax.rsqrt(jnp.sum(v, -1, keepdims=True) / d + 1e-6) for v in total]
            sizes = tuple(jnp.broadcast_to(v, (ROWS, HEAD)) for v in sizes)

            def scaled(j, sizes):
                at = pl.ds(pl.multiple_of(j * WIDE, WIDE), WIDE)
                for g in range(XR // ROWS):
                    wide = xb[slot, g * ROWS : g * ROWS + ROWS, at].astype(jnp.float32)
                    wide = wide * jnp.concatenate([sizes[g]] * 8, axis=1)
                    wide = wide.reshape(2, 8, WIDE) * gain_s[:, at][None]
                    a_s[k, pl.ds(pl.multiple_of(i * XR + g * ROWS, ROWS), ROWS), at] = wide.reshape(ROWS, WIDE).astype(jnp.bfloat16)
                return sizes

            lax.fori_loop(0, d // WIDE, scaled, sizes)
            angles(b)
            if k == 0:
                @pl.when(b == 0)
                def _():
                    for kb in (2, 3):
                        for m in range(3):
                            load_w(0, kb, m).start()
            else:
                more_x(b + NI)
            return carry

        lax.fori_loop(0, NI, one, 0)

    def step(t, carry):
        def is_block(q):
            return (q >= 0) & (q < steps)

        @pl.when(is_block(t - 8) & middle)
        def _():
            q = t - 8
            done(block(q, 0), s_u.at[0, lax.rem(q, NI)])
            for sem in (s_u.at[1], s_e.at[1], s_p.at[1], s_l):
                done(block(q, 1), sem.at[lax.rem(q, NI)])

        @pl.when(is_block(t - 9) & middle)
        def _():
            q = t - 9
            for sem in (s_e, s_p):
                done(block(q, 0), sem.at[0, lax.rem(q, NI)])

        @pl.when(is_block(t - 4) & middle)
        def _():
            load_res(t - 4).start()

        first = t == NI - 1

        @pl.when(first)
        def _():
            for ab in BOTH:
                load_away(0, ab).start()
                load_wo(0, ab).start()

        @pl.when((t == NI) | (t == NI + 1))
        def _():
            for ab in BOTH:
                load_wo(t - 2, ab).start()

        ahead = (t >= NI) & (t + NI < steps)
        middle_turn(t, 0)

        @pl.when(ahead)
        def _():
            with jax.named_scope("project0"):
                project(t, 0, True)

        @pl.when(jnp.logical_not(ahead) & (t < steps))
        def _():
            with jax.named_scope("project0_"):
                project(t, 0, False)

        @pl.when(first)
        def _():
            for ab in BOTH:
                load_away(1, ab).start()
                load_wo(1, ab).start()
            for b in range(NI, 2 * NI):
                load_x(b).start()

        middle_turn(t, 1)

        @pl.when(t < steps)
        def _():
            with jax.named_scope("project1"):
                project(t, 1, False)

        @pl.when(first)
        def _():
            more_w(t, 0)

        @pl.when(t < steps)
        def _():
            with jax.named_scope("rotate"):
                rotate(t)

        middle_turn(t, 2)

        @pl.when((t >= NI) & (t < steps))
        def _():
            with jax.named_scope("attend"):
                attend(t)

        @pl.when(first)
        def _():
            with jax.named_scope("attend_first"):
                attend_first()
            more_w(t, 1)

        middle_turn(t, 3)
        i = lax.rem(t, NI)

        @pl.when(is_block(t - 3) & (i == NI - 1))
        def _():
            send_away(t - 3)

            @pl.when(end)
            def _():
                end_sum(t - 3)

        @pl.when(is_block(t - 2) & (i != NI - 2))
        def _():
            send_away(t - 2)

            @pl.when(end)
            def _():
                end_sum(t - 2)

        @pl.when(t == NI - 1)
        def _():
            with jax.named_scope("norm1"):
                norms(NI, 1)

        @pl.when(is_block(t - 8) & end)
        def _():
            for ab in (1, 0):
                with jax.named_scope("result_w"):
                    done(block(t - 8, ab), r_end.at[ab, lax.rem(t - 8, RING // 4)])
                for u in BOTH:
                    n = 2 * (t - 8) + u
                    result_to_partner(n, ab, y_unit(n, core, ab), core).start()

        @pl.when(is_block(t - 9) & end)
        def _():
            for ab in BOTH:
                done(block(t - 9, ab), s_p.at[ab, lax.rem(t - 9, NI)])

        @pl.when(t == steps + 2)
        def _():
            for n in range(len(stash()) - NI):
                keep(n).start()

        @pl.when(t == steps + 6)
        def _():
            for n in range(len(stash()) - NI, len(stash())):
                keep(n).start()

        @pl.when(is_block(t - 9))
        def _():
            with jax.named_scope("y_w"):
                for ab in BOTH:
                    done(block(t - 9, ab), r_y.at[ab, lax.rem(t - 9, RING // 4)])

        return carry

    with jax.named_scope("angles"):
        first_angles()
    with jax.named_scope("norm0"):
        norms(0, 0)

    with jax.named_scope("barrier"):
        @pl.when(end)
        def _():
            pl.semaphore_wait(barrier, 2)

        @pl.when(middle)
        def _():
            pl.semaphore_wait(barrier, 3)

    lax.fori_loop(0, steps + 9, step, 0)
    done(y_ref.at[pl.ds(0, rows - R)], keep_sem)

    for q in range(steps - 2, steps):
        away_sent(q)

    @pl.when(end)
    def _():
        for q in range(steps - NI, steps):
            end_sent(q)


def solution(mesh):
    def step(x, gain, wq, wk, wv, wo):
        rows, d = x.shape
        own = wq.shape[1]
        chunks = rows // R
        half = HEAD // 2
        freq = np.float32(THETA) ** (-np.arange(half, dtype=np.float32) / half)
        freq = jnp.asarray(np.concatenate([freq, freq])[None], jnp.float32)
        bf16, f32 = jnp.bfloat16, jnp.float32
        hbm = pl.BlockSpec(memory_space=pl.ANY)
        vmem = pl.BlockSpec(memory_space=pltpu.VMEM)
        dma = pltpu.SemaphoreType.DMA
        parts = [((NI, XR, d), "xb"), ((2, R, d), "a"), ((NB, KB, 768), "w"), ((rows, own), "k")]
        y, *kept = pl.pallas_call(
            _kernel,
            out_shape=[jax.ShapeDtypeStruct((rows, d), bf16)] + [pltpu.VMEM(shape, bf16) for shape, _ in parts],
            in_specs=[hbm, vmem, vmem, hbm, hbm, hbm, hbm],
            out_specs=[hbm] + [vmem] * 4,
            scratch_shapes=[
                pltpu.VMEM((8, d), f32),
                pltpu.VMEM((XR, d), bf16),
                pltpu.VMEM((R, 768), f32),
                pltpu.VMEM((NI, 2, own, 2 * PC), bf16),
                pltpu.VMEM((own // HEAD, HEAD + 8, rows), bf16),
                pltpu.VMEM((3, R, own), bf16),
                pltpu.VMEM((own // HEAD, R, HEAD), bf16),
                pltpu.VMEM((2, R, HEAD), f32),
                pltpu.VMEM((2, R, HEAD), f32),
                pltpu.VMEM((2, R, HEAD), f32),
                pltpu.VMEM((2, 1, R), f32),
                pltpu.VMEM((2, HEAD + 8, R), f32),
                pltpu.VMEM((2, RING // 2, R, PC), bf16),
                pltpu.VMEM((2, RING, PR, PC), bf16),
                pltpu.VMEM((8, PR, PC), bf16),
                pltpu.VMEM((2, 4, R, PC), bf16),
                pltpu.VMEM((2, NP // 2, R, PC), bf16),
                pltpu.VMEM((2, R, 2 * PC), bf16),
                pltpu.VMEM((2, 2, own, 2 * PC), bf16),
                dma((NI,)),
                dma((NB,)),
                dma((NI, 2)),
                dma((2, 2)),
                dma((2,)),
                dma((2, RING // 4)),
                dma((2, RING)),
                dma((8,)),
                dma((2, RING // 4)),
                dma((8,)),
                dma((2, RING // 4)),
                dma((2,)),
                dma((2, NI)),
                dma((2, NI)),
                dma((2, NI)),
                dma((NI,)),
                dma,
            ],
            compiler_params=pltpu.CompilerParams(collective_id=1, has_side_effects=True, vmem_limit_bytes=VMEM),
            name="layer",
        )(x, gain, freq, wq, wk, wv, wo)
        return pl.pallas_call(
            _gather,
            out_shape=jax.ShapeDtypeStruct((rows, d), bf16),
            in_specs=[hbm] + [vmem] * 4,
            out_specs=hbm,
            scratch_shapes=[pltpu.VMEM((4, R // 4, d), bf16), dma((4,)), dma((4,)), dma((20,))],
            compiler_params=pltpu.CompilerParams(vmem_limit_bytes=9 * 2**19),
            name="gather",
        )(y, *kept)

    tokens, columns = P("dp", None), P(None, "tp")
    return jax.shard_map(
        step,
        mesh=mesh,
        in_specs=(tokens, P(None), columns, columns, columns, P("tp", None)),
        out_specs=tokens,
        check_vma=False,
    )
```

```python
import functools

import jax
import jax.numpy as jnp
import numpy as np
from jax import lax
from jax.experimental import pallas as pl
from jax.experimental.pallas import tpu as pltpu
from jax.sharding import PartitionSpec as P

HEAD = 128
THETA = 10000
NEG = -1e30
HIDDEN = 2 * NEG
LOG2E = 1.4426950408889634
VMEM = 63 * 2**19
R = 256
KB = 2048
PC = 256
NB = 4
XR = R // 4
KEYS = 512
BOTH = (0, 1)
ROWS = 16
WIDE = 1024
PR = R // 2
NI = 4
NP = 4 * NI
RING = 32
MESH = pl.DeviceIdType.MESH


def _dot(a, b, ca, cb):
    return lax.dot_general(a, b, (((ca,), (cb,)), ((), ())), preferred_element_type=jnp.float32)


def _parts(xb, a_s, wbuf, k_s):
    half = KB // 2
    some = [((pl.ds(0, half), pl.ds((2 * kb + n) * 768, 768)), wbuf.at[kb, pl.ds(n * half, half)]) for kb in range(NB) for n in BOTH]
    some += [((pl.ds(0, half), pl.ds(2 * NB * 768 + n * 1024, 1024)), k_s.at[pl.ds(n * half, half)]) for n in BOTH]
    some += [((pl.ds(half + n * R, R), slice(None)), a_s.at[n]) for n in BOTH]
    return some + [((pl.ds(half + 2 * R + n * XR, XR), slice(None)), xb.at[n]) for n in range(NI)]


def _columns(d, i):
    return [pl.ds((side + side + g) * (d // NI) + i * 2 * PC, 2 * PC) for side in BOTH for g in BOTH]


def _late(rows, d, vt_s, i):
    tiles = [(pl.ds(rows - R + r * PR, PR), at) for at in _columns(d, i) for r in BOTH]
    return [(at, vt_s.at[2 * i + n // NI, :HEAD, pl.ds(n % NI * 2 * PC, 2 * PC)]) for n, at in enumerate(tiles)]


def _gather(y_ref, xb, a_s, wbuf, k_s, vt_s, out_ref, buf, i_sem, o_sem, sem):
    rows, d = y_ref.shape
    last = [(pl.ds(rows - R, R), at) for i in (2, 3) for at in _columns(d, i)]
    loads = [pltpu.make_async_copy(y_ref.at[at], buf.at[b], i_sem.at[b]) for b, at in enumerate(last)]
    stores = [pltpu.make_async_copy(buf.at[b], out_ref.at[at], o_sem.at[b]) for b, at in enumerate(last)]
    parts = _parts(xb, a_s, wbuf, k_s)
    for i in BOTH:
        parts += _late(rows, d, vt_s, i)
    kept = [pltpu.make_async_copy(ref, out_ref.at[at], sem.at[i]) for i, (at, ref) in enumerate(parts)]
    for copy in loads + kept:
        copy.start()
    for load, store in zip(loads, stores):
        load.wait()
        store.start()
    for copy in stores + kept:
        copy.wait()


def _kernel(x_ref, gain_ref, freq_ref, wq_ref, wk_ref, wv_ref, wo_ref, y_ref, xb, a_s, wbuf, k_s, vt_s,
            gain_s, stage_s, acc_s, wo_s, s_s, q_s, turns_s, cos_s, sin_s, top_s, mix_s,
            part, from_e, from_m, obuf, sbuf, xres, away_s,
            x_sem, w_sem, wo_sem, away_sem, xr_sem, r_part, r_e, r_m, r_end, r_mid, r_y, s_o, s_u, s_e, s_p, s_l, keep_sem):
    rows, d = x_ref.shape
    chunks = rows // R
    steps = chunks * NI
    pieces = chunks * NP
    scale = HEAD**-0.5
    e = scale * LOG2E
    tp = lax.axis_index("tp")
    z, core = lax.div(tp, 2), lax.rem(tp, 2)
    middle = (z == 1) | (z == 2)
    end = jnp.logical_not(middle)
    partner = z * 2 + 1 - core
    inner = jnp.where(z < 2, 1, 2) * 2 + core
    outer = jnp.where(z < 2, 0, 3) * 2 + core
    other = (3 - z) * 2 + core
    near = jnp.where(z < 2, 0, 1)
    half = d // 2
    quarter = d // 4

    def col(side, ab, i):
        g = near if ab == 1 else 1 - near
        return pl.multiple_of(side * half + g * quarter + i * PC, PC)

    def chunk(c):
        return lax.div(c, NP)

    def ring(c):
        return lax.rem(c, RING)

    def unit(c):
        return lax.div(lax.rem(c, NP), 2), pl.ds(pl.multiple_of(lax.rem(c, 2) * PR, PR), PR)

    def row(k):
        return pl.ds(pl.multiple_of(k * R, R), R)

    def remote(src, dst, send, recv, to):
        return pltpu.make_async_remote_copy(src, dst, send, recv, device_id={"tp": to}, device_id_type=MESH)

    def stash():
        return _parts(xb, a_s, wbuf, k_s)

    def keep(n):
        at, ref = stash()[n]
        return pltpu.make_async_copy(y_ref.at[at], ref, keep_sem.at[0])

    def keep_late(i):
        for at, ref in _late(rows, d, vt_s, i):
            pltpu.make_async_copy(y_ref.at[at], ref, keep_sem.at[1]).start()

    def done(ref, sem):
        pltpu.make_async_copy(ref, ref, sem).wait()

    def is_piece(c):
        return (c >= 0) & (c < pieces)

    def load_x(b):
        slot = lax.rem(b, NI)
        return pltpu.make_async_copy(x_ref.at[pl.ds(pl.multiple_of(b * XR, XR), XR)], xb.at[slot], x_sem.at[slot])

    def load_w(t, kb, m):
        w = (wq_ref, wk_ref, wv_ref)[m]
        i = lax.rem(t, NI)
        return pltpu.make_async_copy(
            w.at[pl.ds(kb * KB, KB), pl.ds(pl.multiple_of(i * 256, 256), 256)],
            wbuf.at[kb, :, pl.ds(m * 256, 256)], w_sem.at[kb])

    def load_away(q, ab):
        slot = lax.rem(q, 2)
        at = pl.ds(col(1 - core, ab, 2 * lax.rem(q, NI)), 2 * PC)
        return pltpu.make_async_copy(wo_ref.at[:, at], away_s.at[slot, ab], away_sem.at[slot, ab])

    def load_wo(i, ab):
        at = pl.ds(col(core, ab, 2 * i), 2 * PC)
        return pltpu.make_async_copy(wo_ref.at[:, at], wo_s.at[i, ab], wo_sem.at[i, ab])

    def load_res(q):
        slot, i = lax.rem(q, 2), lax.rem(q, NI)
        return pltpu.make_async_copy(
            x_ref.at[row(lax.div(q, NI)), pl.ds(col(core, 1, 2 * i), 2 * PC)], xres.at[slot], xr_sem.at[slot])

    def to_partner(n, ab):
        p, r = lax.rem(n, 4), lax.rem(n, RING // 2)
        return remote(obuf.at[ab, p], part.at[ab, r], s_o.at[lax.div(p, 2)], r_part.at[ab, lax.div(r, 2)], partner)

    def turn_of(c):
        return lax.rem(lax.div(c, 4), NI)

    def held(ab, c):
        i, at = unit(c)
        return sbuf.at[ab, i, at]

    def to_inner(c, ab):
        return remote(held(ab, c), from_e.at[ab, ring(c)], s_u.at[ab, turn_of(c)], r_e.at[ab, ring(c)], inner)

    def to_other(c):
        p = lax.rem(c, 8)
        return remote(held(0, c), from_m.at[p], s_u.at[0, turn_of(c)], r_m.at[p], other)

    def y_at(c, side, ab):
        i, _ = unit(c)
        at = pl.ds(pl.multiple_of(chunk(c) * R + lax.rem(c, 2) * PR, PR), PR)
        return y_ref.at[at, pl.ds(col(side, ab, i), PC)]

    def y_unit(n, side, ab):
        return y_ref.at[row(lax.div(n, NP // 2)), pl.ds(col(side, ab, lax.rem(n, NP // 2)), PC)]

    def result_to_other(c):
        return remote(held(1, c), y_at(c, core, 1), s_u.at[1, turn_of(c)], r_mid.at[lax.rem(c, 8)], other)

    def result_to_outer(c, ab, src):
        return remote(src, y_at(c, core, ab), s_e.at[ab, turn_of(c)], r_end.at[ab, lax.div(ring(c), 4)], outer)

    def result_to_partner(n, ab, src, side):
        q = lax.div(n, 2)
        return remote(src, y_unit(n, side, ab), s_p.at[ab, lax.rem(q, NI)], r_y.at[ab, lax.rem(q, RING // 4)], partner)

    def result_here(n):
        i = lax.rem(n, NP // 2)
        return pltpu.make_async_copy(sbuf.at[1, i], y_unit(n, core, 1), s_l.at[lax.rem(lax.div(n, 2), NI)])

    barrier = pltpu.get_barrier_semaphore()

    def greet(to):
        pl.semaphore_signal(barrier, inc=1, device_id={"tp": to}, device_id_type=MESH)

    for b in range(NI):
        load_x(b).start()
    greet(partner)

    @pl.when(end)
    def _():
        greet(inner)

    @pl.when(middle)
    def _():
        greet(outer)
        greet(other)

    gain_s[...] = jnp.broadcast_to(gain_ref[...].astype(jnp.float32)[None], gain_s.shape)

    for h in range(2 * NI):
        vt_s[h, HEAD:, :] = jnp.ones((8, rows), jnp.bfloat16)
    for kb in BOTH:
        for m in range(3):
            load_w(0, kb, m).start()

    def norm(b, to, top):
        slot = lax.rem(b, NI)
        sizes = []
        for g in range(XR // ROWS):
            wide = xb[slot, g * ROWS : g * ROWS + ROWS, :].astype(jnp.float32)
            sizes.append(lax.rsqrt(jnp.mean(wide * wide, -1, keepdims=True) + 1e-6))
        for g, size in enumerate(sizes):
            wide = xb[slot, g * ROWS : g * ROWS + ROWS, :].astype(jnp.float32) * size
            wide = wide.reshape(2, 8, d) * gain_s[...][None]
            to[pl.ds(pl.multiple_of(top + g * ROWS, ROWS), ROWS), :] = wide.reshape(ROWS, d).astype(jnp.bfloat16)
        angles(b)

    sign = jnp.where(lax.broadcasted_iota(jnp.int32, (8, HEAD), 1) < HEAD // 2, -1.0, 1.0)

    def angles(b):
        k, i = lax.div(b, NI), lax.rem(b, NI)
        here = pl.ds(pl.multiple_of(i * XR, XR), XR)
        angle = jnp.full((8, HEAD), k * R, jnp.int32).astype(jnp.float32) * freq_ref[...]
        c, s = jnp.cos(angle)[:1], (jnp.sin(angle) * sign)[:1]
        cos, sin = turns_s[0, here, :], turns_s[1, here, :]
        cos_s[lax.rem(k, 2), here, :] = cos * c - sin * s
        sin_s[lax.rem(k, 2), here, :] = sin * c + cos * s

    def first_angles():
        token = lax.broadcasted_iota(jnp.int32, (R, HEAD), 0).astype(jnp.float32)
        angle = token * freq_ref[...]
        turns_s[0] = jnp.cos(angle)
        turns_s[1] = jnp.sin(angle) * jnp.concatenate([sign] * (R // 8), axis=0)

    def more_x(b):
        @pl.when(b < steps)
        def _():
            load_x(b).start()

    def project(t, part, ahead):
        p = lax.rem(lax.div(t, NI), 2)
        blocks = (2 * part, 2 * part + 1)
        for kb in blocks:
            done(wbuf.at[kb], w_sem.at[kb])
        if ahead:
            load_x(t + NI).wait()
            norm(t + NI, stage_s, 0)
        for kb in blocks:
            some = _dot(a_s[p, :, kb * KB : (kb + 1) * KB], wbuf[kb], 1, 0)
            acc_s[...] = some if kb == 0 else acc_s[...] + some
        if ahead:
            k, at = lax.rem(lax.div(t + NI, NI), 2), lax.rem(t, NI) * XR
            a_s[k, pl.ds(pl.multiple_of(at, XR), XR), :] = stage_s[...]
            more_x(t + 2 * NI)

        @pl.when((t + 1 < steps) & (t != NI - 1))
        def _():
            more_w(t, part)

    def more_w(t, part):
        for kb in (2 * part, 2 * part + 1):
            for m in range(3):
                load_w(t + 1, kb, m).start()

    def rotate(t):
        k, i = lax.div(t, NI), lax.rem(t, NI)
        p = lax.rem(k, 2)
        lane = lambda h: pl.ds(pl.multiple_of(i * 256 + h * HEAD, HEAD), HEAD)

        def turned(at):
            one = acc_s[:, at : at + HEAD].astype(jnp.bfloat16).astype(jnp.float32)
            return (one * cos_s[p] + pltpu.roll(one, HEAD // 2, 1) * sin_s[p]).astype(jnp.bfloat16)

        for h in BOTH:
            q_s[2 * i + h] = turned(h * HEAD)
            k_s[row(k), lane(h)] = turned(256 + h * HEAD)
            vt_s[2 * i + h, :HEAD, row(k)] = acc_s[:, 512 + h * HEAD : 512 + (h + 1) * HEAD].astype(jnp.bfloat16).T

    def attend(t):
        k, i = lax.div(t, NI), lax.rem(t, NI)
        lane = lambda h: pl.ds(pl.multiple_of(i * 256 + h * HEAD, HEAD), HEAD)
        for h in BOTH:
            top_s[h] = jnp.full((1, R), NEG, jnp.float32)
            mix_s[h] = jnp.zeros((HEAD + 8, R), jnp.float32)

        def block(first, keys, masked):
            here = pl.ds(pl.multiple_of(first, keys), keys)
            scores = [_dot(k_s[here, lane(h)], q_s[2 * i + h], 1, 1) for h in BOTH]
            if masked:
                gap = lax.broadcasted_iota(jnp.int32, (keys, R), 1) - lax.broadcasted_iota(jnp.int32, (keys, R), 0)
                seen = gap >= first - k * R
                scores = [jnp.where(seen, s, HIDDEN) for s in scores]
            weights, keeps = [], []
            for h, s in enumerate(scores):
                old = top_s[h]
                top = jnp.maximum(old, s.max(axis=0, keepdims=True))
                top_s[h] = top
                weights.append(jnp.exp2((s - top) * e).astype(jnp.bfloat16))
                keeps.append(jnp.exp2((old - top) * e))
            for h in BOTH:
                mix_s[h] = mix_s[h] * keeps[h] + _dot(vt_s[2 * i + h, :, here], weights[h], 1, 0)

        whole = lax.div(k * R, KEYS)

        def plain(j, carry):
            block(j * KEYS, KEYS, False)
            return carry

        lax.fori_loop(0, whole, plain, 0)

        @pl.when(lax.rem(k, 2) == 1)
        def _():
            block(whole * KEYS, KEYS, True)

        @pl.when(lax.rem(k, 2) == 0)
        def _():
            block(k * R, R, True)

        for h in BOTH:
            out = mix_s[h, :HEAD, :] * (1 / mix_s[h, HEAD : HEAD + 1, :])
            s_s[lax.rem(k, 3), :, lane(h)] = out.T.astype(jnp.bfloat16)

    def attend_first():
        gap = lax.broadcasted_iota(jnp.int32, (R, R), 1) - lax.broadcasted_iota(jnp.int32, (R, R), 0)
        heads = range(2 * NI)
        scores = [_dot(k_s[:R, h * HEAD : (h + 1) * HEAD], q_s[h], 1, 1) for h in heads]
        weights = []
        for s in scores:
            s = jnp.where(gap >= 0, s, HIDDEN)
            weights.append(jnp.exp2((s - s.max(axis=0, keepdims=True)) * e).astype(jnp.bfloat16))
        for h in heads:
            mix = _dot(vt_s[h, :, :R], weights[h], 1, 0)
            out = mix[:HEAD] * (1 / mix[HEAD : HEAD + 1])
            s_s[0, :, h * HEAD : (h + 1) * HEAD] = out.T.astype(jnp.bfloat16)

    def mine(k):
        return s_s[lax.rem(k, 3)]

    def send_away(q):
        with jax.named_scope("away"):
            @pl.when(q >= 2)
            def _():
                away_sent(q - 2)

            for ab in BOTH:
                load_away(q, ab).wait()
                term = _dot(mine(lax.div(q, NI)), away_s[lax.rem(q, 2), ab], 1, 0)
                for u in BOTH:
                    obuf[ab, lax.rem(2 * q + u, 4)] = term[:, u * PC : (u + 1) * PC].astype(jnp.bfloat16)
                for u in BOTH:
                    to_partner(2 * q + u, ab).start()

            @pl.when(q + 2 < steps)
            def _():
                for ab in BOTH:
                    load_away(q + 2, ab).start()

    def away_sent(q):
        i = lax.rem(q, 2)
        done(obuf.at[:, pl.ds(2 * i, 2)], s_o.at[i])

    def block(q, ab):
        i = lax.rem(q, NI)
        return sbuf.at[ab, pl.ds(2 * i, 2)]

    def terms_of(q, ab):
        return part.at[ab, pl.ds(2 * lax.rem(q, RING // 4), 2)]

    def end_sent(q):
        for ab in BOTH:
            done(block(q, ab), s_u.at[ab, lax.rem(q, NI)])

    def end_sum(q):
        with jax.named_scope("end_sum"):
            i = lax.rem(q, NI)

            @pl.when(q < NI)
            def _():
                for ab in BOTH:
                    load_wo(q, ab).wait()

            @pl.when(q >= NI)
            def _():
                end_sent(q - NI)

            for ab in BOTH:
                term = _dot(mine(lax.div(q, NI)), wo_s[i, ab], 1, 0)
                for u in BOTH:
                    n = 2 * q + u
                    if u == 0:
                        done(terms_of(q, ab), r_part.at[ab, lax.rem(q, RING // 4)])
                    some = term[:, u * PC : (u + 1) * PC] + part[ab, lax.rem(n, RING // 2)].astype(jnp.float32)
                    sbuf[ab, lax.rem(n, NP // 2)] = some.astype(jnp.bfloat16)
                if ab == 0:
                    to_inner(4 * q, 0).start()

                    @pl.when(q > 0)
                    def _():
                        to_inner(4 * q - 2, 1).start()

                    to_inner(4 * q + 1, 0).start()

                    @pl.when(q > 0)
                    def _():
                        to_inner(4 * q - 1, 1).start()

                    to_inner(4 * q + 2, 0).start()
                else:
                    to_inner(4 * q, 1).start()
                    to_inner(4 * q + 3, 0).start()
                    to_inner(4 * q + 1, 1).start()

                    @pl.when(q == steps - 1)
                    def _():
                        to_inner(4 * q + 2, 1).start()
                        to_inner(4 * q + 3, 1).start()

    def middle_pass(c, v):
        q, n, u = lax.div(c, 4), lax.div(c, 2), v // 2
        at = pl.ds(v % 2 * PR, PR)
        with jax.named_scope("pass_w"):
            if v == 0:
                @pl.when(q < NI)
                def _():
                    load_wo(q, 0).wait()

            if v == 0:
                done(terms_of(q, 0), r_part.at[0, lax.rem(q, RING // 4)])
            to_inner(c, 0).wait_recv()
        with jax.named_scope("pass"):
            term = _dot(s_s[lax.rem(chunk(c), 3), at, :], wo_s[lax.rem(q, NI), 0, :, u * PC : (u + 1) * PC], 1, 0)
            term = term + part[0, lax.rem(n, RING // 2), at, :].astype(jnp.float32) + from_e[0, ring(c)].astype(jnp.float32)
            sbuf[0, lax.rem(n, NP // 2), at, :] = term.astype(jnp.bfloat16)
            to_other(c).start()

    def middle_finish(c, v):
        q, n, u = lax.div(c, 4), lax.div(c, 2), v // 2
        at = pl.ds(v % 2 * PR, PR)
        with jax.named_scope("finish_w"):
            if v == 0:
                @pl.when(q < NI)
                def _():
                    load_wo(q, 1).wait()

                load_res(q).wait()
            if v == 0:
                done(terms_of(q, 1), r_part.at[1, lax.rem(q, RING // 4)])
            to_inner(c, 1).wait_recv()
            to_other(c).wait_recv()
        with jax.named_scope("finish"):
            term = _dot(s_s[lax.rem(chunk(c), 3), at, :], wo_s[lax.rem(q, NI), 1, :, u * PC : (u + 1) * PC], 1, 0)
            term = term + part[1, lax.rem(n, RING // 2), at, :].astype(jnp.float32)
            term = term + from_e[1, ring(c)].astype(jnp.float32) + from_m[lax.rem(c, 8)].astype(jnp.float32)
            term = term + xres[lax.rem(q, 2), at, u * PC : (u + 1) * PC].astype(jnp.float32)
            sbuf[1, lax.rem(n, NP // 2), at, :] = term.astype(jnp.bfloat16)
            result_to_outer(c, 1, held(1, c)).start()
            result_to_other(c).start()
            if v % 2 == 1:
                result_to_partner(n, 1, sbuf.at[1, lax.rem(n, NP // 2)], core).start()
                result_here(n).start()

    def middle_forward(c, v):
        src = y_at(c, core, 0)
        with jax.named_scope("forward_w"):
            done(from_m.at[0], r_mid.at[lax.rem(c, 8)])
        result_to_outer(c, 0, src).start()
        if v % 2 == 1:
            n = lax.div(c, 2)
            result_to_partner(n, 0, y_unit(n, core, 0), core).start()

    def middle_turn(t, j):
        s = 4 * t + j

        @pl.when(is_piece(s - 16) & middle)
        def _():
            middle_pass(s - 16, j)

        @pl.when(is_piece(s - 18) & middle)
        def _():
            middle_finish(s - 18, (j + 2) % 4)

        @pl.when(is_piece(s - 20) & middle)
        def _():
            middle_forward(s - 20, j)

    def norms(first, k):
        def one(i, carry):
            b = first + i
            with jax.named_scope("x_w"):
                load_x(b).wait()
            slot = lax.rem(b, NI)

            def squares(j, total):
                at = pl.ds(pl.multiple_of(j * WIDE, WIDE), WIDE)
                for g in range(XR // ROWS):
                    wide = xb[slot, g * ROWS : g * ROWS + ROWS, at].astype(jnp.float32)
                    wide = wide * wide
                    some = wide[:, :HEAD]
                    for n in range(1, 8):
                        some = some + wide[:, n * HEAD : (n + 1) * HEAD]
                    total = total[:g] + (total[g] + some,) + total[g + 1 :]
                return total

            total = lax.fori_loop(0, d // WIDE, squares, (jnp.zeros((ROWS, HEAD), jnp.float32),) * (XR // ROWS))
            sizes = [lax.rsqrt(jnp.sum(v, -1, keepdims=True) / d + 1e-6) for v in total]
            sizes = tuple(jnp.broadcast_to(v, (ROWS, HEAD)) for v in sizes)

            def scaled(j, sizes):
                at = pl.ds(pl.multiple_of(j * WIDE, WIDE), WIDE)
                for g in range(XR // ROWS):
                    wide = xb[slot, g * ROWS : g * ROWS + ROWS, at].astype(jnp.float32)
                    wide = wide * jnp.concatenate([sizes[g]] * 8, axis=1)
                    wide = wide.reshape(2, 8, WIDE) * gain_s[:, at][None]
                    a_s[k, pl.ds(pl.multiple_of(i * XR + g * ROWS, ROWS), ROWS), at] = wide.reshape(ROWS, WIDE).astype(jnp.bfloat16)
                return sizes

            lax.fori_loop(0, d // WIDE, scaled, sizes)
            angles(b)
            if k == 0:
                @pl.when(b == 0)
                def _():
                    for kb in (2, 3):
                        for m in range(3):
                            load_w(0, kb, m).start()
            else:
                more_x(b + NI)
            return carry

        lax.fori_loop(0, NI, one, 0)

    def step(t, carry):
        def is_block(q):
            return (q >= 0) & (q < steps)

        @pl.when(is_block(t - 8) & middle)
        def _():
            q = t - 8
            done(block(q, 0), s_u.at[0, lax.rem(q, NI)])
            for sem in (s_u.at[1], s_e.at[1], s_p.at[1], s_l):
                done(block(q, 1), sem.at[lax.rem(q, NI)])

        @pl.when(is_block(t - 9) & middle)
        def _():
            q = t - 9
            for sem in (s_e, s_p):
                done(block(q, 0), sem.at[0, lax.rem(q, NI)])

        @pl.when(is_block(t - 4) & middle)
        def _():
            load_res(t - 4).start()

        first = t == NI - 1

        @pl.when(first)
        def _():
            for ab in BOTH:
                load_away(0, ab).start()
                load_wo(0, ab).start()

        @pl.when((t == NI) | (t == NI + 1))
        def _():
            for ab in BOTH:
                load_wo(t - 2, ab).start()

        ahead = (t >= NI) & (t + NI < steps)
        middle_turn(t, 0)

        @pl.when(ahead)
        def _():
            with jax.named_scope("project0"):
                project(t, 0, True)

        @pl.when(jnp.logical_not(ahead) & (t < steps))
        def _():
            with jax.named_scope("project0_"):
                project(t, 0, False)

        @pl.when(first)
        def _():
            for ab in BOTH:
                load_away(1, ab).start()
                load_wo(1, ab).start()
            for b in range(NI, 2 * NI):
                load_x(b).start()

        middle_turn(t, 1)

        @pl.when(t < steps)
        def _():
            with jax.named_scope("project1"):
                project(t, 1, False)

        @pl.when(first)
        def _():
            more_w(t, 0)

        @pl.when(t < steps)
        def _():
            with jax.named_scope("rotate"):
                rotate(t)

        middle_turn(t, 2)

        @pl.when((t >= NI) & (t < steps))
        def _():
            with jax.named_scope("attend"):
                attend(t)

        @pl.when(first)
        def _():
            with jax.named_scope("attend_first"):
                attend_first()
            more_w(t, 1)

        middle_turn(t, 3)
        i = lax.rem(t, NI)

        @pl.when(is_block(t - 3) & (i == NI - 1))
        def _():
            send_away(t - 3)

            @pl.when(end)
            def _():
                end_sum(t - 3)

        @pl.when(is_block(t - 2) & (i != NI - 2))
        def _():
            send_away(t - 2)

            @pl.when(end)
            def _():
                end_sum(t - 2)

        @pl.when(t == NI - 1)
        def _():
            with jax.named_scope("norm1"):
                norms(NI, 1)

        @pl.when(is_block(t - 8) & end)
        def _():
            for ab in (1, 0):
                with jax.named_scope("result_w"):
                    done(block(t - 8, ab), r_end.at[ab, lax.rem(t - 8, RING // 4)])
                for u in BOTH:
                    n = 2 * (t - 8) + u
                    result_to_partner(n, ab, y_unit(n, core, ab), core).start()

        @pl.when(is_block(t - 9) & end)
        def _():
            for ab in BOTH:
                done(block(t - 9, ab), s_p.at[ab, lax.rem(t - 9, NI)])

        @pl.when(t == steps + 2)
        def _():
            for n in range(len(stash()) - NI):
                keep(n).start()

        for i in BOTH:
            @pl.when(t == steps + 6 + i)
            def _(i=i):
                keep_late(i)

        @pl.when(t == steps + 6)
        def _():
            for n in range(len(stash()) - NI, len(stash())):
                keep(n).start()

        @pl.when(is_block(t - 9))
        def _():
            with jax.named_scope("y_w"):
                for ab in BOTH:
                    done(block(t - 9, ab), r_y.at[ab, lax.rem(t - 9, RING // 4)])

        return carry

    with jax.named_scope("angles"):
        first_angles()
    with jax.named_scope("norm0"):
        norms(0, 0)

    with jax.named_scope("barrier"):
        @pl.when(end)
        def _():
            pl.semaphore_wait(barrier, 2)

        @pl.when(middle)
        def _():
            pl.semaphore_wait(barrier, 3)

    lax.fori_loop(0, steps + 9, step, 0)
    done(y_ref.at[pl.ds(0, rows - R)], keep_sem.at[0])
    done(y_ref.at[pl.ds(0, PR)], keep_sem.at[1])

    for q in range(steps - 2, steps):
        away_sent(q)

    @pl.when(end)
    def _():
        for q in range(steps - NI, steps):
            end_sent(q)


def solution(mesh):
    def step(x, gain, wq, wk, wv, wo):
        rows, d = x.shape
        own = wq.shape[1]
        chunks = rows // R
        half = HEAD // 2
        freq = np.float32(THETA) ** (-np.arange(half, dtype=np.float32) / half)
        freq = jnp.asarray(np.concatenate([freq, freq])[None], jnp.float32)
        bf16, f32 = jnp.bfloat16, jnp.float32
        hbm = pl.BlockSpec(memory_space=pl.ANY)
        vmem = pl.BlockSpec(memory_space=pltpu.VMEM)
        dma = pltpu.SemaphoreType.DMA
        parts = [(NI, XR, d), (2, R, d), (NB, KB, 768), (rows, own), (own // HEAD, HEAD + 8, rows)]
        y, *kept = pl.pallas_call(
            _kernel,
            out_shape=[jax.ShapeDtypeStruct((rows, d), bf16)] + [pltpu.VMEM(shape, bf16) for shape in parts],
            in_specs=[hbm, vmem, vmem, hbm, hbm, hbm, hbm],
            out_specs=[hbm] + [vmem] * len(parts),
            scratch_shapes=[
                pltpu.VMEM((8, d), f32),
                pltpu.VMEM((XR, d), bf16),
                pltpu.VMEM((R, 768), f32),
                pltpu.VMEM((NI, 2, own, 2 * PC), bf16),
                pltpu.VMEM((3, R, own), bf16),
                pltpu.VMEM((own // HEAD, R, HEAD), bf16),
                pltpu.VMEM((2, R, HEAD), f32),
                pltpu.VMEM((2, R, HEAD), f32),
                pltpu.VMEM((2, R, HEAD), f32),
                pltpu.VMEM((2, 1, R), f32),
                pltpu.VMEM((2, HEAD + 8, R), f32),
                pltpu.VMEM((2, RING // 2, R, PC), bf16),
                pltpu.VMEM((2, RING, PR, PC), bf16),
                pltpu.VMEM((8, PR, PC), bf16),
                pltpu.VMEM((2, 4, R, PC), bf16),
                pltpu.VMEM((2, NP // 2, R, PC), bf16),
                pltpu.VMEM((2, R, 2 * PC), bf16),
                pltpu.VMEM((2, 2, own, 2 * PC), bf16),
                dma((NI,)),
                dma((NB,)),
                dma((NI, 2)),
                dma((2, 2)),
                dma((2,)),
                dma((2, RING // 4)),
                dma((2, RING)),
                dma((8,)),
                dma((2, RING // 4)),
                dma((8,)),
                dma((2, RING // 4)),
                dma((2,)),
                dma((2, NI)),
                dma((2, NI)),
                dma((2, NI)),
                dma((NI,)),
                dma((2,)),
            ],
            compiler_params=pltpu.CompilerParams(collective_id=1, has_side_effects=True, vmem_limit_bytes=VMEM),
            name="layer",
        )(x, gain, freq, wq, wk, wv, wo)
        return pl.pallas_call(
            _gather,
            out_shape=jax.ShapeDtypeStruct((rows, d), bf16),
            in_specs=[hbm] + [vmem] * len(parts),
            out_specs=hbm,
            scratch_shapes=[pltpu.VMEM((NP // 2, R, 2 * PC), bf16), dma((NP // 2,)), dma((NP // 2,)), dma((40,))],
            compiler_params=pltpu.CompilerParams(vmem_limit_bytes=3 * 2**20),
            name="gather",
        )(y, *kept)

    tokens, columns = P("dp", None), P(None, "tp")
    return jax.shard_map(
        step,
        mesh=mesh,
        in_specs=(tokens, P(None), columns, columns, columns, P("tp", None)),
        out_specs=tokens,
        check_vma=False,
    )
```

```python
import functools

import jax
import jax.numpy as jnp
import numpy as np
from jax import lax
from jax.experimental import pallas as pl
from jax.experimental.pallas import tpu as pltpu
from jax.sharding import PartitionSpec as P

HEAD = 128
THETA = 10000
NEG = -1e30
HIDDEN = 2 * NEG
LOG2E = 1.4426950408889634
VMEM = 63 * 2**19
R = 256
KB = 2048
PC = 256
NB = 4
XR = R // 4
KEYS = 512
BOTH = (0, 1)
ROWS = 16
WIDE = 1024
PR = R // 2
NI = 4
NP = 4 * NI
RING = 32
MESH = pl.DeviceIdType.MESH


def _dot(a, b, ca, cb):
    return lax.dot_general(a, b, (((ca,), (cb,)), ((), ())), preferred_element_type=jnp.float32)


def _parts(xb, a_s, wbuf, k_s):
    half = KB // 2
    some = [((pl.ds(0, half), pl.ds((2 * kb + n) * 768, 768)), wbuf.at[kb, pl.ds(n * half, half)]) for kb in range(NB) for n in BOTH]
    some += [((pl.ds(0, half), pl.ds(2 * NB * 768 + n * 1024, 1024)), k_s.at[pl.ds(n * half, half)]) for n in BOTH]
    some += [((pl.ds(half + n * R, R), slice(None)), a_s.at[n]) for n in BOTH]
    return some + [((pl.ds(half + 2 * R + n * XR, XR), slice(None)), xb.at[n]) for n in range(NI)]


def _columns(d, i):
    return [pl.ds((side + side + g) * (d // NI) + i * 2 * PC, 2 * PC) for side in BOTH for g in BOTH]


def _late(rows, d, vt_s, i):
    tiles = [(pl.ds(rows - R + r * PR, PR), at) for at in _columns(d, i) for r in BOTH]
    return [(at, vt_s.at[2 * i + n // NI, :HEAD, pl.ds(n % NI * 2 * PC, 2 * PC)]) for n, at in enumerate(tiles)]


def _gather(y_ref, xb, a_s, wbuf, k_s, vt_s, out_ref, buf, i_sem, o_sem):
    rows, d = y_ref.shape
    last = [(pl.ds(rows - R, R), at) for i in (2, 3) for at in _columns(d, i)]
    loads = [pltpu.make_async_copy(y_ref.at[at], buf.at[b], i_sem.at[b]) for b, at in enumerate(last)]
    stores = [pltpu.make_async_copy(buf.at[b], out_ref.at[at], o_sem.at[0]) for b, at in enumerate(last)]
    kept = [pltpu.make_async_copy(ref, out_ref.at[at], o_sem.at[1]) for at, ref in _parts(xb, a_s, wbuf, k_s)]
    for i in BOTH:
        kept += [pltpu.make_async_copy(ref, out_ref.at[at], o_sem.at[2]) for at, ref in _late(rows, d, vt_s, i)]
    for copy in loads + kept:
        copy.start()
    for load, store in zip(loads, stores):
        load.wait()
        store.start()
    for n, size in enumerate((PR, rows - R, PR)):
        some = out_ref.at[pl.ds(0, size)]
        pltpu.make_async_copy(some, some, o_sem.at[n]).wait()


def _kernel(x_ref, gain_ref, freq_ref, wq_ref, wk_ref, wv_ref, wo_ref, y_ref, xb, a_s, wbuf, k_s, vt_s,
            gain_s, stage_s, acc_s, wo_s, s_s, q_s, turns_s, cos_s, sin_s, top_s, mix_s,
            part, from_e, from_m, obuf, sbuf, xres, away_s,
            x_sem, w_sem, wo_sem, away_sem, xr_sem, r_part, r_e, r_m, r_end, r_mid, r_y, s_o, s_u, s_e, s_p, s_l, keep_sem):
    rows, d = x_ref.shape
    chunks = rows // R
    steps = chunks * NI
    pieces = chunks * NP
    scale = HEAD**-0.5
    e = scale * LOG2E
    tp = lax.axis_index("tp")
    z, core = lax.div(tp, 2), lax.rem(tp, 2)
    middle = (z == 1) | (z == 2)
    end = jnp.logical_not(middle)
    partner = z * 2 + 1 - core
    inner = jnp.where(z < 2, 1, 2) * 2 + core
    outer = jnp.where(z < 2, 0, 3) * 2 + core
    other = (3 - z) * 2 + core
    near = jnp.where(z < 2, 0, 1)
    half = d // 2
    quarter = d // 4

    def col(side, ab, i):
        g = near if ab == 1 else 1 - near
        return pl.multiple_of(side * half + g * quarter + i * PC, PC)

    def chunk(c):
        return lax.div(c, NP)

    def ring(c):
        return lax.rem(c, RING)

    def unit(c):
        return lax.div(lax.rem(c, NP), 2), pl.ds(pl.multiple_of(lax.rem(c, 2) * PR, PR), PR)

    def row(k):
        return pl.ds(pl.multiple_of(k * R, R), R)

    def remote(src, dst, send, recv, to):
        return pltpu.make_async_remote_copy(src, dst, send, recv, device_id={"tp": to}, device_id_type=MESH)

    def stash():
        return _parts(xb, a_s, wbuf, k_s)

    def keep(n):
        at, ref = stash()[n]
        return pltpu.make_async_copy(y_ref.at[at], ref, keep_sem.at[0])

    def keep_late(i):
        for at, ref in _late(rows, d, vt_s, i):
            pltpu.make_async_copy(y_ref.at[at], ref, keep_sem.at[1]).start()

    def done(ref, sem):
        pltpu.make_async_copy(ref, ref, sem).wait()

    def is_piece(c):
        return (c >= 0) & (c < pieces)

    def load_x(b):
        slot = lax.rem(b, NI)
        return pltpu.make_async_copy(x_ref.at[pl.ds(pl.multiple_of(b * XR, XR), XR)], xb.at[slot], x_sem.at[slot])

    def load_w(t, kb, m):
        w = (wq_ref, wk_ref, wv_ref)[m]
        i = lax.rem(t, NI)
        return pltpu.make_async_copy(
            w.at[pl.ds(kb * KB, KB), pl.ds(pl.multiple_of(i * 256, 256), 256)],
            wbuf.at[kb, :, pl.ds(m * 256, 256)], w_sem.at[kb])

    def load_away(q, ab):
        slot = lax.rem(q, 2)
        at = pl.ds(col(1 - core, ab, 2 * lax.rem(q, NI)), 2 * PC)
        return pltpu.make_async_copy(wo_ref.at[:, at], away_s.at[slot, ab], away_sem.at[slot, ab])

    def load_wo(i, ab):
        at = pl.ds(col(core, ab, 2 * i), 2 * PC)
        return pltpu.make_async_copy(wo_ref.at[:, at], wo_s.at[i, ab], wo_sem.at[i, ab])

    def load_res(q):
        slot, i = lax.rem(q, 2), lax.rem(q, NI)
        return pltpu.make_async_copy(
            x_ref.at[row(lax.div(q, NI)), pl.ds(col(core, 1, 2 * i), 2 * PC)], xres.at[slot], xr_sem.at[slot])

    def to_partner(n, ab):
        p, r = lax.rem(n, 4), lax.rem(n, RING // 2)
        return remote(obuf.at[ab, p], part.at[ab, r], s_o.at[lax.div(p, 2)], r_part.at[ab, lax.div(r, 2)], partner)

    def turn_of(c):
        return lax.rem(lax.div(c, 4), NI)

    def held(ab, c):
        i, at = unit(c)
        return sbuf.at[ab, i, at]

    def to_inner(c, ab):
        return remote(held(ab, c), from_e.at[ab, ring(c)], s_u.at[ab, turn_of(c)], r_e.at[ab, ring(c)], inner)

    def to_other(c):
        p = lax.rem(c, 8)
        return remote(held(0, c), from_m.at[p], s_u.at[0, turn_of(c)], r_m.at[p], other)

    def y_at(c, side, ab):
        i, _ = unit(c)
        at = pl.ds(pl.multiple_of(chunk(c) * R + lax.rem(c, 2) * PR, PR), PR)
        return y_ref.at[at, pl.ds(col(side, ab, i), PC)]

    def y_unit(n, side, ab):
        return y_ref.at[row(lax.div(n, NP // 2)), pl.ds(col(side, ab, lax.rem(n, NP // 2)), PC)]

    def result_to_other(c):
        return remote(held(1, c), y_at(c, core, 1), s_u.at[1, turn_of(c)], r_mid.at[lax.rem(c, 8)], other)

    def result_to_outer(c, ab, src):
        return remote(src, y_at(c, core, ab), s_e.at[ab, turn_of(c)], r_end.at[ab, lax.div(ring(c), 4)], outer)

    def result_to_partner(n, ab, src, side):
        q = lax.div(n, 2)
        return remote(src, y_unit(n, side, ab), s_p.at[ab, lax.rem(q, NI)], r_y.at[ab, lax.rem(q, RING // 4)], partner)

    def result_here(n):
        i = lax.rem(n, NP // 2)
        return pltpu.make_async_copy(sbuf.at[1, i], y_unit(n, core, 1), s_l.at[lax.rem(lax.div(n, 2), NI)])

    barrier = pltpu.get_barrier_semaphore()

    def greet(to):
        pl.semaphore_signal(barrier, inc=1, device_id={"tp": to}, device_id_type=MESH)

    for b in range(NI):
        load_x(b).start()
    greet(partner)

    @pl.when(end)
    def _():
        greet(inner)

    @pl.when(middle)
    def _():
        greet(outer)
        greet(other)

    gain_s[...] = jnp.broadcast_to(gain_ref[...].astype(jnp.float32)[None], gain_s.shape)

    for h in range(2 * NI):
        vt_s[h, HEAD:, :] = jnp.ones((8, rows), jnp.bfloat16)
    for kb in BOTH:
        for m in range(3):
            load_w(0, kb, m).start()

    def norm(b, to, top):
        slot = lax.rem(b, NI)
        sizes = []
        for g in range(XR // ROWS):
            wide = xb[slot, g * ROWS : g * ROWS + ROWS, :].astype(jnp.float32)
            sizes.append(lax.rsqrt(jnp.mean(wide * wide, -1, keepdims=True) + 1e-6))
        for g, size in enumerate(sizes):
            wide = xb[slot, g * ROWS : g * ROWS + ROWS, :].astype(jnp.float32) * size
            wide = wide.reshape(2, 8, d) * gain_s[...][None]
            to[pl.ds(pl.multiple_of(top + g * ROWS, ROWS), ROWS), :] = wide.reshape(ROWS, d).astype(jnp.bfloat16)
        angles(b)

    sign = jnp.where(lax.broadcasted_iota(jnp.int32, (8, HEAD), 1) < HEAD // 2, -1.0, 1.0)

    def angles(b):
        k, i = lax.div(b, NI), lax.rem(b, NI)
        here = pl.ds(pl.multiple_of(i * XR, XR), XR)
        angle = jnp.full((8, HEAD), k * R, jnp.int32).astype(jnp.float32) * freq_ref[...]
        c, s = jnp.cos(angle)[:1], (jnp.sin(angle) * sign)[:1]
        cos, sin = turns_s[0, here, :], turns_s[1, here, :]
        cos_s[lax.rem(k, 2), here, :] = cos * c - sin * s
        sin_s[lax.rem(k, 2), here, :] = sin * c + cos * s

    def first_angles():
        token = lax.broadcasted_iota(jnp.int32, (R, HEAD), 0).astype(jnp.float32)
        angle = token * freq_ref[...]
        turns_s[0] = jnp.cos(angle)
        turns_s[1] = jnp.sin(angle) * jnp.concatenate([sign] * (R // 8), axis=0)

    def more_x(b):
        @pl.when(b < steps)
        def _():
            load_x(b).start()

    def project(t, part, ahead):
        p = lax.rem(lax.div(t, NI), 2)
        blocks = (2 * part, 2 * part + 1)
        for kb in blocks:
            done(wbuf.at[kb], w_sem.at[kb])
        if ahead:
            load_x(t + NI).wait()
            norm(t + NI, stage_s, 0)
        for kb in blocks:
            some = _dot(a_s[p, :, kb * KB : (kb + 1) * KB], wbuf[kb], 1, 0)
            acc_s[...] = some if kb == 0 else acc_s[...] + some
        if ahead:
            k, at = lax.rem(lax.div(t + NI, NI), 2), lax.rem(t, NI) * XR
            a_s[k, pl.ds(pl.multiple_of(at, XR), XR), :] = stage_s[...]
            more_x(t + 2 * NI)

        @pl.when((t + 1 < steps) & (t != NI - 1))
        def _():
            more_w(t, part)

    def more_w(t, part):
        for kb in (2 * part, 2 * part + 1):
            for m in range(3):
                load_w(t + 1, kb, m).start()

    def rotate(t):
        k, i = lax.div(t, NI), lax.rem(t, NI)
        p = lax.rem(k, 2)
        lane = lambda h: pl.ds(pl.multiple_of(i * 256 + h * HEAD, HEAD), HEAD)

        def turned(at):
            one = acc_s[:, at : at + HEAD].astype(jnp.bfloat16).astype(jnp.float32)
            return (one * cos_s[p] + pltpu.roll(one, HEAD // 2, 1) * sin_s[p]).astype(jnp.bfloat16)

        for h in BOTH:
            q_s[2 * i + h] = turned(h * HEAD)
            k_s[row(k), lane(h)] = turned(256 + h * HEAD)
            vt_s[2 * i + h, :HEAD, row(k)] = acc_s[:, 512 + h * HEAD : 512 + (h + 1) * HEAD].astype(jnp.bfloat16).T

    def attend(t):
        k, i = lax.div(t, NI), lax.rem(t, NI)
        lane = lambda h: pl.ds(pl.multiple_of(i * 256 + h * HEAD, HEAD), HEAD)
        for h in BOTH:
            top_s[h] = jnp.full((1, R), NEG, jnp.float32)
            mix_s[h] = jnp.zeros((HEAD + 8, R), jnp.float32)

        def block(first, keys, masked):
            here = pl.ds(pl.multiple_of(first, keys), keys)
            scores = [_dot(k_s[here, lane(h)], q_s[2 * i + h], 1, 1) for h in BOTH]
            if masked:
                gap = lax.broadcasted_iota(jnp.int32, (keys, R), 1) - lax.broadcasted_iota(jnp.int32, (keys, R), 0)
                seen = gap >= first - k * R
                scores = [jnp.where(seen, s, HIDDEN) for s in scores]
            weights, keeps = [], []
            for h, s in enumerate(scores):
                old = top_s[h]
                top = jnp.maximum(old, s.max(axis=0, keepdims=True))
                top_s[h] = top
                weights.append(jnp.exp2((s - top) * e).astype(jnp.bfloat16))
                keeps.append(jnp.exp2((old - top) * e))
            for h in BOTH:
                mix_s[h] = mix_s[h] * keeps[h] + _dot(vt_s[2 * i + h, :, here], weights[h], 1, 0)

        whole = lax.div(k * R, KEYS)

        def plain(j, carry):
            block(j * KEYS, KEYS, False)
            return carry

        lax.fori_loop(0, whole, plain, 0)

        @pl.when(lax.rem(k, 2) == 1)
        def _():
            block(whole * KEYS, KEYS, True)

        @pl.when(lax.rem(k, 2) == 0)
        def _():
            block(k * R, R, True)

        for h in BOTH:
            out = mix_s[h, :HEAD, :] * (1 / mix_s[h, HEAD : HEAD + 1, :])
            s_s[lax.rem(k, 3), :, lane(h)] = out.T.astype(jnp.bfloat16)

    def attend_first():
        gap = lax.broadcasted_iota(jnp.int32, (R, R), 1) - lax.broadcasted_iota(jnp.int32, (R, R), 0)
        heads = range(2 * NI)
        scores = [_dot(k_s[:R, h * HEAD : (h + 1) * HEAD], q_s[h], 1, 1) for h in heads]
        weights = []
        for s in scores:
            s = jnp.where(gap >= 0, s, HIDDEN)
            weights.append(jnp.exp2((s - s.max(axis=0, keepdims=True)) * e).astype(jnp.bfloat16))
        for h in heads:
            mix = _dot(vt_s[h, :, :R], weights[h], 1, 0)
            out = mix[:HEAD] * (1 / mix[HEAD : HEAD + 1])
            s_s[0, :, h * HEAD : (h + 1) * HEAD] = out.T.astype(jnp.bfloat16)

    def mine(k):
        return s_s[lax.rem(k, 3)]

    def send_away(q):
        with jax.named_scope("away"):
            @pl.when(q >= 2)
            def _():
                away_sent(q - 2)

            for ab in BOTH:
                load_away(q, ab).wait()
                term = _dot(mine(lax.div(q, NI)), away_s[lax.rem(q, 2), ab], 1, 0)
                for u in BOTH:
                    obuf[ab, lax.rem(2 * q + u, 4)] = term[:, u * PC : (u + 1) * PC].astype(jnp.bfloat16)
                for u in BOTH:
                    to_partner(2 * q + u, ab).start()

            @pl.when(q + 2 < steps)
            def _():
                for ab in BOTH:
                    load_away(q + 2, ab).start()

    def away_sent(q):
        i = lax.rem(q, 2)
        done(obuf.at[:, pl.ds(2 * i, 2)], s_o.at[i])

    def block(q, ab):
        i = lax.rem(q, NI)
        return sbuf.at[ab, pl.ds(2 * i, 2)]

    def terms_of(q, ab):
        return part.at[ab, pl.ds(2 * lax.rem(q, RING // 4), 2)]

    def end_sent(q):
        for ab in BOTH:
            done(block(q, ab), s_u.at[ab, lax.rem(q, NI)])

    def end_sum(q):
        with jax.named_scope("end_sum"):
            i = lax.rem(q, NI)

            @pl.when(q < NI)
            def _():
                for ab in BOTH:
                    load_wo(q, ab).wait()

            @pl.when(q >= NI)
            def _():
                end_sent(q - NI)

            for ab in BOTH:
                term = _dot(mine(lax.div(q, NI)), wo_s[i, ab], 1, 0)
                for u in BOTH:
                    n = 2 * q + u
                    if u == 0:
                        done(terms_of(q, ab), r_part.at[ab, lax.rem(q, RING // 4)])
                    some = term[:, u * PC : (u + 1) * PC] + part[ab, lax.rem(n, RING // 2)].astype(jnp.float32)
                    sbuf[ab, lax.rem(n, NP // 2)] = some.astype(jnp.bfloat16)
                if ab == 0:
                    to_inner(4 * q, 0).start()

                    @pl.when(q > 0)
                    def _():
                        to_inner(4 * q - 2, 1).start()

                    to_inner(4 * q + 1, 0).start()

                    @pl.when(q > 0)
                    def _():
                        to_inner(4 * q - 1, 1).start()

                    to_inner(4 * q + 2, 0).start()
                else:
                    to_inner(4 * q, 1).start()
                    to_inner(4 * q + 3, 0).start()
                    to_inner(4 * q + 1, 1).start()

                    @pl.when(q == steps - 1)
                    def _():
                        to_inner(4 * q + 2, 1).start()
                        to_inner(4 * q + 3, 1).start()

    def middle_pass(c, v):
        q, n, u = lax.div(c, 4), lax.div(c, 2), v // 2
        at = pl.ds(v % 2 * PR, PR)
        with jax.named_scope("pass_w"):
            if v == 0:
                @pl.when(q < NI)
                def _():
                    load_wo(q, 0).wait()

            if v == 0:
                done(terms_of(q, 0), r_part.at[0, lax.rem(q, RING // 4)])
            to_inner(c, 0).wait_recv()
        with jax.named_scope("pass"):
            term = _dot(s_s[lax.rem(chunk(c), 3), at, :], wo_s[lax.rem(q, NI), 0, :, u * PC : (u + 1) * PC], 1, 0)
            term = term + part[0, lax.rem(n, RING // 2), at, :].astype(jnp.float32) + from_e[0, ring(c)].astype(jnp.float32)
            sbuf[0, lax.rem(n, NP // 2), at, :] = term.astype(jnp.bfloat16)
            to_other(c).start()

    def middle_finish(c, v):
        q, n, u = lax.div(c, 4), lax.div(c, 2), v // 2
        at = pl.ds(v % 2 * PR, PR)
        with jax.named_scope("finish_w"):
            if v == 0:
                @pl.when(q < NI)
                def _():
                    load_wo(q, 1).wait()

                load_res(q).wait()
            if v == 0:
                done(terms_of(q, 1), r_part.at[1, lax.rem(q, RING // 4)])
            to_inner(c, 1).wait_recv()
            to_other(c).wait_recv()
        with jax.named_scope("finish"):
            term = _dot(s_s[lax.rem(chunk(c), 3), at, :], wo_s[lax.rem(q, NI), 1, :, u * PC : (u + 1) * PC], 1, 0)
            term = term + part[1, lax.rem(n, RING // 2), at, :].astype(jnp.float32)
            term = term + from_e[1, ring(c)].astype(jnp.float32) + from_m[lax.rem(c, 8)].astype(jnp.float32)
            term = term + xres[lax.rem(q, 2), at, u * PC : (u + 1) * PC].astype(jnp.float32)
            sbuf[1, lax.rem(n, NP // 2), at, :] = term.astype(jnp.bfloat16)
            result_to_outer(c, 1, held(1, c)).start()
            result_to_other(c).start()
            if v % 2 == 1:
                result_to_partner(n, 1, sbuf.at[1, lax.rem(n, NP // 2)], core).start()
                result_here(n).start()

    def middle_forward(c, v):
        src = y_at(c, core, 0)
        with jax.named_scope("forward_w"):
            done(from_m.at[0], r_mid.at[lax.rem(c, 8)])
        result_to_outer(c, 0, src).start()
        if v % 2 == 1:
            n = lax.div(c, 2)
            result_to_partner(n, 0, y_unit(n, core, 0), core).start()

    def middle_turn(t, j):
        s = 4 * t + j

        @pl.when(is_piece(s - 16) & middle)
        def _():
            middle_pass(s - 16, j)

        @pl.when(is_piece(s - 18) & middle)
        def _():
            middle_finish(s - 18, (j + 2) % 4)

        @pl.when(is_piece(s - 20) & middle)
        def _():
            middle_forward(s - 20, j)

    def norms(first, k):
        def one(i, carry):
            b = first + i
            with jax.named_scope("x_w"):
                load_x(b).wait()
            slot = lax.rem(b, NI)

            def squares(j, total):
                at = pl.ds(pl.multiple_of(j * WIDE, WIDE), WIDE)
                for g in range(XR // ROWS):
                    wide = xb[slot, g * ROWS : g * ROWS + ROWS, at].astype(jnp.float32)
                    wide = wide * wide
                    some = wide[:, :HEAD]
                    for n in range(1, 8):
                        some = some + wide[:, n * HEAD : (n + 1) * HEAD]
                    total = total[:g] + (total[g] + some,) + total[g + 1 :]
                return total

            total = lax.fori_loop(0, d // WIDE, squares, (jnp.zeros((ROWS, HEAD), jnp.float32),) * (XR // ROWS))
            sizes = [lax.rsqrt(jnp.sum(v, -1, keepdims=True) / d + 1e-6) for v in total]
            sizes = tuple(jnp.broadcast_to(v, (ROWS, HEAD)) for v in sizes)

            def scaled(j, sizes):
                at = pl.ds(pl.multiple_of(j * WIDE, WIDE), WIDE)
                for g in range(XR // ROWS):
                    wide = xb[slot, g * ROWS : g * ROWS + ROWS, at].astype(jnp.float32)
                    wide = wide * jnp.concatenate([sizes[g]] * 8, axis=1)
                    wide = wide.reshape(2, 8, WIDE) * gain_s[:, at][None]
                    a_s[k, pl.ds(pl.multiple_of(i * XR + g * ROWS, ROWS), ROWS), at] = wide.reshape(ROWS, WIDE).astype(jnp.bfloat16)
                return sizes

            lax.fori_loop(0, d // WIDE, scaled, sizes)
            angles(b)
            if k == 0:
                @pl.when(b == 0)
                def _():
                    for kb in (2, 3):
                        for m in range(3):
                            load_w(0, kb, m).start()
            else:
                more_x(b + NI)
            return carry

        lax.fori_loop(0, NI, one, 0)

    def step(t, carry):
        def is_block(q):
            return (q >= 0) & (q < steps)

        @pl.when(is_block(t - 8) & middle)
        def _():
            q = t - 8
            done(block(q, 0), s_u.at[0, lax.rem(q, NI)])
            for sem in (s_u.at[1], s_e.at[1], s_p.at[1], s_l):
                done(block(q, 1), sem.at[lax.rem(q, NI)])

        @pl.when(is_block(t - 9) & middle)
        def _():
            q = t - 9
            for sem in (s_e, s_p):
                done(block(q, 0), sem.at[0, lax.rem(q, NI)])

        @pl.when(is_block(t - 4) & middle)
        def _():
            load_res(t - 4).start()

        first = t == NI - 1

        @pl.when(first)
        def _():
            for ab in BOTH:
                load_away(0, ab).start()
                load_wo(0, ab).start()

        @pl.when((t == NI) | (t == NI + 1))
        def _():
            for ab in BOTH:
                load_wo(t - 2, ab).start()

        ahead = (t >= NI) & (t + NI < steps)
        middle_turn(t, 0)

        @pl.when(ahead)
        def _():
            with jax.named_scope("project0"):
                project(t, 0, True)

        @pl.when(jnp.logical_not(ahead) & (t < steps))
        def _():
            with jax.named_scope("project0_"):
                project(t, 0, False)

        @pl.when(first)
        def _():
            for ab in BOTH:
                load_away(1, ab).start()
                load_wo(1, ab).start()
            for b in range(NI, 2 * NI):
                load_x(b).start()

        middle_turn(t, 1)

        @pl.when(t < steps)
        def _():
            with jax.named_scope("project1"):
                project(t, 1, False)

        @pl.when(first)
        def _():
            more_w(t, 0)

        @pl.when(t < steps)
        def _():
            with jax.named_scope("rotate"):
                rotate(t)

        middle_turn(t, 2)

        @pl.when((t >= NI) & (t < steps))
        def _():
            with jax.named_scope("attend"):
                attend(t)

        @pl.when(first)
        def _():
            with jax.named_scope("attend_first"):
                attend_first()
            more_w(t, 1)

        middle_turn(t, 3)
        i = lax.rem(t, NI)

        @pl.when(is_block(t - 3) & (i == NI - 1))
        def _():
            send_away(t - 3)

            @pl.when(end)
            def _():
                end_sum(t - 3)

        @pl.when(is_block(t - 2) & (i != NI - 2))
        def _():
            send_away(t - 2)

            @pl.when(end)
            def _():
                end_sum(t - 2)

        @pl.when(t == NI - 1)
        def _():
            with jax.named_scope("norm1"):
                norms(NI, 1)

        @pl.when(is_block(t - 8) & end)
        def _():
            for ab in (1, 0):
                with jax.named_scope("result_w"):
                    done(block(t - 8, ab), r_end.at[ab, lax.rem(t - 8, RING // 4)])
                for u in BOTH:
                    n = 2 * (t - 8) + u
                    result_to_partner(n, ab, y_unit(n, core, ab), core).start()

        @pl.when(is_block(t - 9) & end)
        def _():
            for ab in BOTH:
                done(block(t - 9, ab), s_p.at[ab, lax.rem(t - 9, NI)])

        @pl.when(t == steps + 2)
        def _():
            for n in range(len(stash()) - NI):
                keep(n).start()

        for i in BOTH:
            @pl.when(t == steps + 6 + i)
            def _(i=i):
                keep_late(i)

        @pl.when(t == steps + 6)
        def _():
            for n in range(len(stash()) - NI, len(stash())):
                keep(n).start()

        @pl.when(is_block(t - 9))
        def _():
            with jax.named_scope("y_w"):
                for ab in BOTH:
                    done(block(t - 9, ab), r_y.at[ab, lax.rem(t - 9, RING // 4)])

        return carry

    with jax.named_scope("angles"):
        first_angles()
    with jax.named_scope("norm0"):
        norms(0, 0)

    with jax.named_scope("barrier"):
        @pl.when(end)
        def _():
            pl.semaphore_wait(barrier, 2)

        @pl.when(middle)
        def _():
            pl.semaphore_wait(barrier, 3)

    lax.fori_loop(0, steps + 9, step, 0)
    done(y_ref.at[pl.ds(0, rows - R)], keep_sem.at[0])
    done(y_ref.at[pl.ds(0, PR)], keep_sem.at[1])

    for q in range(steps - 2, steps):
        away_sent(q)

    @pl.when(end)
    def _():
        for q in range(steps - NI, steps):
            end_sent(q)


def solution(mesh):
    def step(x, gain, wq, wk, wv, wo):
        rows, d = x.shape
        own = wq.shape[1]
        chunks = rows // R
        half = HEAD // 2
        freq = np.float32(THETA) ** (-np.arange(half, dtype=np.float32) / half)
        freq = jnp.asarray(np.concatenate([freq, freq])[None], jnp.float32)
        bf16, f32 = jnp.bfloat16, jnp.float32
        hbm = pl.BlockSpec(memory_space=pl.ANY)
        vmem = pl.BlockSpec(memory_space=pltpu.VMEM)
        dma = pltpu.SemaphoreType.DMA
        parts = [(NI, XR, d), (2, R, d), (NB, KB, 768), (rows, own), (own // HEAD, HEAD + 8, rows)]
        y, *kept = pl.pallas_call(
            _kernel,
            out_shape=[jax.ShapeDtypeStruct((rows, d), bf16)] + [pltpu.VMEM(shape, bf16) for shape in parts],
            in_specs=[hbm, vmem, vmem, hbm, hbm, hbm, hbm],
            out_specs=[hbm] + [vmem] * len(parts),
            scratch_shapes=[
                pltpu.VMEM((8, d), f32),
                pltpu.VMEM((XR, d), bf16),
                pltpu.VMEM((R, 768), f32),
                pltpu.VMEM((NI, 2, own, 2 * PC), bf16),
                pltpu.VMEM((3, R, own), bf16),
                pltpu.VMEM((own // HEAD, R, HEAD), bf16),
                pltpu.VMEM((2, R, HEAD), f32),
                pltpu.VMEM((2, R, HEAD), f32),
                pltpu.VMEM((2, R, HEAD), f32),
                pltpu.VMEM((2, 1, R), f32),
                pltpu.VMEM((2, HEAD + 8, R), f32),
                pltpu.VMEM((2, RING // 2, R, PC), bf16),
                pltpu.VMEM((2, RING, PR, PC), bf16),
                pltpu.VMEM((8, PR, PC), bf16),
                pltpu.VMEM((2, 4, R, PC), bf16),
                pltpu.VMEM((2, NP // 2, R, PC), bf16),
                pltpu.VMEM((2, R, 2 * PC), bf16),
                pltpu.VMEM((2, 2, own, 2 * PC), bf16),
                dma((NI,)),
                dma((NB,)),
                dma((NI, 2)),
                dma((2, 2)),
                dma((2,)),
                dma((2, RING // 4)),
                dma((2, RING)),
                dma((8,)),
                dma((2, RING // 4)),
                dma((8,)),
                dma((2, RING // 4)),
                dma((2,)),
                dma((2, NI)),
                dma((2, NI)),
                dma((2, NI)),
                dma((NI,)),
                dma((2,)),
            ],
            compiler_params=pltpu.CompilerParams(collective_id=1, has_side_effects=True, vmem_limit_bytes=VMEM),
            name="layer",
        )(x, gain, freq, wq, wk, wv, wo)
        return pl.pallas_call(
            _gather,
            out_shape=jax.ShapeDtypeStruct((rows, d), bf16),
            in_specs=[hbm] + [vmem] * len(parts),
            out_specs=hbm,
            scratch_shapes=[pltpu.VMEM((NP // 2, R, 2 * PC), bf16), dma((NP // 2,)), dma((3,))],
            compiler_params=pltpu.CompilerParams(vmem_limit_bytes=3 * 2**20),
            name="gather",
        )(y, *kept)

    tokens, columns = P("dp", None), P(None, "tp")
    return jax.shard_map(
        step,
        mesh=mesh,
        in_specs=(tokens, P(None), columns, columns, columns, P("tp", None)),
        out_specs=tokens,
        check_vma=False,
    )
```

```python
import functools

import jax
import jax.numpy as jnp
import numpy as np
from jax import lax
from jax.experimental import pallas as pl
from jax.experimental.pallas import tpu as pltpu
from jax.sharding import PartitionSpec as P

HEAD = 128
THETA = 10000
NEG = -1e30
HIDDEN = 2 * NEG
LOG2E = 1.4426950408889634
VMEM = 63 * 2**19
R = 256
KB = 2048
PC = 256
NB = 4
XR = R // 4
KEYS = 512
BOTH = (0, 1)
ROWS = 16
WIDE = 1024
PR = R // 2
NI = 4
NP = 4 * NI
RING = 32
MESH = pl.DeviceIdType.MESH


def _dot(a, b, ca, cb):
    return lax.dot_general(a, b, (((ca,), (cb,)), ((), ())), preferred_element_type=jnp.float32)


def _parts(xb, a_s, wbuf, k_s):
    half = KB // 2
    some = [((pl.ds(0, half), pl.ds((2 * kb + n) * 768, 768)), wbuf.at[kb, pl.ds(n * half, half)]) for kb in range(NB) for n in BOTH]
    some += [((pl.ds(0, half), pl.ds(2 * NB * 768 + n * 1024, 1024)), k_s.at[pl.ds(n * half, half)]) for n in BOTH]
    some += [((pl.ds(half + n * R, R), slice(None)), a_s.at[n]) for n in BOTH]
    return some + [((pl.ds(half + 2 * R + n * XR, XR), slice(None)), xb.at[n]) for n in range(NI)]


def _columns(d, i):
    return [pl.ds((side + side + g) * (d // NI) + i * 2 * PC, 2 * PC) for side in BOTH for g in BOTH]


def _late(rows, d, vt_s, i):
    tiles = [(pl.ds(rows - R + r * PR, PR), at) for at in _columns(d, i) for r in BOTH]
    return [(at, vt_s.at[2 * i + n // NI, :HEAD, pl.ds(n % NI * 2 * PC, 2 * PC)]) for n, at in enumerate(tiles)]


def _gather(y_ref, xb, a_s, wbuf, k_s, vt_s, out_ref, buf, i_sem, o_sem):
    rows, d = y_ref.shape
    last = [(pl.ds(rows - R, R), at) for i in (2, 3) for at in _columns(d, i)]
    loads = [pltpu.make_async_copy(y_ref.at[at], buf.at[b], i_sem.at[b]) for b, at in enumerate(last)]
    stores = [pltpu.make_async_copy(buf.at[b], out_ref.at[at], o_sem.at[0]) for b, at in enumerate(last)]
    kept = [pltpu.make_async_copy(ref, out_ref.at[at], o_sem.at[1]) for at, ref in _parts(xb, a_s, wbuf, k_s)]
    for i in BOTH:
        kept += [pltpu.make_async_copy(ref, out_ref.at[at], o_sem.at[2]) for at, ref in _late(rows, d, vt_s, i)]
    for copy in loads + kept:
        copy.start()
    for load, store in zip(loads, stores):
        load.wait()
        store.start()
    for n, size in enumerate((PR, rows - R, PR)):
        some = out_ref.at[pl.ds(0, size)]
        pltpu.make_async_copy(some, some, o_sem.at[n]).wait()


def _kernel(x_ref, gain_ref, freq_ref, wq_ref, wk_ref, wv_ref, wo_ref, y_ref, xb, a_s, wbuf, k_s, vt_s,
            gain_s, stage_s, acc_s, wo_s, s_s, q_s, turns_s, cos_s, sin_s, top_s, mix_s,
            part, from_e, from_m, obuf, sbuf, xres, away_s,
            x_sem, w_sem, wo_sem, away_sem, xr_sem, r_part, r_e, r_m, r_end, r_mid, r_y, s_o, s_u, s_e, s_p, s_l, keep_sem):
    rows, d = x_ref.shape
    chunks = rows // R
    steps = chunks * NI
    pieces = chunks * NP
    scale = HEAD**-0.5
    e = scale * LOG2E
    tp = lax.axis_index("tp")
    z, core = lax.div(tp, 2), lax.rem(tp, 2)
    middle = (z == 1) | (z == 2)
    end = jnp.logical_not(middle)
    partner = z * 2 + 1 - core
    inner = jnp.where(z < 2, 1, 2) * 2 + core
    outer = jnp.where(z < 2, 0, 3) * 2 + core
    other = (3 - z) * 2 + core
    near = jnp.where(z < 2, 0, 1)
    half = d // 2
    quarter = d // 4

    def col(side, ab, i):
        g = near if ab == 1 else 1 - near
        return pl.multiple_of(side * half + g * quarter + i * PC, PC)

    def chunk(c):
        return lax.div(c, NP)

    def ring(c):
        return lax.rem(c, RING)

    def unit(c):
        return lax.div(lax.rem(c, NP), 2), pl.ds(pl.multiple_of(lax.rem(c, 2) * PR, PR), PR)

    def row(k):
        return pl.ds(pl.multiple_of(k * R, R), R)

    def remote(src, dst, send, recv, to):
        return pltpu.make_async_remote_copy(src, dst, send, recv, device_id={"tp": to}, device_id_type=MESH)

    def stash():
        return _parts(xb, a_s, wbuf, k_s)

    def keep(n):
        at, ref = stash()[n]
        return pltpu.make_async_copy(y_ref.at[at], ref, keep_sem.at[0])

    def keep_late(i):
        for at, ref in _late(rows, d, vt_s, i):
            pltpu.make_async_copy(y_ref.at[at], ref, keep_sem.at[1]).start()

    def done(ref, sem):
        pltpu.make_async_copy(ref, ref, sem).wait()

    def is_piece(c):
        return (c >= 0) & (c < pieces)

    def load_x(b):
        slot = lax.rem(b, NI)
        return pltpu.make_async_copy(x_ref.at[pl.ds(pl.multiple_of(b * XR, XR), XR)], xb.at[slot], x_sem.at[slot])

    def load_w(t, kb, m):
        w = (wq_ref, wk_ref, wv_ref)[m]
        i = lax.rem(t, NI)
        return pltpu.make_async_copy(
            w.at[pl.ds(kb * KB, KB), pl.ds(pl.multiple_of(i * 256, 256), 256)],
            wbuf.at[kb, :, pl.ds(m * 256, 256)], w_sem.at[kb])

    def load_away(q, ab):
        slot = lax.rem(q, 2)
        at = pl.ds(col(1 - core, ab, 2 * lax.rem(q, NI)), 2 * PC)
        return pltpu.make_async_copy(wo_ref.at[:, at], away_s.at[slot, ab], away_sem.at[slot, ab])

    def load_wo(i, ab):
        at = pl.ds(col(core, ab, 2 * i), 2 * PC)
        return pltpu.make_async_copy(wo_ref.at[:, at], wo_s.at[i, ab], wo_sem.at[i])

    def load_res(q):
        slot, i = lax.rem(q, 2), lax.rem(q, NI)
        return pltpu.make_async_copy(
            x_ref.at[row(lax.div(q, NI)), pl.ds(col(core, 1, 2 * i), 2 * PC)], xres.at[slot], xr_sem.at[slot])

    def to_partner(n, ab):
        p, r = lax.rem(n, 4), lax.rem(n, RING // 2)
        return remote(obuf.at[ab, p], part.at[ab, r], s_o.at[lax.div(p, 2)], r_part.at[ab, lax.div(r, 2)], partner)

    def turn_of(c):
        return lax.rem(lax.div(c, 4), NI)

    def held(ab, c):
        i, at = unit(c)
        return sbuf.at[ab, i, at]

    def to_inner(c, ab):
        return remote(held(ab, c), from_e.at[ab, ring(c)], s_u.at[ab, turn_of(c)], r_e.at[ab, ring(c)], inner)

    def to_other(c):
        p = lax.rem(c, 8)
        return remote(held(0, c), from_m.at[p], s_u.at[0, turn_of(c)], r_m.at[p], other)

    def y_at(c, side, ab):
        i, _ = unit(c)
        at = pl.ds(pl.multiple_of(chunk(c) * R + lax.rem(c, 2) * PR, PR), PR)
        return y_ref.at[at, pl.ds(col(side, ab, i), PC)]

    def y_unit(n, side, ab):
        return y_ref.at[row(lax.div(n, NP // 2)), pl.ds(col(side, ab, lax.rem(n, NP // 2)), PC)]

    def result_to_other(c):
        return remote(held(1, c), y_at(c, core, 1), s_u.at[1, turn_of(c)], r_mid.at[lax.rem(c, 8)], other)

    def result_to_outer(c, ab, src):
        return remote(src, y_at(c, core, ab), s_e.at[ab, turn_of(c)], r_end.at[ab, lax.div(ring(c), 4)], outer)

    def result_to_partner(n, ab, src, side):
        q = lax.div(n, 2)
        return remote(src, y_unit(n, side, ab), s_p.at[ab, lax.rem(q, NI)], r_y.at[lax.rem(q, RING // 4)], partner)

    def result_here(n):
        i = lax.rem(n, NP // 2)
        return pltpu.make_async_copy(sbuf.at[1, i], y_unit(n, core, 1), s_l.at[lax.rem(lax.div(n, 2), NI)])

    barrier = pltpu.get_barrier_semaphore()

    def greet(to):
        pl.semaphore_signal(barrier, inc=1, device_id={"tp": to}, device_id_type=MESH)

    for b in range(NI):
        load_x(b).start()
    greet(partner)

    @pl.when(end)
    def _():
        greet(inner)

    @pl.when(middle)
    def _():
        greet(outer)
        greet(other)

    gain_s[...] = jnp.broadcast_to(gain_ref[...].astype(jnp.float32)[None], gain_s.shape)

    for h in range(2 * NI):
        vt_s[h, HEAD:, :] = jnp.ones((8, rows), jnp.bfloat16)
    for kb in BOTH:
        for m in range(3):
            load_w(0, kb, m).start()

    def norm(b, to, top):
        slot = lax.rem(b, NI)
        sizes = []
        for g in range(XR // ROWS):
            wide = xb[slot, g * ROWS : g * ROWS + ROWS, :].astype(jnp.float32)
            sizes.append(lax.rsqrt(jnp.mean(wide * wide, -1, keepdims=True) + 1e-6))
        for g, size in enumerate(sizes):
            wide = xb[slot, g * ROWS : g * ROWS + ROWS, :].astype(jnp.float32) * size
            wide = wide.reshape(2, 8, d) * gain_s[...][None]
            to[pl.ds(pl.multiple_of(top + g * ROWS, ROWS), ROWS), :] = wide.reshape(ROWS, d).astype(jnp.bfloat16)
        angles(b)

    sign = jnp.where(lax.broadcasted_iota(jnp.int32, (8, HEAD), 1) < HEAD // 2, -1.0, 1.0)

    def angles(b):
        k, i = lax.div(b, NI), lax.rem(b, NI)
        here = pl.ds(pl.multiple_of(i * XR, XR), XR)
        angle = jnp.full((8, HEAD), k * R, jnp.int32).astype(jnp.float32) * freq_ref[...]
        c, s = jnp.cos(angle)[:1], (jnp.sin(angle) * sign)[:1]
        cos, sin = turns_s[0, here, :], turns_s[1, here, :]
        cos_s[lax.rem(k, 2), here, :] = cos * c - sin * s
        sin_s[lax.rem(k, 2), here, :] = sin * c + cos * s

    def first_angles():
        token = lax.broadcasted_iota(jnp.int32, (R, HEAD), 0).astype(jnp.float32)
        angle = token * freq_ref[...]
        turns_s[0] = jnp.cos(angle)
        turns_s[1] = jnp.sin(angle) * jnp.concatenate([sign] * (R // 8), axis=0)

    def more_x(b):
        @pl.when(b < steps)
        def _():
            load_x(b).start()

    def project(t, part, ahead):
        p = lax.rem(lax.div(t, NI), 2)
        blocks = (2 * part, 2 * part + 1)
        for kb in blocks:
            done(wbuf.at[kb], w_sem.at[kb])
        if ahead:
            load_x(t + NI).wait()
            norm(t + NI, stage_s, 0)
        for kb in blocks:
            some = _dot(a_s[p, :, kb * KB : (kb + 1) * KB], wbuf[kb], 1, 0)
            acc_s[...] = some if kb == 0 else acc_s[...] + some
        if ahead:
            k, at = lax.rem(lax.div(t + NI, NI), 2), lax.rem(t, NI) * XR
            a_s[k, pl.ds(pl.multiple_of(at, XR), XR), :] = stage_s[...]
            more_x(t + 2 * NI)

        @pl.when((t + 1 < steps) & (t != NI - 1))
        def _():
            more_w(t, part)

    def more_w(t, part):
        for kb in (2 * part, 2 * part + 1):
            for m in range(3):
                load_w(t + 1, kb, m).start()

    def rotate(t):
        k, i = lax.div(t, NI), lax.rem(t, NI)
        p = lax.rem(k, 2)
        lane = lambda h: pl.ds(pl.multiple_of(i * 256 + h * HEAD, HEAD), HEAD)

        def turned(at):
            one = acc_s[:, at : at + HEAD].astype(jnp.bfloat16).astype(jnp.float32)
            return (one * cos_s[p] + pltpu.roll(one, HEAD // 2, 1) * sin_s[p]).astype(jnp.bfloat16)

        for h in BOTH:
            q_s[2 * i + h] = turned(h * HEAD)
            k_s[row(k), lane(h)] = turned(256 + h * HEAD)
            vt_s[2 * i + h, :HEAD, row(k)] = acc_s[:, 512 + h * HEAD : 512 + (h + 1) * HEAD].astype(jnp.bfloat16).T

    def attend(t):
        k, i = lax.div(t, NI), lax.rem(t, NI)
        lane = lambda h: pl.ds(pl.multiple_of(i * 256 + h * HEAD, HEAD), HEAD)
        for h in BOTH:
            top_s[h] = jnp.full((1, R), NEG, jnp.float32)
            mix_s[h] = jnp.zeros((HEAD + 8, R), jnp.float32)

        def block(first, keys, masked):
            here = pl.ds(pl.multiple_of(first, keys), keys)
            scores = [_dot(k_s[here, lane(h)], q_s[2 * i + h], 1, 1) for h in BOTH]
            if masked:
                gap = lax.broadcasted_iota(jnp.int32, (keys, R), 1) - lax.broadcasted_iota(jnp.int32, (keys, R), 0)
                seen = gap >= first - k * R
                scores = [jnp.where(seen, s, HIDDEN) for s in scores]
            weights, keeps = [], []
            for h, s in enumerate(scores):
                old = top_s[h]
                top = jnp.maximum(old, s.max(axis=0, keepdims=True))
                top_s[h] = top
                weights.append(jnp.exp2((s - top) * e).astype(jnp.bfloat16))
                keeps.append(jnp.exp2((old - top) * e))
            for h in BOTH:
                mix_s[h] = mix_s[h] * keeps[h] + _dot(vt_s[2 * i + h, :, here], weights[h], 1, 0)

        whole = lax.div(k * R, KEYS)

        def plain(j, carry):
            block(j * KEYS, KEYS, False)
            return carry

        lax.fori_loop(0, whole, plain, 0)

        @pl.when(lax.rem(k, 2) == 1)
        def _():
            block(whole * KEYS, KEYS, True)

        @pl.when(lax.rem(k, 2) == 0)
        def _():
            block(k * R, R, True)

        for h in BOTH:
            out = mix_s[h, :HEAD, :] * (1 / mix_s[h, HEAD : HEAD + 1, :])
            s_s[lax.rem(k, 3), :, lane(h)] = out.T.astype(jnp.bfloat16)

    def attend_first():
        gap = lax.broadcasted_iota(jnp.int32, (R, R), 1) - lax.broadcasted_iota(jnp.int32, (R, R), 0)
        heads = range(2 * NI)
        scores = [_dot(k_s[:R, h * HEAD : (h + 1) * HEAD], q_s[h], 1, 1) for h in heads]
        weights = []
        for s in scores:
            s = jnp.where(gap >= 0, s, HIDDEN)
            weights.append(jnp.exp2((s - s.max(axis=0, keepdims=True)) * e).astype(jnp.bfloat16))
        for h in heads:
            mix = _dot(vt_s[h, :, :R], weights[h], 1, 0)
            out = mix[:HEAD] * (1 / mix[HEAD : HEAD + 1])
            s_s[0, :, h * HEAD : (h + 1) * HEAD] = out.T.astype(jnp.bfloat16)

    def mine(k):
        return s_s[lax.rem(k, 3)]

    def send_away(q):
        with jax.named_scope("away"):
            @pl.when(q >= 2)
            def _():
                away_sent(q - 2)

            for ab in BOTH:
                load_away(q, ab).wait()
                term = _dot(mine(lax.div(q, NI)), away_s[lax.rem(q, 2), ab], 1, 0)
                for u in BOTH:
                    obuf[ab, lax.rem(2 * q + u, 4)] = term[:, u * PC : (u + 1) * PC].astype(jnp.bfloat16)
                for u in BOTH:
                    to_partner(2 * q + u, ab).start()

            @pl.when(q + 2 < steps)
            def _():
                for ab in BOTH:
                    load_away(q + 2, ab).start()

    def away_sent(q):
        i = lax.rem(q, 2)
        done(obuf.at[:, pl.ds(2 * i, 2)], s_o.at[i])

    def block(q, ab):
        i = lax.rem(q, NI)
        return sbuf.at[ab, pl.ds(2 * i, 2)]

    def terms_of(q, ab):
        return part.at[ab, pl.ds(2 * lax.rem(q, RING // 4), 2)]

    def end_sent(q):
        for ab in BOTH:
            done(block(q, ab), s_u.at[ab, lax.rem(q, NI)])

    def end_sum(q):
        with jax.named_scope("end_sum"):
            i = lax.rem(q, NI)

            @pl.when(q < NI)
            def _():
                done(wo_s.at[q], wo_sem.at[q])

            @pl.when(q >= NI)
            def _():
                end_sent(q - NI)

            for ab in BOTH:
                term = _dot(mine(lax.div(q, NI)), wo_s[i, ab], 1, 0)
                for u in BOTH:
                    n = 2 * q + u
                    if u == 0:
                        done(terms_of(q, ab), r_part.at[ab, lax.rem(q, RING // 4)])
                    some = term[:, u * PC : (u + 1) * PC] + part[ab, lax.rem(n, RING // 2)].astype(jnp.float32)
                    sbuf[ab, lax.rem(n, NP // 2)] = some.astype(jnp.bfloat16)
                if ab == 0:
                    to_inner(4 * q, 0).start()

                    @pl.when(q > 0)
                    def _():
                        to_inner(4 * q - 2, 1).start()

                    to_inner(4 * q + 1, 0).start()

                    @pl.when(q > 0)
                    def _():
                        to_inner(4 * q - 1, 1).start()

                    to_inner(4 * q + 2, 0).start()
                else:
                    to_inner(4 * q, 1).start()
                    to_inner(4 * q + 3, 0).start()
                    to_inner(4 * q + 1, 1).start()

                    @pl.when(q == steps - 1)
                    def _():
                        to_inner(4 * q + 2, 1).start()
                        to_inner(4 * q + 3, 1).start()

    def middle_pass(c, v):
        q, n, u = lax.div(c, 4), lax.div(c, 2), v // 2
        at = pl.ds(v % 2 * PR, PR)
        with jax.named_scope("pass_w"):
            if v == 0:
                @pl.when(q < NI)
                def _():
                    done(wo_s.at[q], wo_sem.at[q])

            if v == 0:
                done(terms_of(q, 0), r_part.at[0, lax.rem(q, RING // 4)])
            to_inner(c, 0).wait_recv()
        with jax.named_scope("pass"):
            term = _dot(s_s[lax.rem(chunk(c), 3), at, :], wo_s[lax.rem(q, NI), 0, :, u * PC : (u + 1) * PC], 1, 0)
            term = term + part[0, lax.rem(n, RING // 2), at, :].astype(jnp.float32) + from_e[0, ring(c)].astype(jnp.float32)
            sbuf[0, lax.rem(n, NP // 2), at, :] = term.astype(jnp.bfloat16)
            to_other(c).start()

    def middle_finish(c, v):
        q, n, u = lax.div(c, 4), lax.div(c, 2), v // 2
        at = pl.ds(v % 2 * PR, PR)
        with jax.named_scope("finish_w"):
            if v == 0:
                load_res(q).wait()
            if v == 0:
                done(terms_of(q, 1), r_part.at[1, lax.rem(q, RING // 4)])
            to_inner(c, 1).wait_recv()
            to_other(c).wait_recv()
        with jax.named_scope("finish"):
            term = _dot(s_s[lax.rem(chunk(c), 3), at, :], wo_s[lax.rem(q, NI), 1, :, u * PC : (u + 1) * PC], 1, 0)
            term = term + part[1, lax.rem(n, RING // 2), at, :].astype(jnp.float32)
            term = term + from_e[1, ring(c)].astype(jnp.float32) + from_m[lax.rem(c, 8)].astype(jnp.float32)
            term = term + xres[lax.rem(q, 2), at, u * PC : (u + 1) * PC].astype(jnp.float32)
            sbuf[1, lax.rem(n, NP // 2), at, :] = term.astype(jnp.bfloat16)
            result_to_outer(c, 1, held(1, c)).start()
            result_to_other(c).start()
            if v % 2 == 1:
                result_to_partner(n, 1, sbuf.at[1, lax.rem(n, NP // 2)], core).start()
                result_here(n).start()

    def middle_forward(c, v):
        src = y_at(c, core, 0)
        with jax.named_scope("forward_w"):
            done(from_m.at[0], r_mid.at[lax.rem(c, 8)])
        result_to_outer(c, 0, src).start()
        if v % 2 == 1:
            n = lax.div(c, 2)
            result_to_partner(n, 0, y_unit(n, core, 0), core).start()

    def middle_turn(t, j):
        s = 4 * t + j

        @pl.when(is_piece(s - 16) & middle)
        def _():
            middle_pass(s - 16, j)

        @pl.when(is_piece(s - 18) & middle)
        def _():
            middle_finish(s - 18, (j + 2) % 4)

        @pl.when(is_piece(s - 20) & middle)
        def _():
            middle_forward(s - 20, j)

    def norms(first, k):
        def one(i, carry):
            b = first + i
            with jax.named_scope("x_w"):
                load_x(b).wait()
            slot = lax.rem(b, NI)

            def squares(j, total):
                at = pl.ds(pl.multiple_of(j * WIDE, WIDE), WIDE)
                for g in range(XR // ROWS):
                    wide = xb[slot, g * ROWS : g * ROWS + ROWS, at].astype(jnp.float32)
                    wide = wide * wide
                    some = wide[:, :HEAD]
                    for n in range(1, 8):
                        some = some + wide[:, n * HEAD : (n + 1) * HEAD]
                    total = total[:g] + (total[g] + some,) + total[g + 1 :]
                return total

            total = lax.fori_loop(0, d // WIDE, squares, (jnp.zeros((ROWS, HEAD), jnp.float32),) * (XR // ROWS))
            sizes = [lax.rsqrt(jnp.sum(v, -1, keepdims=True) / d + 1e-6) for v in total]
            sizes = tuple(jnp.broadcast_to(v, (ROWS, HEAD)) for v in sizes)

            def scaled(j, sizes):
                at = pl.ds(pl.multiple_of(j * WIDE, WIDE), WIDE)
                for g in range(XR // ROWS):
                    wide = xb[slot, g * ROWS : g * ROWS + ROWS, at].astype(jnp.float32)
                    wide = wide * jnp.concatenate([sizes[g]] * 8, axis=1)
                    wide = wide.reshape(2, 8, WIDE) * gain_s[:, at][None]
                    a_s[k, pl.ds(pl.multiple_of(i * XR + g * ROWS, ROWS), ROWS), at] = wide.reshape(ROWS, WIDE).astype(jnp.bfloat16)
                return sizes

            lax.fori_loop(0, d // WIDE, scaled, sizes)
            angles(b)
            if k == 0:
                @pl.when(b == 0)
                def _():
                    for kb in (2, 3):
                        for m in range(3):
                            load_w(0, kb, m).start()
            else:
                more_x(b + NI)
            return carry

        lax.fori_loop(0, NI, one, 0)

    def step(t, carry):
        def is_block(q):
            return (q >= 0) & (q < steps)

        @pl.when(is_block(t - 8) & middle)
        def _():
            q = t - 8
            done(block(q, 0), s_u.at[0, lax.rem(q, NI)])
            for sem in (s_u.at[1], s_e.at[1], s_p.at[1], s_l):
                done(block(q, 1), sem.at[lax.rem(q, NI)])

        @pl.when(is_block(t - 9) & middle)
        def _():
            q = t - 9
            for sem in (s_e, s_p):
                done(block(q, 0), sem.at[0, lax.rem(q, NI)])

        @pl.when(is_block(t - 4) & middle)
        def _():
            load_res(t - 4).start()

        first = t == NI - 1

        @pl.when(first)
        def _():
            for ab in BOTH:
                load_away(0, ab).start()
                load_wo(0, ab).start()

        @pl.when((t == NI) | (t == NI + 1))
        def _():
            for ab in BOTH:
                load_wo(t - 2, ab).start()

        ahead = (t >= NI) & (t + NI < steps)
        middle_turn(t, 0)

        @pl.when(ahead)
        def _():
            with jax.named_scope("project0"):
                project(t, 0, True)

        @pl.when(jnp.logical_not(ahead) & (t < steps))
        def _():
            with jax.named_scope("project0_"):
                project(t, 0, False)

        @pl.when(first)
        def _():
            for ab in BOTH:
                load_away(1, ab).start()
                load_wo(1, ab).start()
            for b in range(NI, 2 * NI):
                load_x(b).start()

        middle_turn(t, 1)

        @pl.when(t < steps)
        def _():
            with jax.named_scope("project1"):
                project(t, 1, False)

        @pl.when(first)
        def _():
            more_w(t, 0)

        @pl.when(t < steps)
        def _():
            with jax.named_scope("rotate"):
                rotate(t)

        middle_turn(t, 2)

        @pl.when((t >= NI) & (t < steps))
        def _():
            with jax.named_scope("attend"):
                attend(t)

        @pl.when(first)
        def _():
            with jax.named_scope("attend_first"):
                attend_first()
            more_w(t, 1)

        middle_turn(t, 3)
        i = lax.rem(t, NI)

        @pl.when(is_block(t - 3) & (i == NI - 1))
        def _():
            send_away(t - 3)

            @pl.when(end)
            def _():
                end_sum(t - 3)

        @pl.when(is_block(t - 2) & (i != NI - 2))
        def _():
            send_away(t - 2)

            @pl.when(end)
            def _():
                end_sum(t - 2)

        @pl.when(t == NI - 1)
        def _():
            with jax.named_scope("norm1"):
                norms(NI, 1)

        @pl.when(is_block(t - 8) & end)
        def _():
            for ab in (1, 0):
                with jax.named_scope("result_w"):
                    done(block(t - 8, ab), r_end.at[ab, lax.rem(t - 8, RING // 4)])
                for u in BOTH:
                    n = 2 * (t - 8) + u
                    result_to_partner(n, ab, y_unit(n, core, ab), core).start()

        @pl.when(is_block(t - 9) & end)
        def _():
            for ab in BOTH:
                done(block(t - 9, ab), s_p.at[ab, lax.rem(t - 9, NI)])

        @pl.when(t == steps + 2)
        def _():
            for n in range(len(stash()) - NI):
                keep(n).start()

        for i in BOTH:
            @pl.when(t == steps + 6 + i)
            def _(i=i):
                keep_late(i)

        @pl.when(t == steps + 6)
        def _():
            for n in range(len(stash()) - NI, len(stash())):
                keep(n).start()

        @pl.when(is_block(t - 9))
        def _():
            with jax.named_scope("y_w"):
                done(sbuf.at[:, pl.ds(0, 2)], r_y.at[lax.rem(t - 9, RING // 4)])

        return carry

    with jax.named_scope("angles"):
        first_angles()
    with jax.named_scope("norm0"):
        norms(0, 0)

    with jax.named_scope("barrier"):
        @pl.when(end)
        def _():
            pl.semaphore_wait(barrier, 2)

        @pl.when(middle)
        def _():
            pl.semaphore_wait(barrier, 3)

    lax.fori_loop(0, steps + 9, step, 0)
    done(y_ref.at[pl.ds(0, rows - R)], keep_sem.at[0])
    done(y_ref.at[pl.ds(0, PR)], keep_sem.at[1])

    for q in range(steps - 2, steps):
        away_sent(q)

    @pl.when(end)
    def _():
        for q in range(steps - NI, steps):
            end_sent(q)


def solution(mesh):
    def step(x, gain, wq, wk, wv, wo):
        rows, d = x.shape
        own = wq.shape[1]
        chunks = rows // R
        half = HEAD // 2
        freq = np.float32(THETA) ** (-np.arange(half, dtype=np.float32) / half)
        freq = jnp.asarray(np.concatenate([freq, freq])[None], jnp.float32)
        bf16, f32 = jnp.bfloat16, jnp.float32
        hbm = pl.BlockSpec(memory_space=pl.ANY)
        vmem = pl.BlockSpec(memory_space=pltpu.VMEM)
        dma = pltpu.SemaphoreType.DMA
        parts = [(NI, XR, d), (2, R, d), (NB, KB, 768), (rows, own), (own // HEAD, HEAD + 8, rows)]
        y, *kept = pl.pallas_call(
            _kernel,
            out_shape=[jax.ShapeDtypeStruct((rows, d), bf16)] + [pltpu.VMEM(shape, bf16) for shape in parts],
            in_specs=[hbm, vmem, vmem, hbm, hbm, hbm, hbm],
            out_specs=[hbm] + [vmem] * len(parts),
            scratch_shapes=[
                pltpu.VMEM((8, d), f32),
                pltpu.VMEM((XR, d), bf16),
                pltpu.VMEM((R, 768), f32),
                pltpu.VMEM((NI, 2, own, 2 * PC), bf16),
                pltpu.VMEM((3, R, own), bf16),
                pltpu.VMEM((own // HEAD, R, HEAD), bf16),
                pltpu.VMEM((2, R, HEAD), f32),
                pltpu.VMEM((2, R, HEAD), f32),
                pltpu.VMEM((2, R, HEAD), f32),
                pltpu.VMEM((2, 1, R), f32),
                pltpu.VMEM((2, HEAD + 8, R), f32),
                pltpu.VMEM((2, RING // 2, R, PC), bf16),
                pltpu.VMEM((2, RING, PR, PC), bf16),
                pltpu.VMEM((8, PR, PC), bf16),
                pltpu.VMEM((2, 4, R, PC), bf16),
                pltpu.VMEM((2, NP // 2, R, PC), bf16),
                pltpu.VMEM((2, R, 2 * PC), bf16),
                pltpu.VMEM((2, 2, own, 2 * PC), bf16),
                dma((NI,)),
                dma((NB,)),
                dma((NI,)),
                dma((2, 2)),
                dma((2,)),
                dma((2, RING // 4)),
                dma((2, RING)),
                dma((8,)),
                dma((2, RING // 4)),
                dma((8,)),
                dma((RING // 4,)),
                dma((2,)),
                dma((2, NI)),
                dma((2, NI)),
                dma((2, NI)),
                dma((NI,)),
                dma((2,)),
            ],
            compiler_params=pltpu.CompilerParams(collective_id=1, has_side_effects=True, vmem_limit_bytes=VMEM),
            name="layer",
        )(x, gain, freq, wq, wk, wv, wo)
        return pl.pallas_call(
            _gather,
            out_shape=jax.ShapeDtypeStruct((rows, d), bf16),
            in_specs=[hbm] + [vmem] * len(parts),
            out_specs=hbm,
            scratch_shapes=[pltpu.VMEM((NP // 2, R, 2 * PC), bf16), dma((NP // 2,)), dma((3,))],
            compiler_params=pltpu.CompilerParams(vmem_limit_bytes=3 * 2**20),
            name="gather",
        )(y, *kept)

    tokens, columns = P("dp", None), P(None, "tp")
    return jax.shard_map(
        step,
        mesh=mesh,
        in_specs=(tokens, P(None), columns, columns, columns, P("tp", None)),
        out_specs=tokens,
        check_vma=False,
    )
```
